8 devices in a mesh: col: 2 (over z, y), row: 2 (over x), depth: 2 (over core).
Axes of the slice: x: 2, y: 2, z: 1, core: 2. Of those that a mesh axis runs over, the one named last changes fastest.
Arguments:
- a_mat: bfloat16 [3072, 6144], P(('depth', 'row', 'col'))
- b_mat: bfloat16 [6144, 5120], P(('depth', 'row', 'col'))
Outputs:
- output: bfloat16 [3072, 5120], P(('depth', 'row', 'col'))
All inputs are finite; a program needn't handle non-finite values.
Results may differ from the reference program's by a relative error of at most 0.001.
Values are sent between devices in bfloat16 or wider.
A program may use at most 1 GiB of HBM per device.

```python
import jax
import jax.numpy as jnp

D = 3072
F = 5120
TOKENS = 6144


def setup_inputs(seed: int = 0) -> dict:
    key_a, key_b = jax.random.split(jax.random.key(seed))
    a_vals = jax.random.normal(key_a, (D, TOKENS), jnp.float32)
    b_vals = jax.random.normal(key_b, (TOKENS, F), jnp.float32) * (TOKENS ** -0.5)
    return {"a_mat": a_vals.astype(jnp.bfloat16), "b_mat": b_vals.astype(jnp.bfloat16)}


def reference(a_mat, b_mat):
    product = jnp.dot(a_mat, b_mat, preferred_element_type=jnp.float32)
    return product.astype(jnp.bfloat16)
```

```python
import jax
import jax.numpy as jnp
from jax import lax
from jax.experimental import pallas as pl
from jax.experimental.pallas import tpu as pltpu
from jax.sharding import PartitionSpec as P

MESH = pl.DeviceIdType.MESH
TN = 512
LAG = 2


def kernel(a_ref, b_ref, c_ref, b_buf, a_own, a_nbr, p_own, p_snd, p_rcv, stage,
           ld_a, ld_b, a_snd_sem, a_rcv_sem, x_snd_sem, x_rcv_sem, d_snd_sem, d_rcv_sem,
           r_snd_sem, r_rcv_sem, c_snd_sem, c_rcv_sem, out_sem):
    depth, row, col = lax.axis_index("depth"), lax.axis_index("row"), lax.axis_index("col")
    to_y, to_x, to_d = {"col": 1 - col}, {"row": 1 - row}, {"depth": 1 - depth}
    rows, k_rows = a_ref.shape[0], b_ref.shape[0]
    half = rows // 2
    n_chunks = b_buf.shape[0]

    def k_block(place, c):
        d = 1 - depth if place % 2 else depth
        r = 1 - row if place // 2 else row
        return pl.ds(pl.multiple_of((d * 4 + r * 2 + c) * k_rows, k_rows), k_rows)

    def slot(place):
        return pl.ds(place * k_rows, k_rows)

    def cols(j):
        return pl.ds(pl.multiple_of(j * TN, TN), TN)

    def load_a(place):
        return pltpu.make_async_copy(a_ref.at[:, k_block(place, col)], a_own.at[:, slot(place)], ld_a.at[place])

    def load_b(j):
        return pltpu.make_async_copy(b_ref.at[:, cols(j)], b_buf.at[j, slot(0), :], ld_b.at[j])

    def send_a(h, place):
        return pltpu.make_async_remote_copy(
            src_ref=a_ref.at[pl.ds(h * half, half), k_block(place, 1 - col)],
            dst_ref=a_nbr.at[pl.ds(h * half, half), slot(place)],
            send_sem=a_snd_sem.at[h, place], recv_sem=a_rcv_sem.at[h, place], device_id=to_y, device_id_type=MESH)

    def send_x(j):
        return pltpu.make_async_remote_copy(
            src_ref=b_ref.at[:, cols(j)], dst_ref=b_buf.at[j, slot(2), :],
            send_sem=x_snd_sem.at[j], recv_sem=x_rcv_sem.at[j], device_id=to_x, device_id_type=MESH)

    def send_d(j):
        return pltpu.make_async_remote_copy(
            src_ref=b_ref.at[:, cols(j)], dst_ref=b_buf.at[j, slot(1), :],
            send_sem=d_snd_sem.at[j], recv_sem=d_rcv_sem.at[j], device_id=to_d, device_id_type=MESH)

    def relay(j):
        return pltpu.make_async_remote_copy(
            src_ref=b_buf.at[j, slot(2), :], dst_ref=b_buf.at[j, slot(3), :],
            send_sem=r_snd_sem.at[j], recv_sem=r_rcv_sem.at[j], device_id=to_d, device_id_type=MESH)

    def send_c(j, h):
        return pltpu.make_async_remote_copy(
            src_ref=p_snd.at[j, pl.ds(h * half, half), :], dst_ref=p_rcv.at[j, pl.ds(h * half, half), :],
            send_sem=c_snd_sem.at[j, h], recv_sem=c_rcv_sem.at[j, h], device_id=to_y, device_id_type=MESH)

    def store_c(j, s):
        return pltpu.make_async_copy(stage.at[s], c_ref.at[:, cols(j)], out_sem.at[s])

    for place in range(4):
        load_a(place).start()

    @pl.loop(0, n_chunks)
    def _(j):
        load_b(j).start()

    barrier = pltpu.get_barrier_semaphore()
    for peer in (to_y, to_x, to_d):
        pl.semaphore_signal(barrier, inc=1, device_id=peer, device_id_type=MESH)
    pl.semaphore_wait(barrier, 3)

    for h in range(2):
        for place in range(4):
            send_a(h, place).start()

    @pl.loop(0, n_chunks)
    def _(j):
        send_x(j).start()
        send_d(j).start()

    for place in range(4):
        load_a(place).wait()

    def part(j, h):
        p_snd[j, pl.ds(h * half, half), :] = jnp.dot(
            a_nbr[pl.ds(h * half, half), :], b_buf[j], preferred_element_type=jnp.float32)

    @pl.loop(0, n_chunks)
    def _(j):
        send_x(j).wait_recv()
        relay(j).start()
        load_b(j).wait()
        send_d(j).wait_recv()
        relay(j).wait_recv()

        @pl.when(j == 0)
        def _():
            for place in range(4):
                send_a(0, place).wait_recv()

        @pl.when(j == LAG)
        def _():
            for place in range(4):
                send_a(1, place).wait_recv()

        part(j, 0)

        @pl.when(j >= LAG)
        def _():
            part(j - LAG, 1)

        p_own[j] = jnp.dot(a_own[...], b_buf[j], preferred_element_type=jnp.float32)
        send_c(j, 0).start()

        @pl.when(j >= LAG)
        def _():
            send_c(j - LAG, 1).start()

    @pl.loop(n_chunks - LAG, n_chunks)
    def _(j):
        part(j, 1)

    def finish(j):
        s = lax.rem(j, 2)

        @pl.when(j >= 2)
        def _():
            store_c(j - 2, s).wait()

        for h in range(2):
            send_c(j, h).wait_recv()
            piece = pl.ds(h * half, half)
            stage[s, piece, :] = (p_own[j, piece, :] + p_rcv[j, piece, :]).astype(stage.dtype)
        store_c(j, s).start()

    finish(0)
    for j in range(n_chunks - LAG, n_chunks):
        send_c(j, 1).start()

    @pl.loop(1, n_chunks)
    def _(j):
        finish(j)

    for h in range(2):
        for place in range(4):
            send_a(h, place).wait_send()

    @pl.loop(0, n_chunks)
    def _(j):
        send_x(j).wait_send()
        send_d(j).wait_send()
        relay(j).wait_send()
        for h in range(2):
            send_c(j, h).wait_send()

    for j in range(n_chunks - 2, n_chunks):
        store_c(j, j % 2).wait()


def solution(mesh):
    all_axes = ("depth", "row", "col")

    def device_block(a_rows, b_rows):
        rows, depth = a_rows.shape
        k_rows, n = b_rows.shape
        k = 4 * k_rows
        n_chunks = n // TN
        dma = pltpu.SemaphoreType.DMA
        return pl.pallas_call(
            kernel,
            out_shape=jax.ShapeDtypeStruct((rows, n), jnp.bfloat16),
            in_specs=[pl.BlockSpec(memory_space=pl.ANY)] * 2,
            out_specs=pl.BlockSpec(memory_space=pl.ANY),
            scratch_shapes=[
                pltpu.VMEM((n_chunks, k, TN), jnp.bfloat16),
                pltpu.VMEM((rows, k), jnp.bfloat16),
                pltpu.VMEM((rows, k), jnp.bfloat16),
                pltpu.VMEM((n_chunks, rows, TN), jnp.float32),
                pltpu.VMEM((n_chunks, rows, TN), jnp.float32),
                pltpu.VMEM((n_chunks, rows, TN), jnp.float32),
                pltpu.VMEM((2, rows, TN), jnp.bfloat16),
                dma((4,)), dma((n_chunks,)),
                dma((2, 4)), dma((2, 4)),
                dma((n_chunks,)), dma((n_chunks,)),
                dma((n_chunks,)), dma((n_chunks,)),
                dma((n_chunks,)), dma((n_chunks,)),
                dma((n_chunks, 2)), dma((n_chunks, 2)),
                dma((2,)),
            ],
            compiler_params=pltpu.CompilerParams(
                collective_id=0, has_side_effects=True, vmem_limit_bytes=67043328),
        )(a_rows, b_rows)

    return jax.shard_map(device_block, mesh=mesh, in_specs=(P(all_axes, None), P(all_axes, None)),
                         out_specs=P(all_axes, None), check_vma=False)
```

```python
import jax
import jax.numpy as jnp
from jax import lax
from jax.experimental import pallas as pl
from jax.experimental.pallas import tpu as pltpu
from jax.sharding import PartitionSpec as P

MESH = pl.DeviceIdType.MESH
TN = 512
LAG = 2


def kernel(a_ref, b_ref, c_ref, b_buf, a_own, a_nbr, p_own, p_snd, p_rcv, a_first,
           ld_f, ld_a, ld_b, a_snd_sem, a_rcv_sem, x_snd_sem, x_rcv_sem, d_snd_sem, d_rcv_sem,
           r_snd_sem, r_rcv_sem, c_snd_sem, c_rcv_sem):
    depth, row, col = lax.axis_index("depth"), lax.axis_index("row"), lax.axis_index("col")
    to_y, to_x, to_d = {"col": 1 - col}, {"row": 1 - row}, {"depth": 1 - depth}
    rows, k_rows = a_ref.shape[0], b_ref.shape[0]
    half = rows // 2
    n_chunks = b_buf.shape[0]

    def k_block(place, c):
        d = 1 - depth if place % 2 else depth
        r = 1 - row if place // 2 else row
        return pl.ds(pl.multiple_of((d * 4 + r * 2 + c) * k_rows, k_rows), k_rows)

    def slot(place):
        return pl.ds(place * k_rows, k_rows)

    def cols(j):
        return pl.ds(pl.multiple_of(j * TN, TN), TN)

    def load_a(place):
        return pltpu.make_async_copy(a_ref.at[:, k_block(place, col)], a_own.at[:, slot(place)], ld_a.at[place])

    def load_b(j):
        return pltpu.make_async_copy(b_ref.at[:, cols(j)], b_buf.at[j, slot(0), :], ld_b.at[j])

    def load_first():
        return pltpu.make_async_copy(a_ref.at[pl.ds(0, half), k_block(0, 1 - col)], a_first, ld_f)

    def send_a(h, place):
        first = h == 0 and place == 0
        return pltpu.make_async_remote_copy(
            src_ref=a_first if first else a_ref.at[pl.ds(h * half, half), k_block(place, 1 - col)],
            dst_ref=a_nbr.at[pl.ds(h * half, half), slot(place)],
            send_sem=a_snd_sem.at[h, place], recv_sem=a_rcv_sem.at[h, place], device_id=to_y, device_id_type=MESH)

    def send_x(j):
        return pltpu.make_async_remote_copy(
            src_ref=b_ref.at[:, cols(j)], dst_ref=b_buf.at[j, slot(2), :],
            send_sem=x_snd_sem.at[j], recv_sem=x_rcv_sem.at[j], device_id=to_x, device_id_type=MESH)

    def send_d(j):
        return pltpu.make_async_remote_copy(
            src_ref=b_ref.at[:, cols(j)], dst_ref=b_buf.at[j, slot(1), :],
            send_sem=d_snd_sem.at[j], recv_sem=d_rcv_sem.at[j], device_id=to_d, device_id_type=MESH)

    def relay(j):
        return pltpu.make_async_remote_copy(
            src_ref=b_buf.at[j, slot(2), :], dst_ref=b_buf.at[j, slot(3), :],
            send_sem=r_snd_sem.at[j], recv_sem=r_rcv_sem.at[j], device_id=to_d, device_id_type=MESH)

    def send_c(j, h):
        return pltpu.make_async_remote_copy(
            src_ref=p_snd.at[j, pl.ds(h * half, half), :], dst_ref=p_rcv.at[j, pl.ds(h * half, half), :],
            send_sem=c_snd_sem.at[j, h], recv_sem=c_rcv_sem.at[j, h], device_id=to_y, device_id_type=MESH)

    load_first().start()

    barrier = pltpu.get_barrier_semaphore()
    for peer in (to_y, to_x, to_d):
        pl.semaphore_signal(barrier, inc=1, device_id=peer, device_id_type=MESH)
    pl.semaphore_wait(barrier, 3)

    load_first().wait()
    for h in range(2):
        for place in range(4):
            send_a(h, place).start()

    @pl.loop(0, n_chunks)
    def _(j):
        send_x(j).start()

    for place in range(4):
        load_a(place).start()

    @pl.loop(0, n_chunks)
    def _(j):
        send_d(j).start()
        load_b(j).start()

    for place in range(4):
        load_a(place).wait()

    def part(j, h):
        p_snd[j, pl.ds(h * half, half), :] = jnp.dot(
            a_nbr[pl.ds(h * half, half), :], b_buf[j], preferred_element_type=jnp.float32)

    @pl.loop(0, n_chunks)
    def _(j):
        send_x(j).wait_recv()
        relay(j).start()
        load_b(j).wait()
        send_d(j).wait_recv()
        relay(j).wait_recv()

        @pl.when(j == 0)
        def _():
            for place in range(4):
                send_a(0, place).wait_recv()

        @pl.when(j == LAG)
        def _():
            for place in range(4):
                send_a(1, place).wait_recv()

        part(j, 0)

        @pl.when(j >= LAG)
        def _():
            part(j - LAG, 1)

        p_own[j] = jnp.dot(a_own[...], b_buf[j], preferred_element_type=jnp.float32)
        send_c(j, 0).start()

        @pl.when(j >= LAG)
        def _():
            send_c(j - LAG, 1).start()

    @pl.loop(n_chunks - LAG, n_chunks)
    def _(j):
        part(j, 1)

    def finish(j):
        for h in range(2):
            send_c(j, h).wait_recv()
            piece = pl.ds(h * half, half)
            c_ref[piece, cols(j)] = (p_own[j, piece, :] + p_rcv[j, piece, :]).astype(c_ref.dtype)

    finish(0)
    for j in range(n_chunks - LAG, n_chunks):
        send_c(j, 1).start()

    @pl.loop(1, n_chunks)
    def _(j):
        finish(j)

    for h in range(2):
        for place in range(4):
            send_a(h, place).wait_send()

    @pl.loop(0, n_chunks)
    def _(j):
        send_x(j).wait_send()
        send_d(j).wait_send()
        relay(j).wait_send()
        for h in range(2):
            send_c(j, h).wait_send()


def solution(mesh):
    all_axes = ("depth", "row", "col")

    def device_block(a_rows, b_rows):
        rows, depth = a_rows.shape
        k_rows, n = b_rows.shape
        k = 4 * k_rows
        n_chunks = n // TN
        dma = pltpu.SemaphoreType.DMA
        return pl.pallas_call(
            kernel,
            out_shape=pltpu.VMEM((rows, n), jnp.bfloat16),
            in_specs=[pl.BlockSpec(memory_space=pl.ANY)] * 2,
            out_specs=pl.BlockSpec(memory_space=pltpu.VMEM),
            scratch_shapes=[
                pltpu.VMEM((n_chunks, k, TN), jnp.bfloat16),
                pltpu.VMEM((rows, k), jnp.bfloat16),
                pltpu.VMEM((rows, k), jnp.bfloat16),
                pltpu.VMEM((n_chunks, rows, TN), jnp.float32),
                pltpu.VMEM((n_chunks, rows, TN), jnp.float32),
                pltpu.VMEM((n_chunks, rows, TN), jnp.float32),
                pltpu.VMEM((rows // 2, k_rows), jnp.bfloat16),
                dma, dma((4,)), dma((n_chunks,)),
                dma((2, 4)), dma((2, 4)),
                dma((n_chunks,)), dma((n_chunks,)),
                dma((n_chunks,)), dma((n_chunks,)),
                dma((n_chunks,)), dma((n_chunks,)),
                dma((n_chunks, 2)), dma((n_chunks, 2)),
            ],
            compiler_params=pltpu.CompilerParams(
                collective_id=0, has_side_effects=True, vmem_limit_bytes=67043328 - 2 * rows * n),
        )(a_rows, b_rows)

    return jax.shard_map(device_block, mesh=mesh, in_specs=(P(all_axes, None), P(all_axes, None)),
                         out_specs=P(all_axes, None), check_vma=False)
```

```python
import jax
import jax.numpy as jnp
from jax import lax
from jax.experimental import pallas as pl
from jax.experimental.pallas import tpu as pltpu
from jax.sharding import PartitionSpec as P

MESH = pl.DeviceIdType.MESH
TN = 512
LAG = 2
EXTRA = 96


def kernel(a_ref, b_ref, c_ref, b_buf, a_own, a_nbr, p_own, p_snd, p_rcv, a_first, a_fwd,
           ld_f, ld_a, ld_b, a_snd_sem, a_rcv_sem, x_snd_sem, x_rcv_sem, d_snd_sem, d_rcv_sem,
           r_snd_sem, r_rcv_sem, c_snd_sem, c_rcv_sem, f_snd_sem, f_rcv_sem, fwd_sem,
           pair_sem, core_sem):
    depth, row, col = lax.axis_index("depth"), lax.axis_index("row"), lax.axis_index("col")
    to_y, to_x, to_d = {"col": 1 - col}, {"row": 1 - row}, {"depth": 1 - depth}
    rows, k_rows = a_ref.shape[0], b_ref.shape[0]
    half = rows // 2
    n_chunks = b_buf.shape[0]

    def k_block(place, c):
        d = 1 - depth if place % 2 else depth
        r = 1 - row if place // 2 else row
        return pl.ds(pl.multiple_of((d * 4 + r * 2 + c) * k_rows, k_rows), k_rows)

    def slot(place):
        return pl.ds(place * k_rows, k_rows)

    def cols(j):
        return pl.ds(pl.multiple_of(j * TN, TN), TN)

    def load_a(place):
        return pltpu.make_async_copy(a_ref.at[:, k_block(place, col)], a_own.at[:, slot(place)], ld_a.at[place])

    def load_b(j):
        return pltpu.make_async_copy(b_ref.at[:, cols(j)], b_buf.at[j, slot(0), :], ld_b.at[j])

    def load_first():
        return pltpu.make_async_copy(a_ref.at[pl.ds(0, half), k_block(0, 1 - col)], a_first, ld_f)

    pieces = [(0, half, p) for p in range(4)] + [(half, half, p) for p in range(3)]
    pieces += [(half, half - EXTRA, 3), (rows - EXTRA, EXTRA, 3)]
    last = len(pieces) - 1

    def send_a(i):
        start, size, place = pieces[i]
        return pltpu.make_async_remote_copy(
            src_ref=a_first if i == 0 else a_ref.at[pl.ds(start, size), k_block(place, 1 - col)],
            dst_ref=a_nbr.at[pl.ds(start, size), slot(place)],
            send_sem=a_snd_sem.at[i], recv_sem=a_rcv_sem.at[i], device_id=to_y, device_id_type=MESH)

    def hand_over():
        start, size, place = pieces[last]
        return pltpu.make_async_remote_copy(
            src_ref=a_ref.at[pl.ds(start, size), k_block(place, 1 - col)], dst_ref=a_fwd,
            send_sem=f_snd_sem, recv_sem=f_rcv_sem, device_id=to_d, device_id_type=MESH)

    def send_for_other():
        start, size, place = pieces[last]
        return pltpu.make_async_remote_copy(
            src_ref=a_fwd, dst_ref=a_nbr.at[pl.ds(start, size), slot(place)],
            send_sem=fwd_sem, recv_sem=a_rcv_sem.at[last],
            device_id={"col": 1 - col, "depth": 0}, device_id_type=MESH)

    def send_x(j):
        return pltpu.make_async_remote_copy(
            src_ref=b_ref.at[:, cols(j)], dst_ref=b_buf.at[j, slot(2), :],
            send_sem=x_snd_sem.at[j], recv_sem=x_rcv_sem.at[j], device_id=to_x, device_id_type=MESH)

    def send_d(j):
        return pltpu.make_async_remote_copy(
            src_ref=b_ref.at[:, cols(j)], dst_ref=b_buf.at[j, slot(1), :],
            send_sem=d_snd_sem.at[j], recv_sem=d_rcv_sem.at[j], device_id=to_d, device_id_type=MESH)

    def relay(j):
        return pltpu.make_async_remote_copy(
            src_ref=b_buf.at[j, slot(2), :], dst_ref=b_buf.at[j, slot(3), :],
            send_sem=r_snd_sem.at[j], recv_sem=r_rcv_sem.at[j], device_id=to_d, device_id_type=MESH)

    def send_c(j, h):
        return pltpu.make_async_remote_copy(
            src_ref=p_snd.at[j, pl.ds(h * half, half), :], dst_ref=p_rcv.at[j, pl.ds(h * half, half), :],
            send_sem=c_snd_sem.at[j, h], recv_sem=c_rcv_sem.at[j, h], device_id=to_y, device_id_type=MESH)

    load_first().start()

    barrier = pltpu.get_barrier_semaphore()
    for peer in (to_y, {"depth": 0, "row": lax.rem(row + 1 - depth, 2)}):
        pl.semaphore_signal(barrier, inc=1, device_id=peer, device_id_type=MESH)
    pl.semaphore_wait(barrier, 3 - 2 * depth)

    load_first().wait()
    for i in range(last):
        send_a(i).start()

    @pl.when(depth == 0)
    def _():
        hand_over().start()
        pl.semaphore_signal(pair_sem, inc=1, device_id=to_x, device_id_type=MESH)
        pl.semaphore_wait(pair_sem, 1)
        pl.semaphore_signal(core_sem, inc=1, device_id=to_d, device_id_type=MESH)

    @pl.when(depth == 1)
    def _():
        send_a(last).start()
        pl.semaphore_wait(core_sem, 1)

    @pl.loop(0, n_chunks)
    def _(j):
        send_x(j).start()

    for place in range(4):
        load_a(place).start()

    @pl.loop(0, n_chunks)
    def _(j):
        send_d(j).start()
        load_b(j).start()

    @pl.when(depth == 1)
    def _():
        hand_over().wait_recv()
        send_for_other().start()

    for place in range(4):
        load_a(place).wait()

    def part(j, h):
        p_snd[j, pl.ds(h * half, half), :] = jnp.dot(
            a_nbr[pl.ds(h * half, half), :], b_buf[j], preferred_element_type=jnp.float32)

    @pl.loop(0, n_chunks)
    def _(j):
        send_x(j).wait_recv()
        relay(j).start()
        load_b(j).wait()
        send_d(j).wait_recv()
        relay(j).wait_recv()

        @pl.when(j == 0)
        def _():
            for i in range(4):
                send_a(i).wait_recv()

        @pl.when(j == LAG)
        def _():
            for i in range(4, last + 1):
                send_a(i).wait_recv()

        part(j, 0)

        @pl.when(j >= LAG)
        def _():
            part(j - LAG, 1)

        p_own[j] = jnp.dot(a_own[...], b_buf[j], preferred_element_type=jnp.float32)
        send_c(j, 0).start()

        @pl.when(j >= LAG)
        def _():
            send_c(j - LAG, 1).start()

    @pl.loop(n_chunks - LAG, n_chunks)
    def _(j):
        part(j, 1)

    def finish(j):
        for h in range(2):
            send_c(j, h).wait_recv()
            piece = pl.ds(h * half, half)
            c_ref[piece, cols(j)] = (p_own[j, piece, :] + p_rcv[j, piece, :]).astype(c_ref.dtype)

    finish(0)
    for j in range(n_chunks - LAG, n_chunks):
        send_c(j, 1).start()

    @pl.loop(1, n_chunks)
    def _(j):
        finish(j)

    for i in range(last):
        send_a(i).wait_send()

    @pl.when(depth == 0)
    def _():
        hand_over().wait_send()

    @pl.when(depth == 1)
    def _():
        send_a(last).wait_send()
        send_for_other().wait_send()

    @pl.loop(0, n_chunks)
    def _(j):
        send_x(j).wait_send()
        send_d(j).wait_send()
        relay(j).wait_send()
        for h in range(2):
            send_c(j, h).wait_send()


def solution(mesh):
    all_axes = ("depth", "row", "col")

    def device_block(a_rows, b_rows):
        rows, depth = a_rows.shape
        k_rows, n = b_rows.shape
        k = 4 * k_rows
        n_chunks = n // TN
        dma = pltpu.SemaphoreType.DMA
        return pl.pallas_call(
            kernel,
            out_shape=pltpu.VMEM((rows, n), jnp.bfloat16),
            in_specs=[pl.BlockSpec(memory_space=pl.ANY)] * 2,
            out_specs=pl.BlockSpec(memory_space=pltpu.VMEM),
            scratch_shapes=[
                pltpu.VMEM((n_chunks, k, TN), jnp.bfloat16),
                pltpu.VMEM((rows, k), jnp.bfloat16),
                pltpu.VMEM((rows, k), jnp.bfloat16),
                pltpu.VMEM((n_chunks, rows, TN), jnp.float32),
                pltpu.VMEM((n_chunks, rows, TN), jnp.float32),
                pltpu.VMEM((n_chunks, rows, TN), jnp.float32),
                pltpu.VMEM((rows // 2, k_rows), jnp.bfloat16),
                pltpu.VMEM((EXTRA, k_rows), jnp.bfloat16),
                dma, dma((4,)), dma((n_chunks,)),
                dma((9,)), dma((9,)),
                dma((n_chunks,)), dma((n_chunks,)),
                dma((n_chunks,)), dma((n_chunks,)),
                dma((n_chunks,)), dma((n_chunks,)),
                dma((n_chunks, 2)), dma((n_chunks, 2)),
                dma, dma, dma,
                pltpu.SemaphoreType.REGULAR, pltpu.SemaphoreType.REGULAR,
            ],
            compiler_params=pltpu.CompilerParams(
                collective_id=0, has_side_effects=True, vmem_limit_bytes=67043328 - 2 * rows * n),
        )(a_rows, b_rows)

    return jax.shard_map(device_block, mesh=mesh, in_specs=(P(all_axes, None), P(all_axes, None)),
                         out_specs=P(all_axes, None), check_vma=False)
```

```python
import jax
import jax.numpy as jnp
from jax import lax
from jax.experimental import pallas as pl
from jax.experimental.pallas import tpu as pltpu
from jax.sharding import PartitionSpec as P

MESH = pl.DeviceIdType.MESH
TN = 512
LAG = 2
EXTRA = 48


def kernel(a_ref, b_ref, c_ref, b_buf, a_own, a_nbr, p_own, p_snd, p_rcv, a_first, a_fwd,
           ld_f, ld_a, ld_b, a_snd_sem, a_rcv_sem, x_snd_sem, x_rcv_sem, d_snd_sem, d_rcv_sem,
           r_snd_sem, r_rcv_sem, c_snd_sem, c_rcv_sem, f_snd_sem, f_rcv_sem, fwd_sem,
           pair_sem, core_sem):
    depth, row, col = lax.axis_index("depth"), lax.axis_index("row"), lax.axis_index("col")
    to_y, to_x, to_d = {"col": 1 - col}, {"row": 1 - row}, {"depth": 1 - depth}
    rows, k_rows = a_ref.shape[0], b_ref.shape[0]
    half = rows // 2
    n_chunks = b_buf.shape[0]

    def k_block(place, c):
        d = 1 - depth if place % 2 else depth
        r = 1 - row if place // 2 else row
        return pl.ds(pl.multiple_of((d * 4 + r * 2 + c) * k_rows, k_rows), k_rows)

    def slot(place):
        return pl.ds(place * k_rows, k_rows)

    def cols(j):
        return pl.ds(pl.multiple_of(j * TN, TN), TN)

    def load_a(place):
        return pltpu.make_async_copy(a_ref.at[:, k_block(place, col)], a_own.at[:, slot(place)], ld_a.at[place])

    def load_b(j):
        return pltpu.make_async_copy(b_ref.at[:, cols(j)], b_buf.at[j, slot(0), :], ld_b.at[j])

    def load_first():
        return pltpu.make_async_copy(a_ref.at[pl.ds(0, half), k_block(0, 1 - col)], a_first, ld_f)

    pieces = [(0, half, p) for p in range(4)] + [(half, half, p) for p in range(3)]
    pieces += [(half, half - EXTRA, 3), (rows - EXTRA, EXTRA, 3)]
    last = len(pieces) - 1

    def send_a(i):
        start, size, place = pieces[i]
        return pltpu.make_async_remote_copy(
            src_ref=a_first if i == 0 else a_ref.at[pl.ds(start, size), k_block(place, 1 - col)],
            dst_ref=a_nbr.at[pl.ds(start, size), slot(place)],
            send_sem=a_snd_sem.at[i], recv_sem=a_rcv_sem.at[i], device_id=to_y, device_id_type=MESH)

    def hand_over():
        start, size, place = pieces[last]
        return pltpu.make_async_remote_copy(
            src_ref=a_ref.at[pl.ds(start, size), k_block(place, 1 - col)], dst_ref=a_fwd,
            send_sem=f_snd_sem, recv_sem=f_rcv_sem, device_id=to_d, device_id_type=MESH)

    def send_for_other():
        start, size, place = pieces[last]
        return pltpu.make_async_remote_copy(
            src_ref=a_fwd, dst_ref=a_nbr.at[pl.ds(start, size), slot(place)],
            send_sem=fwd_sem, recv_sem=a_rcv_sem.at[last],
            device_id={"col": 1 - col, "depth": 0}, device_id_type=MESH)

    def send_x(j):
        return pltpu.make_async_remote_copy(
            src_ref=b_ref.at[:, cols(j)], dst_ref=b_buf.at[j, slot(2), :],
            send_sem=x_snd_sem.at[j], recv_sem=x_rcv_sem.at[j], device_id=to_x, device_id_type=MESH)

    def send_d(j):
        return pltpu.make_async_remote_copy(
            src_ref=b_ref.at[:, cols(j)], dst_ref=b_buf.at[j, slot(1), :],
            send_sem=d_snd_sem.at[j], recv_sem=d_rcv_sem.at[j], device_id=to_d, device_id_type=MESH)

    def relay(j):
        return pltpu.make_async_remote_copy(
            src_ref=b_buf.at[j, slot(2), :], dst_ref=b_buf.at[j, slot(3), :],
            send_sem=r_snd_sem.at[j], recv_sem=r_rcv_sem.at[j], device_id=to_d, device_id_type=MESH)

    def send_c(j, h):
        return pltpu.make_async_remote_copy(
            src_ref=p_snd.at[j, pl.ds(h * half, half), :], dst_ref=p_rcv.at[j, pl.ds(h * half, half), :],
            send_sem=c_snd_sem.at[j, h], recv_sem=c_rcv_sem.at[j, h], device_id=to_y, device_id_type=MESH)

    load_first().start()

    barrier = pltpu.get_barrier_semaphore()
    for peer in (to_y, {"depth": 0, "row": lax.rem(row + 1 - depth, 2)}):
        pl.semaphore_signal(barrier, inc=1, device_id=peer, device_id_type=MESH)
    pl.semaphore_wait(barrier, 3 - 2 * depth)

    load_first().wait()
    for i in range(last):
        send_a(i).start()

    @pl.when(depth == 0)
    def _():
        hand_over().start()
        pl.semaphore_signal(pair_sem, inc=1, device_id=to_x, device_id_type=MESH)
        pl.semaphore_wait(pair_sem, 1)
        pl.semaphore_signal(core_sem, inc=1, device_id=to_d, device_id_type=MESH)

    @pl.when(depth == 1)
    def _():
        send_a(last).start()
        pl.semaphore_wait(core_sem, 1)

    @pl.loop(0, n_chunks)
    def _(j):
        send_x(j).start()

    for place in range(4):
        load_a(place).start()

    @pl.loop(0, n_chunks)
    def _(j):
        send_d(j).start()
        load_b(j).start()

    @pl.when(depth == 1)
    def _():
        hand_over().wait_recv()
        send_for_other().start()

    for place in range(4):
        load_a(place).wait()

    def part(j, h):
        p_snd[j, pl.ds(h * half, half), :] = jnp.dot(
            a_nbr[pl.ds(h * half, half), :], b_buf[j], preferred_element_type=jnp.float32)

    @pl.loop(0, n_chunks)
    def _(j):
        send_x(j).wait_recv()
        relay(j).start()
        load_b(j).wait()
        send_d(j).wait_recv()
        relay(j).wait_recv()

        @pl.when(j == 0)
        def _():
            for i in range(4):
                send_a(i).wait_recv()

        @pl.when(j == LAG)
        def _():
            for i in range(4, last + 1):
                send_a(i).wait_recv()

        part(j, 0)

        @pl.when(j >= LAG)
        def _():
            part(j - LAG, 1)

        p_own[j] = jnp.dot(a_own[...], b_buf[j], preferred_element_type=jnp.float32)
        send_c(j, 0).start()

        @pl.when(j >= LAG)
        def _():
            send_c(j - LAG, 1).start()

    @pl.loop(n_chunks - LAG, n_chunks)
    def _(j):
        part(j, 1)

    def finish(j):
        for h in range(2):
            send_c(j, h).wait_recv()
            piece = pl.ds(h * half, half)
            c_ref[piece, cols(j)] = (p_own[j, piece, :] + p_rcv[j, piece, :]).astype(c_ref.dtype)

    finish(0)
    for j in range(n_chunks - LAG, n_chunks):
        send_c(j, 1).start()

    @pl.loop(1, n_chunks)
    def _(j):
        finish(j)

    for i in range(last):
        send_a(i).wait_send()

    @pl.when(depth == 0)
    def _():
        hand_over().wait_send()

    @pl.when(depth == 1)
    def _():
        send_a(last).wait_send()
        send_for_other().wait_send()

    @pl.loop(0, n_chunks)
    def _(j):
        send_x(j).wait_send()
        send_d(j).wait_send()
        relay(j).wait_send()
        for h in range(2):
            send_c(j, h).wait_send()


def solution(mesh):
    all_axes = ("depth", "row", "col")

    def device_block(a_rows, b_rows):
        rows, depth = a_rows.shape
        k_rows, n = b_rows.shape
        k = 4 * k_rows
        n_chunks = n // TN
        dma = pltpu.SemaphoreType.DMA
        return pl.pallas_call(
            kernel,
            out_shape=pltpu.VMEM((rows, n), jnp.bfloat16),
            in_specs=[pl.BlockSpec(memory_space=pl.ANY)] * 2,
            out_specs=pl.BlockSpec(memory_space=pltpu.VMEM),
            scratch_shapes=[
                pltpu.VMEM((n_chunks, k, TN), jnp.bfloat16),
                pltpu.VMEM((rows, k), jnp.bfloat16),
                pltpu.VMEM((rows, k), jnp.bfloat16),
                pltpu.VMEM((n_chunks, rows, TN), jnp.float32),
                pltpu.VMEM((n_chunks, rows, TN), jnp.float32),
                pltpu.VMEM((n_chunks, rows, TN), jnp.float32),
                pltpu.VMEM((rows // 2, k_rows), jnp.bfloat16),
                pltpu.VMEM((EXTRA, k_rows), jnp.bfloat16),
                dma, dma((4,)), dma((n_chunks,)),
                dma((9,)), dma((9,)),
                dma((n_chunks,)), dma((n_chunks,)),
                dma((n_chunks,)), dma((n_chunks,)),
                dma((n_chunks,)), dma((n_chunks,)),
                dma((n_chunks, 2)), dma((n_chunks, 2)),
                dma, dma, dma,
                pltpu.SemaphoreType.REGULAR, pltpu.SemaphoreType.REGULAR,
            ],
            compiler_params=pltpu.CompilerParams(
                collective_id=0, has_side_effects=True, vmem_limit_bytes=67043328 - 2 * rows * n),
        )(a_rows, b_rows)

    return jax.shard_map(device_block, mesh=mesh, in_specs=(P(all_axes, None), P(all_axes, None)),
                         out_specs=P(all_axes, None), check_vma=False)
```

```python
import jax
import jax.numpy as jnp
from jax import lax
from jax.experimental import pallas as pl
from jax.experimental.pallas import tpu as pltpu
from jax.sharding import PartitionSpec as P

MESH = pl.DeviceIdType.MESH
TN = 512
LAG = 2
AHEAD = 2
EXTRA = 96


def kernel(a_ref, b_ref, c_ref, b_buf, a_own, a_nbr, p_own, p_snd, p_rcv, a_first, a_fwd,
           ld_f, ld_a, ld_b, a_snd_sem, a_rcv_sem, x_snd_sem, x_rcv_sem, d_snd_sem, d_rcv_sem,
           r_snd_sem, r_rcv_sem, c_snd_sem, c_rcv_sem, f_snd_sem, f_rcv_sem, fwd_sem,
           pair_sem, core_sem):
    depth, row, col = lax.axis_index("depth"), lax.axis_index("row"), lax.axis_index("col")
    to_y, to_x, to_d = {"col": 1 - col}, {"row": 1 - row}, {"depth": 1 - depth}
    rows, k_rows = a_ref.shape[0], b_ref.shape[0]
    half = rows // 2
    n_chunks = b_buf.shape[0]

    def k_block(place, c):
        d = 1 - depth if place % 2 else depth
        r = 1 - row if place // 2 else row
        return pl.ds(pl.multiple_of((d * 4 + r * 2 + c) * k_rows, k_rows), k_rows)

    def slot(place):
        return pl.ds(place * k_rows, k_rows)

    def cols(j):
        return pl.ds(pl.multiple_of(j * TN, TN), TN)

    def load_a(place):
        return pltpu.make_async_copy(a_ref.at[:, k_block(place, col)], a_own.at[:, slot(place)], ld_a.at[place])

    def load_b(j):
        return pltpu.make_async_copy(b_ref.at[:, cols(j)], b_buf.at[j, slot(0), :], ld_b.at[j])

    def load_first():
        return pltpu.make_async_copy(a_ref.at[pl.ds(0, half), k_block(0, 1 - col)], a_first, ld_f)

    pieces = [(0, half, p) for p in range(4)] + [(half, half, p) for p in range(3)]
    pieces += [(half, half - EXTRA, 3), (rows - EXTRA, EXTRA, 3)]
    last = len(pieces) - 1

    def send_a(i):
        start, size, place = pieces[i]
        return pltpu.make_async_remote_copy(
            src_ref=a_first if i == 0 else a_ref.at[pl.ds(start, size), k_block(place, 1 - col)],
            dst_ref=a_nbr.at[pl.ds(start, size), slot(place)],
            send_sem=a_snd_sem.at[i], recv_sem=a_rcv_sem.at[i], device_id=to_y, device_id_type=MESH)

    def hand_over():
        start, size, place = pieces[last]
        return pltpu.make_async_remote_copy(
            src_ref=a_ref.at[pl.ds(start, size), k_block(place, 1 - col)], dst_ref=a_fwd,
            send_sem=f_snd_sem, recv_sem=f_rcv_sem, device_id=to_d, device_id_type=MESH)

    def send_for_other():
        start, size, place = pieces[last]
        return pltpu.make_async_remote_copy(
            src_ref=a_fwd, dst_ref=a_nbr.at[pl.ds(start, size), slot(place)],
            send_sem=fwd_sem, recv_sem=a_rcv_sem.at[last],
            device_id={"col": 1 - col, "depth": 0}, device_id_type=MESH)

    def send_x(j):
        return pltpu.make_async_remote_copy(
            src_ref=b_ref.at[:, cols(j)], dst_ref=b_buf.at[j, slot(2), :],
            send_sem=x_snd_sem.at[j], recv_sem=x_rcv_sem.at[j], device_id=to_x, device_id_type=MESH)

    def send_d(j):
        return pltpu.make_async_remote_copy(
            src_ref=b_ref.at[:, cols(j)], dst_ref=b_buf.at[j, slot(1), :],
            send_sem=d_snd_sem.at[j], recv_sem=d_rcv_sem.at[j], device_id=to_d, device_id_type=MESH)

    def relay(j):
        return pltpu.make_async_remote_copy(
            src_ref=b_buf.at[j, slot(2), :], dst_ref=b_buf.at[j, slot(3), :],
            send_sem=r_snd_sem.at[j], recv_sem=r_rcv_sem.at[j], device_id=to_d, device_id_type=MESH)

    def send_c(j, h):
        return pltpu.make_async_remote_copy(
            src_ref=p_snd.at[j, pl.ds(h * half, half), :], dst_ref=p_rcv.at[j, pl.ds(h * half, half), :],
            send_sem=c_snd_sem.at[j, h], recv_sem=c_rcv_sem.at[j, h], device_id=to_y, device_id_type=MESH)

    load_first().start()

    barrier = pltpu.get_barrier_semaphore()
    for peer in (to_y, {"depth": 0, "row": lax.rem(row + 1 - depth, 2)}):
        pl.semaphore_signal(barrier, inc=1, device_id=peer, device_id_type=MESH)
    pl.semaphore_wait(barrier, 3 - 2 * depth)

    load_first().wait()
    for i in range(last):
        send_a(i).start()

    @pl.when(depth == 0)
    def _():
        hand_over().start()
        pl.semaphore_signal(pair_sem, inc=1, device_id=to_x, device_id_type=MESH)
        pl.semaphore_wait(pair_sem, 1)
        pl.semaphore_signal(core_sem, inc=1, device_id=to_d, device_id_type=MESH)

    @pl.when(depth == 1)
    def _():
        send_a(last).start()
        pl.semaphore_wait(core_sem, 1)

    @pl.loop(0, n_chunks)
    def _(j):
        send_x(j).start()

    for place in range(4):
        load_a(place).start()

    def bring(j):
        send_d(j).start()
        load_b(j).start()

    for j in range(AHEAD):
        bring(j)

    @pl.when(depth == 1)
    def _():
        hand_over().wait_recv()
        send_for_other().start()

    for place in range(4):
        load_a(place).wait()

    def part(j, h):
        p_snd[j, pl.ds(h * half, half), :] = jnp.dot(
            a_nbr[pl.ds(h * half, half), :], b_buf[j], preferred_element_type=jnp.float32)

    @pl.loop(0, n_chunks)
    def _(j):
        send_x(j).wait_recv()
        relay(j).start()

        @pl.when(j < n_chunks - AHEAD)
        def _():
            bring(j + AHEAD)

        load_b(j).wait()
        send_d(j).wait_recv()
        relay(j).wait_recv()

        @pl.when(j == 0)
        def _():
            for i in range(4):
                send_a(i).wait_recv()

        @pl.when(j == LAG)
        def _():
            for i in range(4, last + 1):
                send_a(i).wait_recv()

        part(j, 0)

        @pl.when(j >= LAG)
        def _():
            part(j - LAG, 1)

        p_own[j] = jnp.dot(a_own[...], b_buf[j], preferred_element_type=jnp.float32)
        send_c(j, 0).start()

        @pl.when(j >= LAG)
        def _():
            send_c(j - LAG, 1).start()

    @pl.loop(n_chunks - LAG, n_chunks)
    def _(j):
        part(j, 1)

    def finish(j):
        for h in range(2):
            send_c(j, h).wait_recv()
            piece = pl.ds(h * half, half)
            c_ref[piece, cols(j)] = (p_own[j, piece, :] + p_rcv[j, piece, :]).astype(c_ref.dtype)

    finish(0)
    for j in range(n_chunks - LAG, n_chunks):
        send_c(j, 1).start()

    @pl.loop(1, n_chunks - LAG)
    def _(j):
        finish(j)

    for i in range(last):
        send_a(i).wait_send()

    @pl.when(depth == 0)
    def _():
        hand_over().wait_send()

    @pl.when(depth == 1)
    def _():
        send_a(last).wait_send()
        send_for_other().wait_send()

    @pl.loop(0, n_chunks)
    def _(j):
        send_x(j).wait_send()
        send_d(j).wait_send()
        relay(j).wait_send()

    @pl.loop(0, n_chunks - LAG)
    def _(j):
        for h in range(2):
            send_c(j, h).wait_send()

    for j in range(n_chunks - LAG, n_chunks):
        finish(j)
    for j in range(n_chunks - LAG, n_chunks):
        for h in range(2):
            send_c(j, h).wait_send()


def solution(mesh):
    all_axes = ("depth", "row", "col")

    def device_block(a_rows, b_rows):
        rows, depth = a_rows.shape
        k_rows, n = b_rows.shape
        k = 4 * k_rows
        n_chunks = n // TN
        dma = pltpu.SemaphoreType.DMA
        return pl.pallas_call(
            kernel,
            out_shape=pltpu.VMEM((rows, n), jnp.bfloat16),
            in_specs=[pl.BlockSpec(memory_space=pl.ANY)] * 2,
            out_specs=pl.BlockSpec(memory_space=pltpu.VMEM),
            scratch_shapes=[
                pltpu.VMEM((n_chunks, k, TN), jnp.bfloat16),
                pltpu.VMEM((rows, k), jnp.bfloat16),
                pltpu.VMEM((rows, k), jnp.bfloat16),
                pltpu.VMEM((n_chunks, rows, TN), jnp.float32),
                pltpu.VMEM((n_chunks, rows, TN), jnp.float32),
                pltpu.VMEM((n_chunks, rows, TN), jnp.float32),
                pltpu.VMEM((rows // 2, k_rows), jnp.bfloat16),
                pltpu.VMEM((EXTRA, k_rows), jnp.bfloat16),
                dma, dma((4,)), dma((n_chunks,)),
                dma((9,)), dma((9,)),
                dma((n_chunks,)), dma((n_chunks,)),
                dma((n_chunks,)), dma((n_chunks,)),
                dma((n_chunks,)), dma((n_chunks,)),
                dma((n_chunks, 2)), dma((n_chunks, 2)),
                dma, dma, dma,
                pltpu.SemaphoreType.REGULAR, pltpu.SemaphoreType.REGULAR,
            ],
            compiler_params=pltpu.CompilerParams(
                collective_id=0, has_side_effects=True, vmem_limit_bytes=67043328 - 2 * rows * n),
        )(a_rows, b_rows)

    return jax.shard_map(device_block, mesh=mesh, in_specs=(P(all_axes, None), P(all_axes, None)),
                         out_specs=P(all_axes, None), check_vma=False)
```

```python
import jax
import jax.numpy as jnp
from jax import lax
from jax.experimental import pallas as pl
from jax.experimental.pallas import tpu as pltpu
from jax.sharding import PartitionSpec as P

MESH = pl.DeviceIdType.MESH
TN = 512
LAG = 2
AHEAD = 2
EXTRA = 96


def kernel(a_ref, b_ref, c_ref, b_buf, a_own, a_nbr, p_own, p_snd, p_rcv, a_first, a_fwd,
           ld_f, ld_a, ld_b, a_snd_sem, a_rcv_sem, x_snd_sem, x_rcv_sem, d_snd_sem, d_rcv_sem,
           r_snd_sem, r_rcv_sem, c_snd_sem, c_rcv_sem, f_snd_sem, f_rcv_sem, fwd_sem,
           pair_sem, core_sem):
    depth, row, col = lax.axis_index("depth"), lax.axis_index("row"), lax.axis_index("col")
    to_y, to_x, to_d = {"col": 1 - col}, {"row": 1 - row}, {"depth": 1 - depth}
    rows, k_rows = a_ref.shape[0], b_ref.shape[0]
    half = rows // 2
    n_chunks = b_buf.shape[0]

    def k_block(place, c):
        d = 1 - depth if place % 2 else depth
        r = 1 - row if place // 2 else row
        return pl.ds(pl.multiple_of((d * 4 + r * 2 + c) * k_rows, k_rows), k_rows)

    def slot(place):
        return pl.ds(place * k_rows, k_rows)

    def cols(j):
        return pl.ds(pl.multiple_of(j * TN, TN), TN)

    def load_a(place):
        return pltpu.make_async_copy(a_ref.at[:, k_block(place, col)], a_own.at[:, slot(place)], ld_a.at[place])

    def load_b(j):
        return pltpu.make_async_copy(b_ref.at[:, cols(j)], b_buf.at[j, slot(0), :], ld_b.at[j])

    def load_first():
        return pltpu.make_async_copy(a_ref.at[pl.ds(0, half), k_block(0, 1 - col)], a_first, ld_f)

    pieces = [(0, half, p) for p in range(4)] + [(half, half, p) for p in range(3)]
    pieces += [(half, half - EXTRA, 3), (rows - EXTRA, EXTRA, 3)]
    last = len(pieces) - 1

    def send_a(i):
        start, size, place = pieces[i]
        return pltpu.make_async_remote_copy(
            src_ref=a_first if i == 0 else a_ref.at[pl.ds(start, size), k_block(place, 1 - col)],
            dst_ref=a_nbr.at[pl.ds(start, size), slot(place)],
            send_sem=a_snd_sem.at[i], recv_sem=a_rcv_sem.at[i], device_id=to_y, device_id_type=MESH)

    def hand_over():
        start, size, place = pieces[last]
        return pltpu.make_async_remote_copy(
            src_ref=a_ref.at[pl.ds(start, size), k_block(place, 1 - col)], dst_ref=a_fwd,
            send_sem=f_snd_sem, recv_sem=f_rcv_sem, device_id=to_d, device_id_type=MESH)

    def send_for_other():
        start, size, place = pieces[last]
        return pltpu.make_async_remote_copy(
            src_ref=a_fwd, dst_ref=a_nbr.at[pl.ds(start, size), slot(place)],
            send_sem=fwd_sem, recv_sem=a_rcv_sem.at[last],
            device_id={"col": 1 - col, "depth": 0}, device_id_type=MESH)

    def send_x(j):
        return pltpu.make_async_remote_copy(
            src_ref=b_ref.at[:, cols(j)], dst_ref=b_buf.at[j, slot(2), :],
            send_sem=x_snd_sem.at[j], recv_sem=x_rcv_sem.at[j], device_id=to_x, device_id_type=MESH)

    def send_d(j):
        return pltpu.make_async_remote_copy(
            src_ref=b_ref.at[:, cols(j)], dst_ref=b_buf.at[j, slot(1), :],
            send_sem=d_snd_sem.at[j], recv_sem=d_rcv_sem.at[j], device_id=to_d, device_id_type=MESH)

    def relay(j):
        return pltpu.make_async_remote_copy(
            src_ref=b_buf.at[j, slot(2), :], dst_ref=b_buf.at[j, slot(3), :],
            send_sem=r_snd_sem.at[j], recv_sem=r_rcv_sem.at[j], device_id=to_d, device_id_type=MESH)

    def send_c(j, start, size):
        h = start // half
        return pltpu.make_async_remote_copy(
            src_ref=p_snd.at[j, pl.ds(start, size), :], dst_ref=p_rcv.at[j, pl.ds(start, size), :],
            send_sem=c_snd_sem.at[j, h], recv_sem=c_rcv_sem.at[j, h], device_id=to_y, device_id_type=MESH)

    load_first().start()

    barrier = pltpu.get_barrier_semaphore()
    for peer in (to_y, {"depth": 0, "row": lax.rem(row + 1 - depth, 2)}):
        pl.semaphore_signal(barrier, inc=1, device_id=peer, device_id_type=MESH)
    pl.semaphore_wait(barrier, 3 - 2 * depth)

    load_first().wait()
    for i in range(last):
        send_a(i).start()

    @pl.when(depth == 0)
    def _():
        hand_over().start()
        pl.semaphore_signal(pair_sem, inc=1, device_id=to_x, device_id_type=MESH)
        pl.semaphore_wait(pair_sem, 1)
        pl.semaphore_signal(core_sem, inc=1, device_id=to_d, device_id_type=MESH)

    @pl.when(depth == 1)
    def _():
        send_a(last).start()
        pl.semaphore_wait(core_sem, 1)

    @pl.loop(0, n_chunks)
    def _(j):
        send_x(j).start()

    for place in range(4):
        load_a(place).start()

    def bring(j):
        send_d(j).start()
        load_b(j).start()

    for j in range(AHEAD):
        bring(j)

    @pl.when(depth == 1)
    def _():
        hand_over().wait_recv()
        send_for_other().start()

    for place in range(4):
        load_a(place).wait()

    def part(j, start, size):
        p_snd[j, pl.ds(start, size), :] = jnp.dot(
            a_nbr[pl.ds(start, size), :], b_buf[j], preferred_element_type=jnp.float32)

    def own(j):
        p_own[j] = jnp.dot(a_own[...], b_buf[j], preferred_element_type=jnp.float32)

    def gather(j):
        send_x(j).wait_recv()
        relay(j).start()

        @pl.when(j < n_chunks - AHEAD)
        def _():
            bring(j + AHEAD)

        load_b(j).wait()
        send_d(j).wait_recv()
        relay(j).wait_recv()

    @pl.loop(0, LAG)
    def _(j):
        gather(j)

        @pl.when(j == 0)
        def _():
            for i in range(4):
                send_a(i).wait_recv()

        part(j, 0, half)
        own(j)
        send_c(j, 0, half).start()

    @pl.loop(LAG, n_chunks)
    def _(j):
        gather(j)

        @pl.when(j == LAG)
        def _():
            for i in range(4, last + 1):
                send_a(i).wait_recv()

            @pl.loop(0, LAG)
            def _(i):
                part(i, half, half)

        part(j, 0, rows)
        own(j)

        @pl.when(j == LAG)
        def _():
            for i in range(LAG):
                send_c(i, half, half).start()

        send_c(j, 0, rows).start()

    def finish(j, start, size):
        send_c(j, start, size).wait_recv()
        piece = pl.ds(start, size)
        c_ref[piece, cols(j)] = (p_own[j, piece, :] + p_rcv[j, piece, :]).astype(c_ref.dtype)

    @pl.loop(0, LAG)
    def _(j):
        finish(j, 0, half)
        finish(j, half, half)

    @pl.loop(LAG, n_chunks - 2)
    def _(j):
        finish(j, 0, rows)

    for i in range(last):
        send_a(i).wait_send()

    @pl.when(depth == 0)
    def _():
        hand_over().wait_send()

    @pl.when(depth == 1)
    def _():
        send_a(last).wait_send()
        send_for_other().wait_send()

    @pl.loop(0, n_chunks)
    def _(j):
        send_x(j).wait_send()
        send_d(j).wait_send()
        relay(j).wait_send()

    @pl.loop(0, LAG)
    def _(j):
        send_c(j, 0, half).wait_send()
        send_c(j, half, half).wait_send()

    @pl.loop(LAG, n_chunks - 2)
    def _(j):
        send_c(j, 0, rows).wait_send()

    for j in range(n_chunks - 2, n_chunks):
        finish(j, 0, rows)
    for j in range(n_chunks - 2, n_chunks):
        send_c(j, 0, rows).wait_send()


def solution(mesh):
    all_axes = ("depth", "row", "col")

    def device_block(a_rows, b_rows):
        rows, depth = a_rows.shape
        k_rows, n = b_rows.shape
        k = 4 * k_rows
        n_chunks = n // TN
        dma = pltpu.SemaphoreType.DMA
        return pl.pallas_call(
            kernel,
            out_shape=pltpu.VMEM((rows, n), jnp.bfloat16),
            in_specs=[pl.BlockSpec(memory_space=pl.ANY)] * 2,
            out_specs=pl.BlockSpec(memory_space=pltpu.VMEM),
            scratch_shapes=[
                pltpu.VMEM((n_chunks, k, TN), jnp.bfloat16),
                pltpu.VMEM((rows, k), jnp.bfloat16),
                pltpu.VMEM((rows, k), jnp.bfloat16),
                pltpu.VMEM((n_chunks, rows, TN), jnp.float32),
                pltpu.VMEM((n_chunks, rows, TN), jnp.float32),
                pltpu.VMEM((n_chunks, rows, TN), jnp.float32),
                pltpu.VMEM((rows // 2, k_rows), jnp.bfloat16),
                pltpu.VMEM((EXTRA, k_rows), jnp.bfloat16),
                dma, dma((4,)), dma((n_chunks,)),
                dma((9,)), dma((9,)),
                dma((n_chunks,)), dma((n_chunks,)),
                dma((n_chunks,)), dma((n_chunks,)),
                dma((n_chunks,)), dma((n_chunks,)),
                dma((n_chunks, 2)), dma((n_chunks, 2)),
                dma, dma, dma,
                pltpu.SemaphoreType.REGULAR, pltpu.SemaphoreType.REGULAR,
            ],
            compiler_params=pltpu.CompilerParams(
                collective_id=0, has_side_effects=True, vmem_limit_bytes=67043328 - 2 * rows * n),
        )(a_rows, b_rows)

    return jax.shard_map(device_block, mesh=mesh, in_specs=(P(all_axes, None), P(all_axes, None)),
                         out_specs=P(all_axes, None), check_vma=False)
```

```python
import jax
import jax.numpy as jnp
from jax import lax
from jax.experimental import pallas as pl
from jax.experimental.pallas import tpu as pltpu
from jax.sharding import PartitionSpec as P

MESH = pl.DeviceIdType.MESH
TN = 512
LAG = 2
AHEAD = 2
PARTS = 8
EXTRA = 96


def kernel(a_ref, b_ref, c_ref, b_buf, a_own, a_nbr, p_own, p_snd, p_rcv, a_first, a_fwd,
           ld_f, ld_a, ld_b, a_snd_sem, a_rcv_sem, x_snd_sem, x_rcv_sem, d_snd_sem, d_rcv_sem,
           r_snd_sem, r_rcv_sem, c_snd_sem, c_rcv_sem, f_snd_sem, f_rcv_sem, fwd_sem,
           pair_sem, core_sem):
    depth, row, col = lax.axis_index("depth"), lax.axis_index("row"), lax.axis_index("col")
    to_y, to_x, to_d = {"col": 1 - col}, {"row": 1 - row}, {"depth": 1 - depth}
    rows, k_rows = a_ref.shape[0], b_ref.shape[0]
    half = rows // 2
    n_chunks = b_buf.shape[0]

    def k_block(place, c):
        d = 1 - depth if place % 2 else depth
        r = 1 - row if place // 2 else row
        return pl.ds(pl.multiple_of((d * 4 + r * 2 + c) * k_rows, k_rows), k_rows)

    def slot(place):
        return pl.ds(place * k_rows, k_rows)

    def cols(j):
        return pl.ds(pl.multiple_of(j * TN, TN), TN)

    def load_a(place):
        return pltpu.make_async_copy(a_ref.at[:, k_block(place, col)], a_own.at[:, slot(place)], ld_a.at[place])

    def load_b(j):
        return pltpu.make_async_copy(b_ref.at[:, cols(j)], b_buf.at[j, slot(0), :], ld_b.at[j])

    def load_first():
        return pltpu.make_async_copy(a_ref.at[pl.ds(0, half), k_block(0, 1 - col)], a_first, ld_f)

    pieces = [(0, half, p) for p in range(4)] + [(half, half, p) for p in range(3)]
    pieces += [(half, half - EXTRA, 3), (rows - EXTRA, EXTRA, 3)]
    last = len(pieces) - 1

    def send_a(i):
        start, size, place = pieces[i]
        return pltpu.make_async_remote_copy(
            src_ref=a_first if i == 0 else a_ref.at[pl.ds(start, size), k_block(place, 1 - col)],
            dst_ref=a_nbr.at[pl.ds(start, size), slot(place)],
            send_sem=a_snd_sem.at[i], recv_sem=a_rcv_sem.at[i], device_id=to_y, device_id_type=MESH)

    def hand_over():
        start, size, place = pieces[last]
        return pltpu.make_async_remote_copy(
            src_ref=a_ref.at[pl.ds(start, size), k_block(place, 1 - col)], dst_ref=a_fwd,
            send_sem=f_snd_sem, recv_sem=f_rcv_sem, device_id=to_d, device_id_type=MESH)

    def send_for_other():
        start, size, place = pieces[last]
        return pltpu.make_async_remote_copy(
            src_ref=a_fwd, dst_ref=a_nbr.at[pl.ds(start, size), slot(place)],
            send_sem=fwd_sem, recv_sem=a_rcv_sem.at[last],
            device_id={"col": 1 - col, "depth": 0}, device_id_type=MESH)

    def send_x(j):
        return pltpu.make_async_remote_copy(
            src_ref=b_ref.at[:, cols(j)], dst_ref=b_buf.at[j, slot(2), :],
            send_sem=x_snd_sem.at[j], recv_sem=x_rcv_sem.at[j], device_id=to_x, device_id_type=MESH)

    def send_d(j):
        return pltpu.make_async_remote_copy(
            src_ref=b_ref.at[:, cols(j)], dst_ref=b_buf.at[j, slot(1), :],
            send_sem=d_snd_sem.at[j], recv_sem=d_rcv_sem.at[j], device_id=to_d, device_id_type=MESH)

    def relay(j):
        return pltpu.make_async_remote_copy(
            src_ref=b_buf.at[j, slot(2), :], dst_ref=b_buf.at[j, slot(3), :],
            send_sem=r_snd_sem.at[j], recv_sem=r_rcv_sem.at[j], device_id=to_d, device_id_type=MESH)

    def send_c(j, h):
        return pltpu.make_async_remote_copy(
            src_ref=p_snd.at[j, pl.ds(h * half, half), :], dst_ref=p_rcv.at[j, pl.ds(h * half, half), :],
            send_sem=c_snd_sem.at[j, h], recv_sem=c_rcv_sem.at[j, h], device_id=to_y, device_id_type=MESH)

    load_first().start()

    barrier = pltpu.get_barrier_semaphore()
    for peer in (to_y, {"depth": 0, "row": lax.rem(row + 1 - depth, 2)}):
        pl.semaphore_signal(barrier, inc=1, device_id=peer, device_id_type=MESH)
    pl.semaphore_wait(barrier, 3 - 2 * depth)

    load_first().wait()
    for i in range(last):
        send_a(i).start()

    @pl.when(depth == 0)
    def _():
        hand_over().start()
        pl.semaphore_signal(pair_sem, inc=1, device_id=to_x, device_id_type=MESH)
        pl.semaphore_wait(pair_sem, 1)
        pl.semaphore_signal(core_sem, inc=1, device_id=to_d, device_id_type=MESH)

    @pl.when(depth == 1)
    def _():
        send_a(last).start()
        pl.semaphore_wait(core_sem, 1)

    @pl.loop(0, n_chunks)
    def _(j):
        send_x(j).start()

    for place in range(4):
        load_a(place).start()

    def bring(j):
        send_d(j).start()
        load_b(j).start()

    for j in range(AHEAD):
        bring(j)

    @pl.when(depth == 1)
    def _():
        hand_over().wait_recv()
        send_for_other().start()

    for place in range(4):
        load_a(place).wait()

    def part(j, h):
        p_snd[j, pl.ds(h * half, half), :] = jnp.dot(
            a_nbr[pl.ds(h * half, half), :], b_buf[j], preferred_element_type=jnp.float32)

    @pl.loop(0, n_chunks)
    def _(j):
        send_x(j).wait_recv()
        relay(j).start()

        @pl.when(j < n_chunks - AHEAD)
        def _():
            bring(j + AHEAD)

        load_b(j).wait()
        send_d(j).wait_recv()
        relay(j).wait_recv()

        @pl.when(j == 0)
        def _():
            for i in range(4):
                send_a(i).wait_recv()

        @pl.when(j == LAG)
        def _():
            for i in range(4, last + 1):
                send_a(i).wait_recv()

        part(j, 0)

        @pl.when(j >= LAG)
        def _():
            part(j - LAG, 1)

        p_own[j] = jnp.dot(a_own[...], b_buf[j], preferred_element_type=jnp.float32)
        send_c(j, 0).start()

        @pl.when(j >= LAG)
        def _():
            send_c(j - LAG, 1).start()

    @pl.loop(n_chunks - LAG, n_chunks)
    def _(j):
        part(j, 1)

    def finish(j):
        for h in range(2):
            send_c(j, h).wait_recv()
            piece = pl.ds(h * half, half)
            c_ref[piece, cols(j)] = (p_own[j, piece, :] + p_rcv[j, piece, :]).astype(c_ref.dtype)

    finish(0)
    for j in range(n_chunks - LAG, n_chunks):
        send_c(j, 1).start()

    @pl.loop(1, n_chunks - LAG)
    def _(j):
        finish(j)

    for i in range(last):
        send_a(i).wait_send()

    @pl.when(depth == 0)
    def _():
        hand_over().wait_send()

    @pl.when(depth == 1)
    def _():
        send_a(last).wait_send()
        send_for_other().wait_send()

    @pl.loop(0, n_chunks)
    def _(j):
        send_x(j).wait_send()
        send_d(j).wait_send()
        relay(j).wait_send()

    @pl.loop(0, n_chunks - LAG)
    def _(j):
        for h in range(2):
            send_c(j, h).wait_send()

    for j in range(n_chunks - LAG, n_chunks):
        finish(j)
    for j in range(n_chunks - LAG, n_chunks):
        for h in range(2):
            send_c(j, h).wait_send()


def put_out(c_ref, out_ref, sem):
    rows = c_ref.shape[0] // PARTS

    def copy(i):
        piece = pl.ds(i * rows, rows)
        return pltpu.make_async_copy(c_ref.at[piece], out_ref.at[piece], sem.at[i])

    for i in range(PARTS):
        copy(i).start()
    for i in range(PARTS):
        copy(i).wait()


def solution(mesh):
    all_axes = ("depth", "row", "col")

    def device_block(a_rows, b_rows):
        rows, depth = a_rows.shape
        k_rows, n = b_rows.shape
        k = 4 * k_rows
        n_chunks = n // TN
        dma = pltpu.SemaphoreType.DMA
        c = pl.pallas_call(
            kernel,
            out_shape=pltpu.VMEM((rows, n), jnp.bfloat16),
            in_specs=[pl.BlockSpec(memory_space=pl.ANY)] * 2,
            out_specs=pl.BlockSpec(memory_space=pltpu.VMEM),
            scratch_shapes=[
                pltpu.VMEM((n_chunks, k, TN), jnp.bfloat16),
                pltpu.VMEM((rows, k), jnp.bfloat16),
                pltpu.VMEM((rows, k), jnp.bfloat16),
                pltpu.VMEM((n_chunks, rows, TN), jnp.float32),
                pltpu.VMEM((n_chunks, rows, TN), jnp.float32),
                pltpu.VMEM((n_chunks, rows, TN), jnp.float32),
                pltpu.VMEM((rows // 2, k_rows), jnp.bfloat16),
                pltpu.VMEM((EXTRA, k_rows), jnp.bfloat16),
                dma, dma((4,)), dma((n_chunks,)),
                dma((9,)), dma((9,)),
                dma((n_chunks,)), dma((n_chunks,)),
                dma((n_chunks,)), dma((n_chunks,)),
                dma((n_chunks,)), dma((n_chunks,)),
                dma((n_chunks, 2)), dma((n_chunks, 2)),
                dma, dma, dma,
                pltpu.SemaphoreType.REGULAR, pltpu.SemaphoreType.REGULAR,
            ],
            compiler_params=pltpu.CompilerParams(
                collective_id=0, has_side_effects=True, vmem_limit_bytes=67043328 - 2 * rows * n),
        )(a_rows, b_rows)
        return pl.pallas_call(
            put_out,
            out_shape=jax.ShapeDtypeStruct((rows, n), jnp.bfloat16),
            in_specs=[pl.BlockSpec(memory_space=pltpu.VMEM)],
            out_specs=pl.BlockSpec(memory_space=pl.ANY),
            scratch_shapes=[dma((PARTS,))],
            compiler_params=pltpu.CompilerParams(vmem_limit_bytes=2 ** 20),
        )(pltpu.with_memory_space_constraint(c, pltpu.VMEM))

    return jax.shard_map(device_block, mesh=mesh, in_specs=(P(all_axes, None), P(all_axes, None)),
                         out_specs=P(all_axes, None), check_vma=False)
```

```python
import jax
import jax.numpy as jnp
from jax import lax
from jax.experimental import pallas as pl
from jax.experimental.pallas import tpu as pltpu
from jax.sharding import PartitionSpec as P

MESH = pl.DeviceIdType.MESH
TN = 512
LAG = 2
AHEAD = 2
ROUND = 16
EXTRA = 96


def kernel(a_ref, b_ref, c_ref, b_buf, a_own, a_nbr, p_own, p_snd, p_rcv, a_first, a_fwd,
           ld_f, ld_a, ld_b, a_snd_sem, a_rcv_sem, x_snd_sem, x_rcv_sem, d_snd_sem, d_rcv_sem,
           r_snd_sem, r_rcv_sem, c_snd_sem, c_rcv_sem, f_snd_sem, f_rcv_sem, fwd_sem,
           pair_sem, core_sem, round_buf, round_snd, round_rcv):
    depth, row, col = lax.axis_index("depth"), lax.axis_index("row"), lax.axis_index("col")
    to_y, to_x, to_d = {"col": 1 - col}, {"row": 1 - row}, {"depth": 1 - depth}
    rows, k_rows = a_ref.shape[0], b_ref.shape[0]
    half = rows // 2
    n_chunks = b_buf.shape[0]

    def k_block(place, c):
        d = 1 - depth if place % 2 else depth
        r = 1 - row if place // 2 else row
        return pl.ds(pl.multiple_of((d * 4 + r * 2 + c) * k_rows, k_rows), k_rows)

    def slot(place):
        return pl.ds(place * k_rows, k_rows)

    def cols(j):
        return pl.ds(pl.multiple_of(j * TN, TN), TN)

    def load_a(place):
        return pltpu.make_async_copy(a_ref.at[:, k_block(place, col)], a_own.at[:, slot(place)], ld_a.at[place])

    def load_b(j):
        return pltpu.make_async_copy(b_ref.at[:, cols(j)], b_buf.at[j, slot(0), :], ld_b.at[j])

    def load_first():
        return pltpu.make_async_copy(a_ref.at[pl.ds(0, half), k_block(0, 1 - col)], a_first, ld_f)

    pieces = [(0, half, p) for p in range(4)] + [(half, half, p) for p in range(3)]
    pieces += [(half, half - EXTRA, 3), (rows - EXTRA, EXTRA, 3)]
    last = len(pieces) - 1

    def send_a(i):
        start, size, place = pieces[i]
        return pltpu.make_async_remote_copy(
            src_ref=a_first if i == 0 else a_ref.at[pl.ds(start, size), k_block(place, 1 - col)],
            dst_ref=a_nbr.at[pl.ds(start, size), slot(place)],
            send_sem=a_snd_sem.at[i], recv_sem=a_rcv_sem.at[i], device_id=to_y, device_id_type=MESH)

    def hand_over():
        start, size, place = pieces[last]
        return pltpu.make_async_remote_copy(
            src_ref=a_ref.at[pl.ds(start, size), k_block(place, 1 - col)], dst_ref=a_fwd,
            send_sem=f_snd_sem, recv_sem=f_rcv_sem, device_id=to_d, device_id_type=MESH)

    def send_for_other():
        start, size, place = pieces[last]
        return pltpu.make_async_remote_copy(
            src_ref=a_fwd, dst_ref=a_nbr.at[pl.ds(start, size), slot(place)],
            send_sem=fwd_sem, recv_sem=a_rcv_sem.at[last],
            device_id={"col": 1 - col, "depth": 0}, device_id_type=MESH)

    def send_x(j):
        return pltpu.make_async_remote_copy(
            src_ref=b_ref.at[:, cols(j)], dst_ref=b_buf.at[j, slot(2), :],
            send_sem=x_snd_sem.at[j], recv_sem=x_rcv_sem.at[j], device_id=to_x, device_id_type=MESH)

    def send_d(j):
        return pltpu.make_async_remote_copy(
            src_ref=b_ref.at[:, cols(j)], dst_ref=b_buf.at[j, slot(1), :],
            send_sem=d_snd_sem.at[j], recv_sem=d_rcv_sem.at[j], device_id=to_d, device_id_type=MESH)

    def relay(j):
        return pltpu.make_async_remote_copy(
            src_ref=b_buf.at[j, slot(2), :], dst_ref=b_buf.at[j, slot(3), :],
            send_sem=r_snd_sem.at[j], recv_sem=r_rcv_sem.at[j], device_id=to_d, device_id_type=MESH)

    tail_rows = pl.ds(rows - ROUND, ROUND)
    source = (depth == 1) & (row == 0) & (col == 1)
    first_relay = (depth == 1) & (row == 1) & (col == 1)
    second_relay = (depth == 1) & (row == 1) & (col == 0)

    def send_tail():
        return pltpu.make_async_remote_copy(
            src_ref=p_snd.at[n_chunks - 1, tail_rows, :], dst_ref=p_rcv.at[n_chunks - 1, tail_rows, :],
            send_sem=round_snd.at[0], recv_sem=round_rcv.at[0], device_id=to_y, device_id_type=MESH)

    def go_round(step):
        src = p_snd.at[n_chunks - 1, tail_rows, :] if step == 0 else round_buf
        dst = p_rcv.at[n_chunks - 1, tail_rows, :] if step == 2 else round_buf
        return pltpu.make_async_remote_copy(
            src_ref=src, dst_ref=dst, send_sem=round_snd.at[1], recv_sem=round_rcv.at[0 if step == 2 else 1],
            device_id=to_y if step == 1 else to_x, device_id_type=MESH)

    def send_c(j, h):
        return pltpu.make_async_remote_copy(
            src_ref=p_snd.at[j, pl.ds(h * half, half), :], dst_ref=p_rcv.at[j, pl.ds(h * half, half), :],
            send_sem=c_snd_sem.at[j, h], recv_sem=c_rcv_sem.at[j, h], device_id=to_y, device_id_type=MESH)

    load_first().start()

    barrier = pltpu.get_barrier_semaphore()
    for peer in (to_y, {"depth": 0, "row": lax.rem(row + 1 - depth, 2)}):
        pl.semaphore_signal(barrier, inc=1, device_id=peer, device_id_type=MESH)
    pl.semaphore_wait(barrier, 3 - 2 * depth)

    load_first().wait()
    for i in range(last):
        send_a(i).start()

    @pl.when(depth == 0)
    def _():
        hand_over().start()
        pl.semaphore_signal(pair_sem, inc=1, device_id=to_x, device_id_type=MESH)
        pl.semaphore_wait(pair_sem, 1)
        pl.semaphore_signal(core_sem, inc=1, device_id=to_d, device_id_type=MESH)

    @pl.when(depth == 1)
    def _():
        send_a(last).start()
        pl.semaphore_wait(core_sem, 1)

    @pl.loop(0, n_chunks)
    def _(j):
        send_x(j).start()

    for place in range(4):
        load_a(place).start()

    def bring(j):
        send_d(j).start()
        load_b(j).start()

    for j in range(AHEAD):
        bring(j)

    @pl.when(depth == 1)
    def _():
        hand_over().wait_recv()
        send_for_other().start()

    for place in range(4):
        load_a(place).wait()

    def part(j, h):
        p_snd[j, pl.ds(h * half, half), :] = jnp.dot(
            a_nbr[pl.ds(h * half, half), :], b_buf[j], preferred_element_type=jnp.float32)

    @pl.loop(0, n_chunks)
    def _(j):
        send_x(j).wait_recv()
        relay(j).start()

        @pl.when(j < n_chunks - AHEAD)
        def _():
            bring(j + AHEAD)

        load_b(j).wait()
        send_d(j).wait_recv()
        relay(j).wait_recv()

        @pl.when(j == 0)
        def _():
            for i in range(4):
                send_a(i).wait_recv()

        @pl.when(j == LAG)
        def _():
            for i in range(4, last + 1):
                send_a(i).wait_recv()

        part(j, 0)

        @pl.when(j >= LAG)
        def _():
            part(j - LAG, 1)

        p_own[j] = jnp.dot(a_own[...], b_buf[j], preferred_element_type=jnp.float32)
        send_c(j, 0).start()

        @pl.when(j >= LAG)
        def _():
            send_c(j - LAG, 1).start()

    @pl.loop(n_chunks - LAG, n_chunks)
    def _(j):
        part(j, 1)

    def send_last():
        piece = pl.ds(half, half - ROUND)
        return pltpu.make_async_remote_copy(
            src_ref=p_snd.at[n_chunks - 1, piece, :], dst_ref=p_rcv.at[n_chunks - 1, piece, :],
            send_sem=c_snd_sem.at[n_chunks - 1, 1], recv_sem=c_rcv_sem.at[n_chunks - 1, 1],
            device_id=to_y, device_id_type=MESH)

    def add(j, piece):
        c_ref[piece, cols(j)] = (p_own[j, piece, :] + p_rcv[j, piece, :]).astype(c_ref.dtype)

    def finish(j):
        for h in range(2):
            send_c(j, h).wait_recv()
            add(j, pl.ds(h * half, half))

    finish(0)
    for j in range(n_chunks - LAG, n_chunks - 1):
        send_c(j, 1).start()

    @pl.when(source)
    def _():
        go_round(0).start()

    @pl.when(first_relay)
    def _():
        go_round(0).wait_recv()
        go_round(1).start()

    send_last().start()

    @pl.when(jnp.logical_not(source))
    def _():
        send_tail().start()

    @pl.loop(1, n_chunks - LAG)
    def _(j):
        finish(j)

    for i in range(last):
        send_a(i).wait_send()

    @pl.when(depth == 0)
    def _():
        hand_over().wait_send()

    @pl.when(depth == 1)
    def _():
        send_a(last).wait_send()
        send_for_other().wait_send()

    @pl.loop(0, n_chunks)
    def _(j):
        send_x(j).wait_send()
        send_d(j).wait_send()
        relay(j).wait_send()

    @pl.loop(0, n_chunks - LAG)
    def _(j):
        for h in range(2):
            send_c(j, h).wait_send()

    for j in range(n_chunks - LAG, n_chunks - 1):
        finish(j)
        for h in range(2):
            send_c(j, h).wait_send()

    @pl.when(second_relay)
    def _():
        go_round(1).wait_recv()
        go_round(2).start()

    send_c(n_chunks - 1, 0).wait_recv()
    add(n_chunks - 1, pl.ds(0, half))
    send_last().wait_recv()
    add(n_chunks - 1, pl.ds(half, half - ROUND))
    send_tail().wait_recv()
    add(n_chunks - 1, tail_rows)

    @pl.when(source | first_relay | second_relay)
    def _():
        go_round(0).wait_send()

    send_c(n_chunks - 1, 0).wait_send()
    send_last().wait_send()

    @pl.when(jnp.logical_not(source))
    def _():
        send_tail().wait_send()


def solution(mesh):
    all_axes = ("depth", "row", "col")

    def device_block(a_rows, b_rows):
        rows, depth = a_rows.shape
        k_rows, n = b_rows.shape
        k = 4 * k_rows
        n_chunks = n // TN
        dma = pltpu.SemaphoreType.DMA
        return pl.pallas_call(
            kernel,
            out_shape=pltpu.VMEM((rows, n), jnp.bfloat16),
            in_specs=[pl.BlockSpec(memory_space=pl.ANY)] * 2,
            out_specs=pl.BlockSpec(memory_space=pltpu.VMEM),
            scratch_shapes=[
                pltpu.VMEM((n_chunks, k, TN), jnp.bfloat16),
                pltpu.VMEM((rows, k), jnp.bfloat16),
                pltpu.VMEM((rows, k), jnp.bfloat16),
                pltpu.VMEM((n_chunks, rows, TN), jnp.float32),
                pltpu.VMEM((n_chunks, rows, TN), jnp.float32),
                pltpu.VMEM((n_chunks, rows, TN), jnp.float32),
                pltpu.VMEM((rows // 2, k_rows), jnp.bfloat16),
                pltpu.VMEM((EXTRA, k_rows), jnp.bfloat16),
                dma, dma((4,)), dma((n_chunks,)),
                dma((9,)), dma((9,)),
                dma((n_chunks,)), dma((n_chunks,)),
                dma((n_chunks,)), dma((n_chunks,)),
                dma((n_chunks,)), dma((n_chunks,)),
                dma((n_chunks, 2)), dma((n_chunks, 2)),
                dma, dma, dma,
                pltpu.SemaphoreType.REGULAR, pltpu.SemaphoreType.REGULAR,
                pltpu.VMEM((ROUND, TN), jnp.float32), dma((2,)), dma((2,)),
            ],
            compiler_params=pltpu.CompilerParams(
                collective_id=0, has_side_effects=True, vmem_limit_bytes=67043328 - 2 * rows * n),
        )(a_rows, b_rows)

    return jax.shard_map(device_block, mesh=mesh, in_specs=(P(all_axes, None), P(all_axes, None)),
                         out_specs=P(all_axes, None), check_vma=False)
```

```python
import jax
import jax.numpy as jnp
from jax import lax
from jax.experimental import pallas as pl
from jax.experimental.pallas import tpu as pltpu
from jax.sharding import PartitionSpec as P

MESH = pl.DeviceIdType.MESH
TN = 512
LAG = 2
AHEAD = 2
ROUND = 16
EXTRA = 96


def kernel(a_ref, b_ref, c_ref, b_buf, a_own, a_nbr, p_own, p_snd, p_rcv, a_first, a_fwd,
           ld_f, ld_a, ld_b, a_snd_sem, a_rcv_sem, x_snd_sem, x_rcv_sem, d_snd_sem, d_rcv_sem,
           r_snd_sem, r_rcv_sem, c_snd_sem, c_rcv_sem, f_snd_sem, f_rcv_sem, fwd_sem,
           pair_sem, core_sem, round_buf, round_snd, round_rcv):
    depth, row, col = lax.axis_index("depth"), lax.axis_index("row"), lax.axis_index("col")
    to_y, to_x, to_d = {"col": 1 - col}, {"row": 1 - row}, {"depth": 1 - depth}
    rows, k_rows = a_ref.shape[0], b_ref.shape[0]
    half = rows // 2
    n_chunks = b_buf.shape[0]

    def k_block(place, c):
        d = 1 - depth if place % 2 else depth
        r = 1 - row if place // 2 else row
        return pl.ds(pl.multiple_of((d * 4 + r * 2 + c) * k_rows, k_rows), k_rows)

    def slot(place):
        return pl.ds(place * k_rows, k_rows)

    def cols(j):
        return pl.ds(pl.multiple_of(j * TN, TN), TN)

    def load_a(place):
        return pltpu.make_async_copy(a_ref.at[:, k_block(place, col)], a_own.at[:, slot(place)], ld_a.at[place])

    def load_b(j):
        return pltpu.make_async_copy(b_ref.at[:, cols(j)], b_buf.at[j, slot(0), :], ld_b.at[j])

    def load_first():
        return pltpu.make_async_copy(a_ref.at[pl.ds(0, half), k_block(0, 1 - col)], a_first, ld_f)

    pieces = [(0, half, p) for p in range(4)] + [(half, half, p) for p in range(3)]
    pieces += [(half, half - EXTRA, 3), (rows - EXTRA, EXTRA, 3)]
    last = len(pieces) - 1

    def send_a(i):
        start, size, place = pieces[i]
        return pltpu.make_async_remote_copy(
            src_ref=a_first if i == 0 else a_ref.at[pl.ds(start, size), k_block(place, 1 - col)],
            dst_ref=a_nbr.at[pl.ds(start, size), slot(place)],
            send_sem=a_snd_sem.at[i], recv_sem=a_rcv_sem.at[i], device_id=to_y, device_id_type=MESH)

    def hand_over():
        start, size, place = pieces[last]
        return pltpu.make_async_remote_copy(
            src_ref=a_ref.at[pl.ds(start, size), k_block(place, 1 - col)], dst_ref=a_fwd,
            send_sem=f_snd_sem, recv_sem=f_rcv_sem, device_id=to_d, device_id_type=MESH)

    def send_for_other():
        start, size, place = pieces[last]
        return pltpu.make_async_remote_copy(
            src_ref=a_fwd, dst_ref=a_nbr.at[pl.ds(start, size), slot(place)],
            send_sem=fwd_sem, recv_sem=a_rcv_sem.at[last],
            device_id={"col": 1 - col, "depth": 0}, device_id_type=MESH)

    def send_x(j):
        return pltpu.make_async_remote_copy(
            src_ref=b_ref.at[:, cols(j)], dst_ref=b_buf.at[j, slot(2), :],
            send_sem=x_snd_sem.at[j], recv_sem=x_rcv_sem.at[j], device_id=to_x, device_id_type=MESH)

    def send_d(j):
        return pltpu.make_async_remote_copy(
            src_ref=b_ref.at[:, cols(j)], dst_ref=b_buf.at[j, slot(1), :],
            send_sem=d_snd_sem.at[j], recv_sem=d_rcv_sem.at[j], device_id=to_d, device_id_type=MESH)

    def relay(j):
        return pltpu.make_async_remote_copy(
            src_ref=b_buf.at[j, slot(2), :], dst_ref=b_buf.at[j, slot(3), :],
            send_sem=r_snd_sem.at[j], recv_sem=r_rcv_sem.at[j], device_id=to_d, device_id_type=MESH)

    tail_rows = pl.ds(rows - ROUND, ROUND)
    source = (depth == 1) & (row == 0) & (col == 1)
    first_relay = (depth == 1) & (row == 1) & (col == 1)
    second_relay = (depth == 1) & (row == 1) & (col == 0)

    def send_tail():
        return pltpu.make_async_remote_copy(
            src_ref=p_snd.at[n_chunks - 1, tail_rows, :], dst_ref=p_rcv.at[n_chunks - 1, tail_rows, :],
            send_sem=round_snd.at[0], recv_sem=round_rcv.at[0], device_id=to_y, device_id_type=MESH)

    def go_round(step):
        src = p_snd.at[n_chunks - 1, tail_rows, :] if step == 0 else round_buf
        dst = p_rcv.at[n_chunks - 1, tail_rows, :] if step == 2 else round_buf
        return pltpu.make_async_remote_copy(
            src_ref=src, dst_ref=dst, send_sem=round_snd.at[1], recv_sem=round_rcv.at[0 if step == 2 else 1],
            device_id=to_y if step == 1 else to_x, device_id_type=MESH)

    def send_c(j, h):
        return pltpu.make_async_remote_copy(
            src_ref=p_snd.at[j, pl.ds(h * half, half), :], dst_ref=p_rcv.at[j, pl.ds(h * half, half), :],
            send_sem=c_snd_sem.at[j, h], recv_sem=c_rcv_sem.at[j, h], device_id=to_y, device_id_type=MESH)

    load_first().start()

    barrier = pltpu.get_barrier_semaphore()
    for peer in (to_y, {"depth": 0, "row": lax.rem(row + 1 - depth, 2)}):
        pl.semaphore_signal(barrier, inc=1, device_id=peer, device_id_type=MESH)
    pl.semaphore_wait(barrier, 3 - 2 * depth)

    for i in range(1, 4):
        send_a(i).start()
    load_first().wait()
    send_a(0).start()
    for i in range(4, last):
        send_a(i).start()

    @pl.when(depth == 0)
    def _():
        hand_over().start()
        pl.semaphore_signal(pair_sem, inc=1, device_id=to_x, device_id_type=MESH)
        pl.semaphore_wait(pair_sem, 1)
        pl.semaphore_signal(core_sem, inc=1, device_id=to_d, device_id_type=MESH)

    @pl.when(depth == 1)
    def _():
        send_a(last).start()
        pl.semaphore_wait(core_sem, 1)

    @pl.loop(0, n_chunks)
    def _(j):
        send_x(j).start()

    for place in range(4):
        load_a(place).start()

    def bring(j):
        send_d(j).start()
        load_b(j).start()

    for j in range(AHEAD):
        bring(j)

    @pl.when(depth == 1)
    def _():
        hand_over().wait_recv()
        send_for_other().start()

    for place in range(4):
        load_a(place).wait()

    def part(j, h):
        p_snd[j, pl.ds(h * half, half), :] = jnp.dot(
            a_nbr[pl.ds(h * half, half), :], b_buf[j], preferred_element_type=jnp.float32)

    @pl.loop(0, n_chunks)
    def _(j):
        send_x(j).wait_recv()
        relay(j).start()

        @pl.when(j < n_chunks - AHEAD)
        def _():
            bring(j + AHEAD)

        load_b(j).wait()
        send_d(j).wait_recv()
        relay(j).wait_recv()

        @pl.when(j == 0)
        def _():
            for i in range(4):
                send_a(i).wait_recv()

        @pl.when(j == LAG)
        def _():
            for i in range(4, last + 1):
                send_a(i).wait_recv()

        part(j, 0)

        @pl.when(j >= LAG)
        def _():
            part(j - LAG, 1)

        p_own[j] = jnp.dot(a_own[...], b_buf[j], preferred_element_type=jnp.float32)
        send_c(j, 0).start()

        @pl.when(j >= LAG)
        def _():
            send_c(j - LAG, 1).start()

    @pl.loop(n_chunks - LAG, n_chunks)
    def _(j):
        part(j, 1)

    def send_last():
        piece = pl.ds(half, half - ROUND)
        return pltpu.make_async_remote_copy(
            src_ref=p_snd.at[n_chunks - 1, piece, :], dst_ref=p_rcv.at[n_chunks - 1, piece, :],
            send_sem=c_snd_sem.at[n_chunks - 1, 1], recv_sem=c_rcv_sem.at[n_chunks - 1, 1],
            device_id=to_y, device_id_type=MESH)

    def add(j, piece):
        c_ref[piece, cols(j)] = (p_own[j, piece, :] + p_rcv[j, piece, :]).astype(c_ref.dtype)

    def finish(j):
        for h in range(2):
            send_c(j, h).wait_recv()
            add(j, pl.ds(h * half, half))

    finish(0)
    for j in range(n_chunks - LAG, n_chunks - 1):
        send_c(j, 1).start()

    @pl.when(source)
    def _():
        go_round(0).start()

    @pl.when(first_relay)
    def _():
        go_round(0).wait_recv()
        go_round(1).start()

    send_last().start()

    @pl.when(jnp.logical_not(source))
    def _():
        send_tail().start()

    @pl.loop(1, n_chunks - LAG)
    def _(j):
        finish(j)

    for i in range(last):
        send_a(i).wait_send()

    @pl.when(depth == 0)
    def _():
        hand_over().wait_send()

    @pl.when(depth == 1)
    def _():
        send_a(last).wait_send()
        send_for_other().wait_send()

    @pl.loop(0, n_chunks)
    def _(j):
        send_x(j).wait_send()
        send_d(j).wait_send()
        relay(j).wait_send()

    @pl.loop(0, n_chunks - LAG)
    def _(j):
        for h in range(2):
            send_c(j, h).wait_send()

    for j in range(n_chunks - LAG, n_chunks - 1):
        finish(j)
        for h in range(2):
            send_c(j, h).wait_send()

    @pl.when(second_relay)
    def _():
        go_round(1).wait_recv()
        go_round(2).start()

    send_c(n_chunks - 1, 0).wait_recv()
    add(n_chunks - 1, pl.ds(0, half))
    send_last().wait_recv()
    add(n_chunks - 1, pl.ds(half, half - ROUND))
    send_tail().wait_recv()
    add(n_chunks - 1, tail_rows)

    @pl.when(source | first_relay | second_relay)
    def _():
        go_round(0).wait_send()

    send_c(n_chunks - 1, 0).wait_send()
    send_last().wait_send()

    @pl.when(jnp.logical_not(source))
    def _():
        send_tail().wait_send()


def solution(mesh):
    all_axes = ("depth", "row", "col")

    def device_block(a_rows, b_rows):
        rows, depth = a_rows.shape
        k_rows, n = b_rows.shape
        k = 4 * k_rows
        n_chunks = n // TN
        dma = pltpu.SemaphoreType.DMA
        return pl.pallas_call(
            kernel,
            out_shape=pltpu.VMEM((rows, n), jnp.bfloat16),
            in_specs=[pl.BlockSpec(memory_space=pl.ANY)] * 2,
            out_specs=pl.BlockSpec(memory_space=pltpu.VMEM),
            scratch_shapes=[
                pltpu.VMEM((n_chunks, k, TN), jnp.bfloat16),
                pltpu.VMEM((rows, k), jnp.bfloat16),
                pltpu.VMEM((rows, k), jnp.bfloat16),
                pltpu.VMEM((n_chunks, rows, TN), jnp.float32),
                pltpu.VMEM((n_chunks, rows, TN), jnp.float32),
                pltpu.VMEM((n_chunks, rows, TN), jnp.float32),
                pltpu.VMEM((rows // 2, k_rows), jnp.bfloat16),
                pltpu.VMEM((EXTRA, k_rows), jnp.bfloat16),
                dma, dma((4,)), dma((n_chunks,)),
                dma((9,)), dma((9,)),
                dma((n_chunks,)), dma((n_chunks,)),
                dma((n_chunks,)), dma((n_chunks,)),
                dma((n_chunks,)), dma((n_chunks,)),
                dma((n_chunks, 2)), dma((n_chunks, 2)),
                dma, dma, dma,
                pltpu.SemaphoreType.REGULAR, pltpu.SemaphoreType.REGULAR,
                pltpu.VMEM((ROUND, TN), jnp.float32), dma((2,)), dma((2,)),
            ],
            compiler_params=pltpu.CompilerParams(
                collective_id=0, has_side_effects=True, vmem_limit_bytes=67043328 - 2 * rows * n),
        )(a_rows, b_rows)

    return jax.shard_map(device_block, mesh=mesh, in_specs=(P(all_axes, None), P(all_axes, None)),
                         out_specs=P(all_axes, None), check_vma=False)
```

```python
import jax
import jax.numpy as jnp
from jax import lax
from jax.experimental import pallas as pl
from jax.experimental.pallas import tpu as pltpu
from jax.sharding import PartitionSpec as P

MESH = pl.DeviceIdType.MESH
TN = 512
LAG = 2
AHEAD = 2
ROUND = 16
EXTRA = 96


def kernel(a_ref, b_ref, c_ref, b_buf, a_own, a_nbr, p_own, p_snd, p_rcv, a_fwd,
           ld_a, ld_b, a_snd_sem, a_rcv_sem, x_snd_sem, x_rcv_sem, d_snd_sem, d_rcv_sem,
           r_snd_sem, r_rcv_sem, c_snd_sem, c_rcv_sem, f_snd_sem, f_rcv_sem, fwd_sem,
           pair_sem, core_sem, round_buf, round_snd, round_rcv):
    depth, row, col = lax.axis_index("depth"), lax.axis_index("row"), lax.axis_index("col")
    to_y, to_x, to_d = {"col": 1 - col}, {"row": 1 - row}, {"depth": 1 - depth}
    rows, k_rows = a_ref.shape[0], b_ref.shape[0]
    half = rows // 2
    n_chunks = b_buf.shape[0]

    def k_block(place, c):
        d = 1 - depth if place % 2 else depth
        r = 1 - row if place // 2 else row
        return pl.ds(pl.multiple_of((d * 4 + r * 2 + c) * k_rows, k_rows), k_rows)

    def slot(place):
        return pl.ds(place * k_rows, k_rows)

    def cols(j):
        return pl.ds(pl.multiple_of(j * TN, TN), TN)

    def load_a(place):
        return pltpu.make_async_copy(a_ref.at[:, k_block(place, col)], a_own.at[:, slot(place)], ld_a.at[place])

    def load_b(j):
        return pltpu.make_async_copy(b_ref.at[:, cols(j)], b_buf.at[j, slot(0), :], ld_b.at[j])

    pieces = [(0, half, p) for p in range(4)] + [(half, half, p) for p in range(3)]
    pieces += [(half, half - EXTRA, 3), (rows - EXTRA, EXTRA, 3)]
    last = len(pieces) - 1

    def send_a(i):
        start, size, place = pieces[i]
        return pltpu.make_async_remote_copy(
            src_ref=a_ref.at[pl.ds(start, size), k_block(place, 1 - col)],
            dst_ref=a_nbr.at[pl.ds(start, size), slot(place)],
            send_sem=a_snd_sem.at[i], recv_sem=a_rcv_sem.at[i], device_id=to_y, device_id_type=MESH)

    def hand_over():
        start, size, place = pieces[last]
        return pltpu.make_async_remote_copy(
            src_ref=a_ref.at[pl.ds(start, size), k_block(place, 1 - col)], dst_ref=a_fwd,
            send_sem=f_snd_sem, recv_sem=f_rcv_sem, device_id=to_d, device_id_type=MESH)

    def send_for_other():
        start, size, place = pieces[last]
        return pltpu.make_async_remote_copy(
            src_ref=a_fwd, dst_ref=a_nbr.at[pl.ds(start, size), slot(place)],
            send_sem=fwd_sem, recv_sem=a_rcv_sem.at[last],
            device_id={"col": 1 - col, "depth": 0}, device_id_type=MESH)

    def send_x(j):
        return pltpu.make_async_remote_copy(
            src_ref=b_ref.at[:, cols(j)], dst_ref=b_buf.at[j, slot(2), :],
            send_sem=x_snd_sem.at[j], recv_sem=x_rcv_sem.at[j], device_id=to_x, device_id_type=MESH)

    def send_d(j):
        return pltpu.make_async_remote_copy(
            src_ref=b_ref.at[:, cols(j)], dst_ref=b_buf.at[j, slot(1), :],
            send_sem=d_snd_sem.at[j], recv_sem=d_rcv_sem.at[j], device_id=to_d, device_id_type=MESH)

    def relay(j):
        return pltpu.make_async_remote_copy(
            src_ref=b_buf.at[j, slot(2), :], dst_ref=b_buf.at[j, slot(3), :],
            send_sem=r_snd_sem.at[j], recv_sem=r_rcv_sem.at[j], device_id=to_d, device_id_type=MESH)

    tail_rows = pl.ds(rows - ROUND, ROUND)
    source = (depth == 1) & (row == 0) & (col == 1)
    first_relay = (depth == 1) & (row == 1) & (col == 1)
    second_relay = (depth == 1) & (row == 1) & (col == 0)

    def send_tail():
        return pltpu.make_async_remote_copy(
            src_ref=p_snd.at[n_chunks - 1, tail_rows, :], dst_ref=p_rcv.at[n_chunks - 1, tail_rows, :],
            send_sem=round_snd.at[0], recv_sem=round_rcv.at[0], device_id=to_y, device_id_type=MESH)

    def go_round(step):
        src = p_snd.at[n_chunks - 1, tail_rows, :] if step == 0 else round_buf
        dst = p_rcv.at[n_chunks - 1, tail_rows, :] if step == 2 else round_buf
        return pltpu.make_async_remote_copy(
            src_ref=src, dst_ref=dst, send_sem=round_snd.at[1], recv_sem=round_rcv.at[0 if step == 2 else 1],
            device_id=to_y if step == 1 else to_x, device_id_type=MESH)

    def send_c(j, h):
        return pltpu.make_async_remote_copy(
            src_ref=p_snd.at[j, pl.ds(h * half, half), :], dst_ref=p_rcv.at[j, pl.ds(h * half, half), :],
            send_sem=c_snd_sem.at[j, h], recv_sem=c_rcv_sem.at[j, h], device_id=to_y, device_id_type=MESH)

    barrier = pltpu.get_barrier_semaphore()
    for peer in (to_y, {"depth": 0, "row": lax.rem(row + 1 - depth, 2)}):
        pl.semaphore_signal(barrier, inc=1, device_id=peer, device_id_type=MESH)
    pl.semaphore_wait(barrier, 3 - 2 * depth)

    for i in range(last):
        send_a(i).start()

    @pl.when(depth == 0)
    def _():
        hand_over().start()
        pl.semaphore_signal(pair_sem, inc=1, device_id=to_x, device_id_type=MESH)
        pl.semaphore_wait(pair_sem, 1)
        pl.semaphore_signal(core_sem, inc=1, device_id=to_d, device_id_type=MESH)

    @pl.when(depth == 1)
    def _():
        send_a(last).start()
        pl.semaphore_wait(core_sem, 1)

    @pl.loop(0, n_chunks)
    def _(j):
        send_x(j).start()

    for place in range(4):
        load_a(place).start()

    def bring(j):
        send_d(j).start()
        load_b(j).start()

    for j in range(AHEAD):
        bring(j)

    @pl.when(depth == 1)
    def _():
        hand_over().wait_recv()
        send_for_other().start()

    for place in range(4):
        load_a(place).wait()

    def part(j, h):
        p_snd[j, pl.ds(h * half, half), :] = jnp.dot(
            a_nbr[pl.ds(h * half, half), :], b_buf[j], preferred_element_type=jnp.float32)

    @pl.loop(0, n_chunks)
    def _(j):
        send_x(j).wait_recv()
        relay(j).start()

        @pl.when(j < n_chunks - AHEAD)
        def _():
            bring(j + AHEAD)

        load_b(j).wait()
        send_d(j).wait_recv()
        relay(j).wait_recv()

        @pl.when(j == 0)
        def _():
            for i in range(4):
                send_a(i).wait_recv()

        @pl.when(j == LAG)
        def _():
            for i in range(4, last + 1):
                send_a(i).wait_recv()

        part(j, 0)

        @pl.when(j >= LAG)
        def _():
            part(j - LAG, 1)

        p_own[j] = jnp.dot(a_own[...], b_buf[j], preferred_element_type=jnp.float32)
        send_c(j, 0).start()

        @pl.when(j >= LAG)
        def _():
            send_c(j - LAG, 1).start()

    @pl.loop(n_chunks - LAG, n_chunks)
    def _(j):
        part(j, 1)

    def send_last():
        piece = pl.ds(half, half - ROUND)
        return pltpu.make_async_remote_copy(
            src_ref=p_snd.at[n_chunks - 1, piece, :], dst_ref=p_rcv.at[n_chunks - 1, piece, :],
            send_sem=c_snd_sem.at[n_chunks - 1, 1], recv_sem=c_rcv_sem.at[n_chunks - 1, 1],
            device_id=to_y, device_id_type=MESH)

    def add(j, piece):
        c_ref[piece, cols(j)] = (p_own[j, piece, :] + p_rcv[j, piece, :]).astype(c_ref.dtype)

    def finish(j):
        for h in range(2):
            send_c(j, h).wait_recv()
            add(j, pl.ds(h * half, half))

    finish(0)
    for j in range(n_chunks - LAG, n_chunks - 1):
        send_c(j, 1).start()

    @pl.when(source)
    def _():
        go_round(0).start()

    @pl.when(first_relay)
    def _():
        go_round(0).wait_recv()
        go_round(1).start()

    send_last().start()

    @pl.when(jnp.logical_not(source))
    def _():
        send_tail().start()

    @pl.loop(1, n_chunks - LAG)
    def _(j):
        finish(j)

    for i in range(last):
        send_a(i).wait_send()

    @pl.when(depth == 0)
    def _():
        hand_over().wait_send()

    @pl.when(depth == 1)
    def _():
        send_a(last).wait_send()
        send_for_other().wait_send()

    @pl.loop(0, n_chunks)
    def _(j):
        send_x(j).wait_send()
        send_d(j).wait_send()
        relay(j).wait_send()

    @pl.loop(0, n_chunks - LAG)
    def _(j):
        for h in range(2):
            send_c(j, h).wait_send()

    for j in range(n_chunks - LAG, n_chunks - 1):
        finish(j)
        for h in range(2):
            send_c(j, h).wait_send()

    @pl.when(second_relay)
    def _():
        go_round(1).wait_recv()
        go_round(2).start()

    send_c(n_chunks - 1, 0).wait_recv()
    add(n_chunks - 1, pl.ds(0, half))
    send_last().wait_recv()
    add(n_chunks - 1, pl.ds(half, half - ROUND))
    send_tail().wait_recv()
    add(n_chunks - 1, tail_rows)

    @pl.when(source | first_relay | second_relay)
    def _():
        go_round(0).wait_send()

    send_c(n_chunks - 1, 0).wait_send()
    send_last().wait_send()

    @pl.when(jnp.logical_not(source))
    def _():
        send_tail().wait_send()


def solution(mesh):
    all_axes = ("depth", "row", "col")

    def device_block(a_rows, b_rows):
        rows, depth = a_rows.shape
        k_rows, n = b_rows.shape
        k = 4 * k_rows
        n_chunks = n // TN
        dma = pltpu.SemaphoreType.DMA
        return pl.pallas_call(
            kernel,
            out_shape=pltpu.VMEM((rows, n), jnp.bfloat16),
            in_specs=[pl.BlockSpec(memory_space=pl.ANY)] * 2,
            out_specs=pl.BlockSpec(memory_space=pltpu.VMEM),
            scratch_shapes=[
                pltpu.VMEM((n_chunks, k, TN), jnp.bfloat16),
                pltpu.VMEM((rows, k), jnp.bfloat16),
                pltpu.VMEM((rows, k), jnp.bfloat16),
                pltpu.VMEM((n_chunks, rows, TN), jnp.float32),
                pltpu.VMEM((n_chunks, rows, TN), jnp.float32),
                pltpu.VMEM((n_chunks, rows, TN), jnp.float32),
                pltpu.VMEM((EXTRA, k_rows), jnp.bfloat16),
                dma((4,)), dma((n_chunks,)),
                dma((9,)), dma((9,)),
                dma((n_chunks,)), dma((n_chunks,)),
                dma((n_chunks,)), dma((n_chunks,)),
                dma((n_chunks,)), dma((n_chunks,)),
                dma((n_chunks, 2)), dma((n_chunks, 2)),
                dma, dma, dma,
                pltpu.SemaphoreType.REGULAR, pltpu.SemaphoreType.REGULAR,
                pltpu.VMEM((ROUND, TN), jnp.float32), dma((2,)), dma((2,)),
            ],
            compiler_params=pltpu.CompilerParams(
                collective_id=0, has_side_effects=True, vmem_limit_bytes=67043328 - 2 * rows * n),
        )(a_rows, b_rows)

    return jax.shard_map(device_block, mesh=mesh, in_specs=(P(all_axes, None), P(all_axes, None)),
                         out_specs=P(all_axes, None), check_vma=False)
```

```python
import jax
import jax.numpy as jnp
from jax import lax
from jax.experimental import pallas as pl
from jax.experimental.pallas import tpu as pltpu
from jax.sharding import PartitionSpec as P

MESH = pl.DeviceIdType.MESH
TN = 512
LAG = 2
AHEAD = 2
ROUND = 16
EXTRA = 112


def kernel(a_ref, b_ref, c_ref, b_buf, a_own, a_nbr, p_own, p_snd, p_rcv, a_fwd,
           ld_a, ld_b, a_snd_sem, a_rcv_sem, x_snd_sem, x_rcv_sem, d_snd_sem, d_rcv_sem,
           r_snd_sem, r_rcv_sem, c_snd_sem, c_rcv_sem, f_snd_sem, f_rcv_sem, fwd_sem,
           pair_sem, core_sem, round_buf, round_snd, round_rcv):
    depth, row, col = lax.axis_index("depth"), lax.axis_index("row"), lax.axis_index("col")
    to_y, to_x, to_d = {"col": 1 - col}, {"row": 1 - row}, {"depth": 1 - depth}
    rows, k_rows = a_ref.shape[0], b_ref.shape[0]
    half = rows // 2
    n_chunks = b_buf.shape[0]

    def k_block(place, c):
        d = 1 - depth if place % 2 else depth
        r = 1 - row if place // 2 else row
        return pl.ds(pl.multiple_of((d * 4 + r * 2 + c) * k_rows, k_rows), k_rows)

    def slot(place):
        return pl.ds(place * k_rows, k_rows)

    def cols(j):
        return pl.ds(pl.multiple_of(j * TN, TN), TN)

    def load_a(place):
        return pltpu.make_async_copy(a_ref.at[:, k_block(place, col)], a_own.at[:, slot(place)], ld_a.at[place])

    def load_b(j):
        return pltpu.make_async_copy(b_ref.at[:, cols(j)], b_buf.at[j, slot(0), :], ld_b.at[j])

    pieces = [(0, half, p) for p in range(4)] + [(half, half, p) for p in range(3)]
    pieces += [(half, half - EXTRA, 3), (rows - EXTRA, EXTRA, 3)]
    last = len(pieces) - 1

    def send_a(i):
        start, size, place = pieces[i]
        return pltpu.make_async_remote_copy(
            src_ref=a_ref.at[pl.ds(start, size), k_block(place, 1 - col)],
            dst_ref=a_nbr.at[pl.ds(start, size), slot(place)],
            send_sem=a_snd_sem.at[i], recv_sem=a_rcv_sem.at[i], device_id=to_y, device_id_type=MESH)

    def hand_over():
        start, size, place = pieces[last]
        return pltpu.make_async_remote_copy(
            src_ref=a_ref.at[pl.ds(start, size), k_block(place, 1 - col)], dst_ref=a_fwd,
            send_sem=f_snd_sem, recv_sem=f_rcv_sem, device_id=to_d, device_id_type=MESH)

    def send_for_other():
        start, size, place = pieces[last]
        return pltpu.make_async_remote_copy(
            src_ref=a_fwd, dst_ref=a_nbr.at[pl.ds(start, size), slot(place)],
            send_sem=fwd_sem, recv_sem=a_rcv_sem.at[last],
            device_id={"col": 1 - col, "depth": 0}, device_id_type=MESH)

    def send_x(j):
        return pltpu.make_async_remote_copy(
            src_ref=b_ref.at[:, cols(j)], dst_ref=b_buf.at[j, slot(2), :],
            send_sem=x_snd_sem.at[j], recv_sem=x_rcv_sem.at[j], device_id=to_x, device_id_type=MESH)

    def send_d(j):
        return pltpu.make_async_remote_copy(
            src_ref=b_ref.at[:, cols(j)], dst_ref=b_buf.at[j, slot(1), :],
            send_sem=d_snd_sem.at[j], recv_sem=d_rcv_sem.at[j], device_id=to_d, device_id_type=MESH)

    def relay(j):
        return pltpu.make_async_remote_copy(
            src_ref=b_buf.at[j, slot(2), :], dst_ref=b_buf.at[j, slot(3), :],
            send_sem=r_snd_sem.at[j], recv_sem=r_rcv_sem.at[j], device_id=to_d, device_id_type=MESH)

    tail_rows = pl.ds(rows - ROUND, ROUND)
    source = (depth == 1) & (row == 0) & (col == 1)
    first_relay = (depth == 1) & (row == 1) & (col == 1)
    second_relay = (depth == 1) & (row == 1) & (col == 0)

    def send_tail():
        return pltpu.make_async_remote_copy(
            src_ref=p_snd.at[n_chunks - 1, tail_rows, :], dst_ref=p_rcv.at[n_chunks - 1, tail_rows, :],
            send_sem=round_snd.at[0], recv_sem=round_rcv.at[0], device_id=to_y, device_id_type=MESH)

    def go_round(step):
        src = p_snd.at[n_chunks - 1, tail_rows, :] if step == 0 else round_buf
        dst = p_rcv.at[n_chunks - 1, tail_rows, :] if step == 2 else round_buf
        return pltpu.make_async_remote_copy(
            src_ref=src, dst_ref=dst, send_sem=round_snd.at[1], recv_sem=round_rcv.at[0 if step == 2 else 1],
            device_id=to_y if step == 1 else to_x, device_id_type=MESH)

    def send_c(j, h):
        return pltpu.make_async_remote_copy(
            src_ref=p_snd.at[j, pl.ds(h * half, half), :], dst_ref=p_rcv.at[j, pl.ds(h * half, half), :],
            send_sem=c_snd_sem.at[j, h], recv_sem=c_rcv_sem.at[j, h], device_id=to_y, device_id_type=MESH)

    barrier = pltpu.get_barrier_semaphore()
    for peer in (to_y, {"depth": 0, "row": lax.rem(row + 1 - depth, 2)}):
        pl.semaphore_signal(barrier, inc=1, device_id=peer, device_id_type=MESH)
    pl.semaphore_wait(barrier, 3 - 2 * depth)

    for i in range(last):
        send_a(i).start()

    @pl.when(depth == 0)
    def _():
        hand_over().start()
        pl.semaphore_signal(pair_sem, inc=1, device_id=to_x, device_id_type=MESH)
        pl.semaphore_wait(pair_sem, 1)
        pl.semaphore_signal(core_sem, inc=1, device_id=to_d, device_id_type=MESH)

    @pl.when(depth == 1)
    def _():
        send_a(last).start()
        pl.semaphore_wait(core_sem, 1)

    @pl.loop(0, n_chunks)
    def _(j):
        send_x(j).start()

    for place in range(4):
        load_a(place).start()

    def bring(j):
        send_d(j).start()
        load_b(j).start()

    for j in range(AHEAD):
        bring(j)

    @pl.when(depth == 1)
    def _():
        hand_over().wait_recv()
        send_for_other().start()

    for place in range(4):
        load_a(place).wait()

    def part(j, h):
        p_snd[j, pl.ds(h * half, half), :] = jnp.dot(
            a_nbr[pl.ds(h * half, half), :], b_buf[j], preferred_element_type=jnp.float32)

    @pl.loop(0, n_chunks)
    def _(j):
        send_x(j).wait_recv()
        relay(j).start()

        @pl.when(j < n_chunks - AHEAD)
        def _():
            bring(j + AHEAD)

        load_b(j).wait()
        send_d(j).wait_recv()
        relay(j).wait_recv()

        @pl.when(j == 0)
        def _():
            for i in range(4):
                send_a(i).wait_recv()

        @pl.when(j == LAG)
        def _():
            for i in range(4, last + 1):
                send_a(i).wait_recv()

        part(j, 0)

        @pl.when(j >= LAG)
        def _():
            part(j - LAG, 1)

        p_own[j] = jnp.dot(a_own[...], b_buf[j], preferred_element_type=jnp.float32)
        send_c(j, 0).start()

        @pl.when(j >= LAG)
        def _():
            send_c(j - LAG, 1).start()

    @pl.loop(n_chunks - LAG, n_chunks)
    def _(j):
        part(j, 1)

    def send_last():
        piece = pl.ds(half, half - ROUND)
        return pltpu.make_async_remote_copy(
            src_ref=p_snd.at[n_chunks - 1, piece, :], dst_ref=p_rcv.at[n_chunks - 1, piece, :],
            send_sem=c_snd_sem.at[n_chunks - 1, 1], recv_sem=c_rcv_sem.at[n_chunks - 1, 1],
            device_id=to_y, device_id_type=MESH)

    def add(j, piece):
        c_ref[piece, cols(j)] = (p_own[j, piece, :] + p_rcv[j, piece, :]).astype(c_ref.dtype)

    def finish(j):
        for h in range(2):
            send_c(j, h).wait_recv()
            add(j, pl.ds(h * half, half))

    finish(0)
    for j in range(n_chunks - LAG, n_chunks - 1):
        send_c(j, 1).start()

    @pl.when(source)
    def _():
        go_round(0).start()

    @pl.when(first_relay)
    def _():
        go_round(0).wait_recv()
        go_round(1).start()

    send_last().start()

    @pl.when(jnp.logical_not(source))
    def _():
        send_tail().start()

    @pl.loop(1, n_chunks - LAG)
    def _(j):
        finish(j)

    for i in range(last):
        send_a(i).wait_send()

    @pl.when(depth == 0)
    def _():
        hand_over().wait_send()

    @pl.when(depth == 1)
    def _():
        send_a(last).wait_send()
        send_for_other().wait_send()

    @pl.loop(0, n_chunks)
    def _(j):
        send_x(j).wait_send()
        send_d(j).wait_send()
        relay(j).wait_send()

    @pl.loop(0, n_chunks - LAG)
    def _(j):
        for h in range(2):
            send_c(j, h).wait_send()

    for j in range(n_chunks - LAG, n_chunks - 1):
        finish(j)
        for h in range(2):
            send_c(j, h).wait_send()

    @pl.when(second_relay)
    def _():
        go_round(1).wait_recv()
        go_round(2).start()

    send_c(n_chunks - 1, 0).wait_recv()
    add(n_chunks - 1, pl.ds(0, half))
    send_last().wait_recv()
    add(n_chunks - 1, pl.ds(half, half - ROUND))
    send_tail().wait_recv()
    add(n_chunks - 1, tail_rows)

    @pl.when(source | first_relay | second_relay)
    def _():
        go_round(0).wait_send()

    send_c(n_chunks - 1, 0).wait_send()
    send_last().wait_send()

    @pl.when(jnp.logical_not(source))
    def _():
        send_tail().wait_send()


def solution(mesh):
    all_axes = ("depth", "row", "col")

    def device_block(a_rows, b_rows):
        rows, depth = a_rows.shape
        k_rows, n = b_rows.shape
        k = 4 * k_rows
        n_chunks = n // TN
        dma = pltpu.SemaphoreType.DMA
        return pl.pallas_call(
            kernel,
            out_shape=pltpu.VMEM((rows, n), jnp.bfloat16),
            in_specs=[pl.BlockSpec(memory_space=pl.ANY)] * 2,
            out_specs=pl.BlockSpec(memory_space=pltpu.VMEM),
            scratch_shapes=[
                pltpu.VMEM((n_chunks, k, TN), jnp.bfloat16),
                pltpu.VMEM((rows, k), jnp.bfloat16),
                pltpu.VMEM((rows, k), jnp.bfloat16),
                pltpu.VMEM((n_chunks, rows, TN), jnp.float32),
                pltpu.VMEM((n_chunks, rows, TN), jnp.float32),
                pltpu.VMEM((n_chunks, rows, TN), jnp.float32),
                pltpu.VMEM((EXTRA, k_rows), jnp.bfloat16),
                dma((4,)), dma((n_chunks,)),
                dma((9,)), dma((9,)),
                dma((n_chunks,)), dma((n_chunks,)),
                dma((n_chunks,)), dma((n_chunks,)),
                dma((n_chunks,)), dma((n_chunks,)),
                dma((n_chunks, 2)), dma((n_chunks, 2)),
                dma, dma, dma,
                pltpu.SemaphoreType.REGULAR, pltpu.SemaphoreType.REGULAR,
                pltpu.VMEM((ROUND, TN), jnp.float32), dma((2,)), dma((2,)),
            ],
            compiler_params=pltpu.CompilerParams(
                collective_id=0, has_side_effects=True, vmem_limit_bytes=67043328 - 2 * rows * n),
        )(a_rows, b_rows)

    return jax.shard_map(device_block, mesh=mesh, in_specs=(P(all_axes, None), P(all_axes, None)),
                         out_specs=P(all_axes, None), check_vma=False)
```

```python
import jax
import jax.numpy as jnp
from jax import lax
from jax.experimental import pallas as pl
from jax.experimental.pallas import tpu as pltpu
from jax.sharding import PartitionSpec as P

MESH = pl.DeviceIdType.MESH
TN = 512
LAG = 2
AHEAD = 2
ROUND = 16
EXTRA = 112


def kernel(a_ref, b_ref, c_ref, own_ref, nbr_ref, b_buf, a_own, a_nbr, p_own, p_snd, p_rcv, a_fwd,
           ld_a, ld_b, a_snd_sem, a_rcv_sem, x_snd_sem, x_rcv_sem, d_snd_sem, d_rcv_sem,
           r_snd_sem, r_rcv_sem, c_snd_sem, c_rcv_sem, f_snd_sem, f_rcv_sem, fwd_sem,
           pair_sem, core_sem, round_buf, round_snd, round_rcv):
    depth, row, col = lax.axis_index("depth"), lax.axis_index("row"), lax.axis_index("col")
    to_y, to_x, to_d = {"col": 1 - col}, {"row": 1 - row}, {"depth": 1 - depth}
    rows, k_rows = a_ref.shape[0], b_ref.shape[0]
    half = rows // 2
    n_chunks, n_here = b_buf.shape[0], p_own.shape[0]

    def k_block(place, c):
        d = 1 - depth if place % 2 else depth
        r = 1 - row if place // 2 else row
        return pl.ds(pl.multiple_of((d * 4 + r * 2 + c) * k_rows, k_rows), k_rows)

    def slot(place):
        return pl.ds(place * k_rows, k_rows)

    def cols(j):
        return pl.ds(pl.multiple_of(j * TN, TN), TN)

    def load_a(place):
        return pltpu.make_async_copy(a_ref.at[:, k_block(place, col)], a_own.at[:, slot(place)], ld_a.at[place])

    def load_b(j):
        return pltpu.make_async_copy(b_ref.at[:, cols(j)], b_buf.at[j, slot(0), :], ld_b.at[j])

    pieces = [(0, half, p) for p in range(4)] + [(half, half, p) for p in range(2)]
    pieces += [(half, half - EXTRA, p) for p in (2, 3)] + [(rows - EXTRA, EXTRA, p) for p in (2, 3)]
    last = len(pieces) - 2

    def send_a(i):
        start, size, place = pieces[i]
        return pltpu.make_async_remote_copy(
            src_ref=a_ref.at[pl.ds(start, size), k_block(place, 1 - col)],
            dst_ref=a_nbr.at[pl.ds(start, size), slot(place)],
            send_sem=a_snd_sem.at[i], recv_sem=a_rcv_sem.at[i], device_id=to_y, device_id_type=MESH)

    def hand_over(i):
        start, size, place = pieces[last + i]
        return pltpu.make_async_remote_copy(
            src_ref=a_ref.at[pl.ds(start, size), k_block(place, 1 - col)], dst_ref=a_fwd.at[i],
            send_sem=f_snd_sem.at[i], recv_sem=f_rcv_sem.at[i], device_id=to_d, device_id_type=MESH)

    def send_for_other(i):
        start, size, place = pieces[last + i]
        return pltpu.make_async_remote_copy(
            src_ref=a_fwd.at[i], dst_ref=a_nbr.at[pl.ds(start, size), slot(place)],
            send_sem=fwd_sem.at[i], recv_sem=a_rcv_sem.at[last + i],
            device_id={"col": 1 - col, "depth": 0}, device_id_type=MESH)

    def send_x(j):
        return pltpu.make_async_remote_copy(
            src_ref=b_ref.at[:, cols(j)], dst_ref=b_buf.at[j, slot(2), :],
            send_sem=x_snd_sem.at[j], recv_sem=x_rcv_sem.at[j], device_id=to_x, device_id_type=MESH)

    def send_d(j):
        return pltpu.make_async_remote_copy(
            src_ref=b_ref.at[:, cols(j)], dst_ref=b_buf.at[j, slot(1), :],
            send_sem=d_snd_sem.at[j], recv_sem=d_rcv_sem.at[j], device_id=to_d, device_id_type=MESH)

    def relay(j):
        return pltpu.make_async_remote_copy(
            src_ref=b_buf.at[j, slot(2), :], dst_ref=b_buf.at[j, slot(3), :],
            send_sem=r_snd_sem.at[j], recv_sem=r_rcv_sem.at[j], device_id=to_d, device_id_type=MESH)

    tail_rows = pl.ds(rows - ROUND, ROUND)
    source = (depth == 1) & (row == 0) & (col == 1)
    first_relay = (depth == 1) & (row == 1) & (col == 1)
    second_relay = (depth == 1) & (row == 1) & (col == 0)

    def send_tail():
        return pltpu.make_async_remote_copy(
            src_ref=p_snd.at[n_here - 1, tail_rows, :], dst_ref=p_rcv.at[n_here - 1, tail_rows, :],
            send_sem=round_snd.at[0], recv_sem=round_rcv.at[0], device_id=to_y, device_id_type=MESH)

    def go_round(step):
        src = p_snd.at[n_here - 1, tail_rows, :] if step == 0 else round_buf
        dst = p_rcv.at[n_here - 1, tail_rows, :] if step == 2 else round_buf
        return pltpu.make_async_remote_copy(
            src_ref=src, dst_ref=dst, send_sem=round_snd.at[1], recv_sem=round_rcv.at[0 if step == 2 else 1],
            device_id=to_y if step == 1 else to_x, device_id_type=MESH)

    def send_c(j, h):
        return pltpu.make_async_remote_copy(
            src_ref=p_snd.at[j, pl.ds(h * half, half), :], dst_ref=p_rcv.at[j, pl.ds(h * half, half), :],
            send_sem=c_snd_sem.at[j, h], recv_sem=c_rcv_sem.at[j, h], device_id=to_y, device_id_type=MESH)

    barrier = pltpu.get_barrier_semaphore()
    for peer in (to_y, {"depth": 0, "row": lax.rem(row + 1 - depth, 2)}):
        pl.semaphore_signal(barrier, inc=1, device_id=peer, device_id_type=MESH)
    pl.semaphore_wait(barrier, 3 - 2 * depth)

    for i in range(last):
        send_a(i).start()

    @pl.when(depth == 0)
    def _():
        for i in range(2):
            hand_over(i).start()
        pl.semaphore_signal(pair_sem, inc=1, device_id=to_x, device_id_type=MESH)
        pl.semaphore_wait(pair_sem, 1)
        pl.semaphore_signal(core_sem, inc=1, device_id=to_d, device_id_type=MESH)

    @pl.when(depth == 1)
    def _():
        for i in range(2):
            send_a(last + i).start()
        pl.semaphore_wait(core_sem, 1)

    @pl.loop(0, n_chunks)
    def _(j):
        send_x(j).start()

    for place in range(4):
        load_a(place).start()

    def bring(j):
        send_d(j).start()
        load_b(j).start()

    for j in range(AHEAD):
        bring(j)

    @pl.when(depth == 1)
    def _():
        for i in range(2):
            hand_over(i).wait_recv()
            send_for_other(i).start()

    for place in range(4):
        load_a(place).wait()

    def part(j, h):
        p_snd[j, pl.ds(h * half, half), :] = jnp.dot(
            a_nbr[pl.ds(h * half, half), :], b_buf[j], preferred_element_type=jnp.float32)

    def gather(j):
        send_x(j).wait_recv()
        relay(j).start()

        @pl.when(j < n_chunks - AHEAD)
        def _():
            bring(j + AHEAD)

        load_b(j).wait()
        send_d(j).wait_recv()
        relay(j).wait_recv()

    @pl.loop(0, n_here)
    def _(j):
        gather(j)

        @pl.when(j == 0)
        def _():
            for i in range(4):
                send_a(i).wait_recv()

        @pl.when(j == LAG)
        def _():
            for i in range(4, last + 2):
                send_a(i).wait_recv()

        part(j, 0)

        @pl.when(j >= LAG)
        def _():
            part(j - LAG, 1)

        p_own[j] = jnp.dot(a_own[...], b_buf[j], preferred_element_type=jnp.float32)
        send_c(j, 0).start()

        @pl.when(j >= LAG)
        def _():
            send_c(j - LAG, 1).start()

    @pl.loop(n_here - LAG, n_here)
    def _(j):
        part(j, 1)

    def send_last():
        piece = pl.ds(half, half - ROUND)
        return pltpu.make_async_remote_copy(
            src_ref=p_snd.at[n_here - 1, piece, :], dst_ref=p_rcv.at[n_here - 1, piece, :],
            send_sem=c_snd_sem.at[n_here - 1, 1], recv_sem=c_rcv_sem.at[n_here - 1, 1],
            device_id=to_y, device_id_type=MESH)

    def add(j, piece):
        c_ref[piece, cols(j)] = (p_own[j, piece, :] + p_rcv[j, piece, :]).astype(c_ref.dtype)

    def finish(j):
        for h in range(2):
            send_c(j, h).wait_recv()
            add(j, pl.ds(h * half, half))

    finish(0)
    for j in range(n_here - LAG, n_here - 1):
        send_c(j, 1).start()

    @pl.when(source)
    def _():
        go_round(0).start()

    @pl.when(first_relay)
    def _():
        go_round(0).wait_recv()
        go_round(1).start()

    send_last().start()

    @pl.when(jnp.logical_not(source))
    def _():
        send_tail().start()

    gather(n_chunks - 1)
    nbr_ref[...] = jnp.dot(a_nbr[...], b_buf[n_chunks - 1], preferred_element_type=jnp.float32)
    own_ref[...] = jnp.dot(a_own[...], b_buf[n_chunks - 1], preferred_element_type=jnp.float32)

    @pl.loop(1, n_here - LAG)
    def _(j):
        finish(j)

    for i in range(last):
        send_a(i).wait_send()

    @pl.when(depth == 0)
    def _():
        for i in range(2):
            hand_over(i).wait_send()

    @pl.when(depth == 1)
    def _():
        for i in range(2):
            send_a(last + i).wait_send()
            send_for_other(i).wait_send()

    @pl.loop(0, n_chunks)
    def _(j):
        send_x(j).wait_send()
        send_d(j).wait_send()
        relay(j).wait_send()

    @pl.loop(0, n_here - LAG)
    def _(j):
        for h in range(2):
            send_c(j, h).wait_send()

    for j in range(n_here - LAG, n_here - 1):
        finish(j)
        for h in range(2):
            send_c(j, h).wait_send()

    @pl.when(second_relay)
    def _():
        go_round(1).wait_recv()
        go_round(2).start()

    send_c(n_here - 1, 0).wait_recv()
    add(n_here - 1, pl.ds(0, half))
    send_last().wait_recv()
    add(n_here - 1, pl.ds(half, half - ROUND))
    send_tail().wait_recv()
    add(n_here - 1, tail_rows)

    @pl.when(source | first_relay | second_relay)
    def _():
        go_round(0).wait_send()

    send_c(n_here - 1, 0).wait_send()
    send_last().wait_send()

    @pl.when(jnp.logical_not(source))
    def _():
        send_tail().wait_send()


def last_kernel(own_ref, nbr_ref, out_ref, c_ref, rcv, snd_sem, rcv_sem):
    to_y = {"col": 1 - lax.axis_index("col")}
    half = own_ref.shape[0] // 2

    def send(h):
        piece = pl.ds(h * half, half)
        return pltpu.make_async_remote_copy(
            src_ref=nbr_ref.at[piece], dst_ref=rcv.at[piece], send_sem=snd_sem.at[h], recv_sem=rcv_sem.at[h],
            device_id=to_y, device_id_type=MESH)

    barrier = pltpu.get_barrier_semaphore()
    pl.semaphore_signal(barrier, inc=1, device_id=to_y, device_id_type=MESH)
    pl.semaphore_wait(barrier, 1)
    for h in range(2):
        send(h).start()
    for h in range(2):
        piece = pl.ds(h * half, half)
        send(h).wait_recv()
        c_ref[piece, :] = (own_ref[piece, :] + rcv[piece, :]).astype(c_ref.dtype)
    for h in range(2):
        send(h).wait_send()


def write_first(c_ref, out_ref, sem):
    copy = pltpu.make_async_copy(c_ref, out_ref.at[:, pl.ds(0, c_ref.shape[1])], sem)
    copy.start()
    copy.wait()


def write_last(whole_ref, c_ref, out_ref, sem):
    start = out_ref.shape[1] - c_ref.shape[1]
    copy = pltpu.make_async_copy(c_ref, out_ref.at[:, pl.ds(start, c_ref.shape[1])], sem)
    copy.start()
    copy.wait()


def solution(mesh):
    all_axes = ("depth", "row", "col")

    def device_block(a_rows, b_rows):
        rows, depth = a_rows.shape
        k_rows, n = b_rows.shape
        k = 4 * k_rows
        n_chunks = n // TN
        dma = pltpu.SemaphoreType.DMA
        n_here = n_chunks - 1
        f32 = jnp.float32
        vmem, any_space = pl.BlockSpec(memory_space=pltpu.VMEM), pl.BlockSpec(memory_space=pl.ANY)
        kept = 2 * rows * n_here * TN + 8 * rows * TN
        regular = pltpu.SemaphoreType.REGULAR
        c, own, nbr = pl.pallas_call(
            kernel,
            out_shape=(pltpu.VMEM((rows, n_here * TN), jnp.bfloat16),
                       pltpu.VMEM((rows, TN), f32), pltpu.VMEM((rows, TN), f32)),
            in_specs=[any_space] * 2,
            out_specs=(vmem,) * 3,
            scratch_shapes=[
                pltpu.VMEM((n_chunks, k, TN), jnp.bfloat16),
                pltpu.VMEM((rows, k), jnp.bfloat16),
                pltpu.VMEM((rows, k), jnp.bfloat16),
                pltpu.VMEM((n_here, rows, TN), f32),
                pltpu.VMEM((n_here, rows, TN), f32),
                pltpu.VMEM((n_here, rows, TN), f32),
                pltpu.VMEM((2, EXTRA, k_rows), jnp.bfloat16),
                dma((4,)), dma((n_chunks,)),
                dma((10,)), dma((10,)),
                dma((n_chunks,)), dma((n_chunks,)),
                dma((n_chunks,)), dma((n_chunks,)),
                dma((n_chunks,)), dma((n_chunks,)),
                dma((n_here, 2)), dma((n_here, 2)),
                dma((2,)), dma((2,)), dma((2,)),
                regular, regular,
                pltpu.VMEM((ROUND, TN), f32), dma((2,)), dma((2,)),
            ],
            compiler_params=pltpu.CompilerParams(
                collective_id=0, has_side_effects=True, vmem_limit_bytes=67043328 - kept),
        )(a_rows, b_rows)
        in_vmem = lambda x: pltpu.with_memory_space_constraint(x, pltpu.VMEM)
        small = pltpu.CompilerParams(vmem_limit_bytes=2 ** 20)
        whole = jax.ShapeDtypeStruct((rows, n), jnp.bfloat16)
        out = pl.pallas_call(
            write_first, out_shape=whole, in_specs=[vmem], out_specs=any_space,
            scratch_shapes=[dma], compiler_params=small)(in_vmem(c))
        c_last = pl.pallas_call(
            last_kernel,
            out_shape=pltpu.VMEM((rows, TN), jnp.bfloat16),
            in_specs=[vmem, vmem, pl.BlockSpec(memory_space=pltpu.HBM)],
            out_specs=vmem,
            scratch_shapes=[pltpu.VMEM((rows, TN), f32), dma((2,)), dma((2,))],
            compiler_params=pltpu.CompilerParams(
                collective_id=1, has_side_effects=True, vmem_limit_bytes=2 ** 23),
        )(in_vmem(own), in_vmem(nbr), pltpu.with_memory_space_constraint(out, pltpu.HBM))
        return pl.pallas_call(
            write_last, out_shape=whole, in_specs=[any_space, vmem], out_specs=any_space,
            scratch_shapes=[dma], input_output_aliases={0: 0}, compiler_params=small)(out, in_vmem(c_last))

    return jax.shard_map(device_block, mesh=mesh, in_specs=(P(all_axes, None), P(all_axes, None)),
                         out_specs=P(all_axes, None), check_vma=False)
```

```python
import jax
import jax.numpy as jnp
from jax import lax
from jax.experimental import pallas as pl
from jax.experimental.pallas import tpu as pltpu
from jax.sharding import PartitionSpec as P

MESH = pl.DeviceIdType.MESH
TN = 512
LAG = 2
AHEAD = 2
ROUND = 16
ROUND_N = 384
EXTRA = 80
EARLY = 256


def kernel(a_ref, b_ref, c_ref, own_ref, nbr_ref, b_buf, a_own, a_nbr, p_own, p_snd, p_rcv, a_fwd,
           ld_a, ld_b, a_snd_sem, a_rcv_sem, b_snd_sem, b_rcv_sem, d_snd_sem, d_rcv_sem,
           r_snd_sem, r_rcv_sem, c_snd_sem, c_rcv_sem, f_snd_sem, f_rcv_sem, fwd_sem,
           pair_sem, core_sem, round_buf, round_snd, round_rcv, early_rcv, early_sem):
    depth, row, col = lax.axis_index("depth"), lax.axis_index("row"), lax.axis_index("col")
    to_x, to_y, to_d = {"row": 1 - row}, {"col": 1 - col}, {"depth": 1 - depth}
    rows, k_rows = a_ref.shape[0], b_ref.shape[0]
    half = rows // 2
    n_chunks, n_here = b_buf.shape[0], p_own.shape[0]

    def k_block(place, r):
        d = 1 - depth if place % 2 else depth
        c = 1 - col if place // 2 else col
        return pl.ds(pl.multiple_of((d * 4 + r * 2 + c) * k_rows, k_rows), k_rows)

    def slot(place):
        return pl.ds(place * k_rows, k_rows)

    def cols(j):
        return pl.ds(pl.multiple_of(j * TN, TN), TN)

    def load_a(place):
        return pltpu.make_async_copy(a_ref.at[:, k_block(place, row)], a_own.at[:, slot(place)], ld_a.at[place])

    def load_b(j):
        return pltpu.make_async_copy(b_ref.at[:, cols(j)], b_buf.at[j, slot(0), :], ld_b.at[j])

    pieces = [(0, half, p) for p in range(4)] + [(half, half, p) for p in range(2)]
    pieces += [(half, half - EXTRA, p) for p in (2, 3)] + [(rows - EXTRA, EXTRA, p) for p in (2, 3)]
    last = len(pieces) - 2

    def send_a(i):
        start, size, place = pieces[i]
        return pltpu.make_async_remote_copy(
            src_ref=a_ref.at[pl.ds(start, size), k_block(place, 1 - row)],
            dst_ref=a_nbr.at[pl.ds(start, size), slot(place)],
            send_sem=a_snd_sem.at[i], recv_sem=a_rcv_sem.at[i], device_id=to_x, device_id_type=MESH)

    def hand_over(i):
        start, size, place = pieces[last + i]
        return pltpu.make_async_remote_copy(
            src_ref=a_ref.at[pl.ds(start, size), k_block(place, 1 - row)], dst_ref=a_fwd.at[i],
            send_sem=f_snd_sem.at[i], recv_sem=f_rcv_sem.at[i], device_id=to_d, device_id_type=MESH)

    def send_for_other(i):
        start, size, place = pieces[last + i]
        return pltpu.make_async_remote_copy(
            src_ref=a_fwd.at[i], dst_ref=a_nbr.at[pl.ds(start, size), slot(place)],
            send_sem=fwd_sem.at[i], recv_sem=a_rcv_sem.at[last + i],
            device_id={"row": 1 - row, "depth": 0}, device_id_type=MESH)

    def send_b(j):
        return pltpu.make_async_remote_copy(
            src_ref=b_ref.at[:, cols(j)], dst_ref=b_buf.at[j, slot(2), :],
            send_sem=b_snd_sem.at[j], recv_sem=b_rcv_sem.at[j], device_id=to_y, device_id_type=MESH)

    def send_d(j):
        return pltpu.make_async_remote_copy(
            src_ref=b_ref.at[:, cols(j)], dst_ref=b_buf.at[j, slot(1), :],
            send_sem=d_snd_sem.at[j], recv_sem=d_rcv_sem.at[j], device_id=to_d, device_id_type=MESH)

    def relay(j):
        return pltpu.make_async_remote_copy(
            src_ref=b_buf.at[j, slot(2), :], dst_ref=b_buf.at[j, slot(3), :],
            send_sem=r_snd_sem.at[j], recv_sem=r_rcv_sem.at[j], device_id=to_d, device_id_type=MESH)

    tail_rows = pl.ds(rows - ROUND, ROUND)
    source = (depth == 1) & (row == 1) & (col == 0)
    first_relay = (depth == 1) & (row == 1) & (col == 1)
    second_relay = (depth == 1) & (row == 0) & (col == 1)

    def send_tail():
        return pltpu.make_async_remote_copy(
            src_ref=p_snd.at[n_here - 1, tail_rows, pl.ds(0, ROUND_N)], dst_ref=p_rcv.at[n_here - 1, tail_rows, pl.ds(0, ROUND_N)],
            send_sem=round_snd.at[0], recv_sem=round_rcv.at[0], device_id=to_x, device_id_type=MESH)

    def send_rest():
        rest = pl.ds(ROUND_N, TN - ROUND_N)
        return pltpu.make_async_remote_copy(
            src_ref=p_snd.at[n_here - 1, tail_rows, rest], dst_ref=p_rcv.at[n_here - 1, tail_rows, rest],
            send_sem=round_snd.at[2], recv_sem=round_rcv.at[2], device_id=to_x, device_id_type=MESH)

    early = pl.ds(0, EARLY)

    def send_early():
        return pltpu.make_async_remote_copy(
            src_ref=nbr_ref.at[early], dst_ref=early_rcv, send_sem=early_sem.at[0], recv_sem=early_sem.at[1],
            device_id=to_x, device_id_type=MESH)

    def go_round(step):
        src = p_snd.at[n_here - 1, tail_rows, pl.ds(0, ROUND_N)] if step == 0 else round_buf
        dst = p_rcv.at[n_here - 1, tail_rows, pl.ds(0, ROUND_N)] if step == 2 else round_buf
        return pltpu.make_async_remote_copy(
            src_ref=src, dst_ref=dst, send_sem=round_snd.at[1], recv_sem=round_rcv.at[0 if step == 2 else 1],
            device_id=to_x if step == 1 else to_y, device_id_type=MESH)

    def send_c(j, h):
        return pltpu.make_async_remote_copy(
            src_ref=p_snd.at[j, pl.ds(h * half, half), :], dst_ref=p_rcv.at[j, pl.ds(h * half, half), :],
            send_sem=c_snd_sem.at[j, h], recv_sem=c_rcv_sem.at[j, h], device_id=to_x, device_id_type=MESH)

    barrier = pltpu.get_barrier_semaphore()
    for peer in (to_x, {"depth": 0, "col": lax.rem(col + 1 - depth, 2)}):
        pl.semaphore_signal(barrier, inc=1, device_id=peer, device_id_type=MESH)
    pl.semaphore_wait(barrier, 3 - 2 * depth)

    for i in range(4):
        send_a(i).start()

    @pl.when(depth == 0)
    def _():
        for i in range(4, last):
            send_a(i).start()
        for i in range(2):
            hand_over(i).start()
        pl.semaphore_signal(pair_sem, inc=1, device_id=to_y, device_id_type=MESH)
        pl.semaphore_wait(pair_sem, 1)
        pl.semaphore_signal(core_sem, inc=1, device_id=to_d, device_id_type=MESH)

    @pl.when(depth == 1)
    def _():
        pl.semaphore_wait(core_sem, 1)

    @pl.loop(0, n_chunks)
    def _(j):
        send_b(j).start()

    for place in range(4):
        load_a(place).start()

    def bring(j):
        send_d(j).start()
        load_b(j).start()

    for j in range(AHEAD):
        bring(j)

    @pl.when(depth == 1)
    def _():
        for i in range(2):
            hand_over(i).wait_recv()
            send_for_other(i).start()
        for i in range(4, last + 2):
            send_a(i).start()

    for place in range(4):
        load_a(place).wait()

    def part(j, h):
        p_snd[j, pl.ds(h * half, half), :] = jnp.dot(
            a_nbr[pl.ds(h * half, half), :], b_buf[j], preferred_element_type=jnp.float32)

    def gather(j):
        send_b(j).wait_recv()
        relay(j).start()

        @pl.when(j < n_chunks - AHEAD)
        def _():
            bring(j + AHEAD)

        load_b(j).wait()
        send_d(j).wait_recv()
        relay(j).wait_recv()

    @pl.loop(0, n_here)
    def _(j):
        gather(j)

        @pl.when(j == 0)
        def _():
            for i in range(4):
                send_a(i).wait_recv()

        @pl.when(j == LAG)
        def _():
            for i in range(4, last + 2):
                send_a(i).wait_recv()

        part(j, 0)

        @pl.when(j >= LAG)
        def _():
            part(j - LAG, 1)
            send_c(j, 0).start()

        p_own[j] = jnp.dot(a_own[...], b_buf[j], preferred_element_type=jnp.float32)

        @pl.when(j < LAG)
        def _():
            send_c(j, 0).start()

        @pl.when(j >= LAG)
        def _():
            send_c(j - LAG, 1).start()

    @pl.loop(n_here - LAG, n_here)
    def _(j):
        part(j, 1)

    def send_last():
        piece = pl.ds(half, half - ROUND)
        return pltpu.make_async_remote_copy(
            src_ref=p_snd.at[n_here - 1, piece, :], dst_ref=p_rcv.at[n_here - 1, piece, :],
            send_sem=c_snd_sem.at[n_here - 1, 1], recv_sem=c_rcv_sem.at[n_here - 1, 1],
            device_id=to_x, device_id_type=MESH)

    def add(j, piece):
        c_ref[piece, cols(j)] = (p_own[j, piece, :] + p_rcv[j, piece, :]).astype(c_ref.dtype)

    def finish(j):
        for h in range(2):
            send_c(j, h).wait_recv()
            add(j, pl.ds(h * half, half))

    finish(0)
    for j in range(n_here - LAG, n_here - 1):
        send_c(j, 1).start()

    @pl.when(source)
    def _():
        go_round(0).start()

    @pl.when(first_relay)
    def _():
        go_round(0).wait_recv()
        go_round(1).start()

    send_rest().start()
    send_last().start()

    @pl.when(jnp.logical_not(source))
    def _():
        send_tail().start()

    gather(n_chunks - 1)
    nbr_ref[...] = jnp.dot(a_nbr[...], b_buf[n_chunks - 1], preferred_element_type=jnp.float32)
    own_ref[...] = jnp.dot(a_own[...], b_buf[n_chunks - 1], preferred_element_type=jnp.float32)

    @pl.when(depth == 1)
    def _():
        send_early().start()

    @pl.loop(1, n_here - LAG)
    def _(j):
        finish(j)

    for i in range(last):
        send_a(i).wait_send()

    @pl.when(depth == 0)
    def _():
        for i in range(2):
            hand_over(i).wait_send()

    @pl.when(depth == 1)
    def _():
        for i in range(2):
            send_a(last + i).wait_send()
            send_for_other(i).wait_send()

    @pl.loop(0, n_chunks)
    def _(j):
        send_b(j).wait_send()
        send_d(j).wait_send()
        relay(j).wait_send()

    @pl.loop(0, n_here - LAG)
    def _(j):
        for h in range(2):
            send_c(j, h).wait_send()

    for j in range(n_here - LAG, n_here - 1):
        finish(j)
        for h in range(2):
            send_c(j, h).wait_send()

    @pl.when(second_relay)
    def _():
        go_round(1).wait_recv()
        go_round(2).start()

    send_c(n_here - 1, 0).wait_recv()
    add(n_here - 1, pl.ds(0, half))
    send_last().wait_recv()
    add(n_here - 1, pl.ds(half, half - ROUND))
    send_rest().wait_recv()
    send_tail().wait_recv()
    add(n_here - 1, tail_rows)

    @pl.when(source | first_relay | second_relay)
    def _():
        go_round(0).wait_send()

    @pl.when(depth == 1)
    def _():
        send_early().wait_recv()
        c_ref[early, cols(n_chunks - 1)] = (own_ref[early, :] + early_rcv[...]).astype(c_ref.dtype)
        send_early().wait_send()

    send_c(n_here - 1, 0).wait_send()
    send_last().wait_send()
    send_rest().wait_send()

    @pl.when(jnp.logical_not(source))
    def _():
        send_tail().wait_send()


def last_kernel(own_ref, nbr_ref, out_ref, c_ref, rcv, snd_sem, rcv_sem):
    to_x = {"row": 1 - lax.axis_index("row")}
    depth = lax.axis_index("depth")
    rows = own_ref.shape[0]
    pieces = [pl.ds(0, EARLY), pl.ds(EARLY, rows - EARLY)]

    def send(i):
        return pltpu.make_async_remote_copy(
            src_ref=nbr_ref.at[pieces[i]], dst_ref=rcv.at[pieces[i]], send_sem=snd_sem.at[i], recv_sem=rcv_sem.at[i],
            device_id=to_x, device_id_type=MESH)

    def add(i):
        c_ref[pieces[i], :] = (own_ref[pieces[i], :] + rcv[pieces[i], :]).astype(c_ref.dtype)

    barrier = pltpu.get_barrier_semaphore()
    pl.semaphore_signal(barrier, inc=1, device_id=to_x, device_id_type=MESH)
    pl.semaphore_wait(barrier, 1)

    @pl.when(depth == 0)
    def _():
        send(0).start()

    send(1).start()

    @pl.when(depth == 0)
    def _():
        send(0).wait_recv()
        add(0)

    send(1).wait_recv()
    add(1)

    @pl.when(depth == 0)
    def _():
        send(0).wait_send()

    send(1).wait_send()


def write_first(c_ref, out_ref, sem):
    depth = lax.axis_index("depth")
    n, tail = c_ref.shape[1] - TN, pl.ds(c_ref.shape[1] - TN, TN)
    early = pl.ds(0, EARLY)
    copy = pltpu.make_async_copy(c_ref.at[:, pl.ds(0, n)], out_ref.at[:, pl.ds(0, n)], sem.at[0])
    more = pltpu.make_async_copy(c_ref.at[early, tail], out_ref.at[early, tail], sem.at[1])
    copy.start()

    @pl.when(depth == 1)
    def _():
        more.start()
        more.wait()

    copy.wait()


def write_last(whole_ref, c_ref, out_ref, sem):
    depth = lax.axis_index("depth")
    tail = pl.ds(out_ref.shape[1] - TN, TN)
    early, late = pl.ds(0, EARLY), pl.ds(EARLY, c_ref.shape[0] - EARLY)
    copy = pltpu.make_async_copy(c_ref.at[late], out_ref.at[late, tail], sem.at[0])
    more = pltpu.make_async_copy(c_ref.at[early], out_ref.at[early, tail], sem.at[1])
    copy.start()

    @pl.when(depth == 0)
    def _():
        more.start()
        more.wait()

    copy.wait()


def solution(mesh):
    all_axes = ("depth", "row", "col")

    def device_block(a_rows, b_rows):
        rows, depth = a_rows.shape
        k_rows, n = b_rows.shape
        k = 4 * k_rows
        n_chunks = n // TN
        dma = pltpu.SemaphoreType.DMA
        n_here = n_chunks - 1
        f32 = jnp.float32
        vmem, any_space = pl.BlockSpec(memory_space=pltpu.VMEM), pl.BlockSpec(memory_space=pl.ANY)
        kept = 2 * rows * n + 8 * rows * TN
        regular = pltpu.SemaphoreType.REGULAR
        c, own, nbr = pl.pallas_call(
            kernel,
            out_shape=(pltpu.VMEM((rows, n), jnp.bfloat16),
                       pltpu.VMEM((rows, TN), f32), pltpu.VMEM((rows, TN), f32)),
            in_specs=[any_space] * 2,
            out_specs=(vmem,) * 3,
            scratch_shapes=[
                pltpu.VMEM((n_chunks, k, TN), jnp.bfloat16),
                pltpu.VMEM((rows, k), jnp.bfloat16),
                pltpu.VMEM((rows, k), jnp.bfloat16),
                pltpu.VMEM((n_here, rows, TN), f32),
                pltpu.VMEM((n_here, rows, TN), f32),
                pltpu.VMEM((n_here, rows, TN), f32),
                pltpu.VMEM((2, EXTRA, k_rows), jnp.bfloat16),
                dma((4,)), dma((n_chunks,)),
                dma((10,)), dma((10,)),
                dma((n_chunks,)), dma((n_chunks,)),
                dma((n_chunks,)), dma((n_chunks,)),
                dma((n_chunks,)), dma((n_chunks,)),
                dma((n_here, 2)), dma((n_here, 2)),
                dma((2,)), dma((2,)), dma((2,)),
                regular, regular,
                pltpu.VMEM((ROUND, ROUND_N), f32), dma((3,)), dma((3,)),
                pltpu.VMEM((EARLY, TN), f32), dma((2,)),
            ],
            compiler_params=pltpu.CompilerParams(
                collective_id=0, has_side_effects=True, vmem_limit_bytes=67043328 - kept),
        )(a_rows, b_rows)
        in_vmem = lambda x: pltpu.with_memory_space_constraint(x, pltpu.VMEM)
        small = pltpu.CompilerParams(vmem_limit_bytes=2 ** 20)
        whole = jax.ShapeDtypeStruct((rows, n), jnp.bfloat16)
        out = pl.pallas_call(
            write_first, out_shape=whole, in_specs=[vmem], out_specs=any_space,
            scratch_shapes=[dma((2,))], compiler_params=small)(in_vmem(c))
        c_last = pl.pallas_call(
            last_kernel,
            out_shape=pltpu.VMEM((rows, TN), jnp.bfloat16),
            in_specs=[vmem, vmem, pl.BlockSpec(memory_space=pltpu.HBM)],
            out_specs=vmem,
            scratch_shapes=[pltpu.VMEM((rows, TN), f32), dma((2,)), dma((2,))],
            compiler_params=pltpu.CompilerParams(
                collective_id=1, has_side_effects=True, vmem_limit_bytes=2 ** 23),
        )(in_vmem(own), in_vmem(nbr), pltpu.with_memory_space_constraint(out, pltpu.HBM))
        return pl.pallas_call(
            write_last, out_shape=whole, in_specs=[any_space, vmem], out_specs=any_space,
            scratch_shapes=[dma((2,))], input_output_aliases={0: 0}, compiler_params=small)(out, in_vmem(c_last))

    return jax.shard_map(device_block, mesh=mesh, in_specs=(P(all_axes, None), P(all_axes, None)),
                         out_specs=P(all_axes, None), check_vma=False)
```

```python
import jax
import jax.numpy as jnp
from jax import lax
from jax.experimental import pallas as pl
from jax.experimental.pallas import tpu as pltpu
from jax.sharding import PartitionSpec as P

MESH = pl.DeviceIdType.MESH
TN = 512
LAG = 2
AHEAD = 2
ROUND = 16
ROUND_N = 384
EXTRA = 64
EARLY = 256


def kernel(a_ref, b_ref, c_ref, own_ref, nbr_ref, b_buf, a_own, a_nbr, p_own, p_snd, p_rcv, a_fwd,
           ld_a, ld_b, a_snd_sem, a_rcv_sem, b_snd_sem, b_rcv_sem, d_snd_sem, d_rcv_sem,
           r_snd_sem, r_rcv_sem, c_snd_sem, c_rcv_sem, f_snd_sem, f_rcv_sem, fwd_sem,
           pair_sem, core_sem, round_buf, round_snd, round_rcv, early_rcv, early_sem):
    depth, row, col = lax.axis_index("depth"), lax.axis_index("row"), lax.axis_index("col")
    to_x, to_y, to_d = {"row": 1 - row}, {"col": 1 - col}, {"depth": 1 - depth}
    rows, k_rows = a_ref.shape[0], b_ref.shape[0]
    half = rows // 2
    n_chunks, n_here = b_buf.shape[0], p_own.shape[0]

    def k_block(place, r):
        d = 1 - depth if place % 2 else depth
        c = 1 - col if place // 2 else col
        return pl.ds(pl.multiple_of((d * 4 + r * 2 + c) * k_rows, k_rows), k_rows)

    def slot(place):
        return pl.ds(place * k_rows, k_rows)

    def cols(j):
        return pl.ds(pl.multiple_of(j * TN, TN), TN)

    def load_a(place):
        return pltpu.make_async_copy(a_ref.at[:, k_block(place, row)], a_own.at[:, slot(place)], ld_a.at[place])

    def load_b(j):
        return pltpu.make_async_copy(b_ref.at[:, cols(j)], b_buf.at[j, slot(0), :], ld_b.at[j])

    pieces = [(0, half, p) for p in range(4)] + [(half, half, p) for p in range(2)]
    pieces += [(half, half - EXTRA, p) for p in (2, 3)] + [(rows - EXTRA, EXTRA, p) for p in (2, 3)]
    last = len(pieces) - 2

    def send_a(i):
        start, size, place = pieces[i]
        return pltpu.make_async_remote_copy(
            src_ref=a_ref.at[pl.ds(start, size), k_block(place, 1 - row)],
            dst_ref=a_nbr.at[pl.ds(start, size), slot(place)],
            send_sem=a_snd_sem.at[i], recv_sem=a_rcv_sem.at[i], device_id=to_x, device_id_type=MESH)

    def hand_over(i):
        start, size, place = pieces[last + i]
        return pltpu.make_async_remote_copy(
            src_ref=a_ref.at[pl.ds(start, size), k_block(place, 1 - row)], dst_ref=a_fwd.at[i],
            send_sem=f_snd_sem.at[i], recv_sem=f_rcv_sem.at[i], device_id=to_d, device_id_type=MESH)

    def send_for_other(i):
        start, size, place = pieces[last + i]
        return pltpu.make_async_remote_copy(
            src_ref=a_fwd.at[i], dst_ref=a_nbr.at[pl.ds(start, size), slot(place)],
            send_sem=fwd_sem.at[i], recv_sem=a_rcv_sem.at[last + i],
            device_id={"row": 1 - row, "depth": 0}, device_id_type=MESH)

    def send_b(j):
        return pltpu.make_async_remote_copy(
            src_ref=b_ref.at[:, cols(j)], dst_ref=b_buf.at[j, slot(2), :],
            send_sem=b_snd_sem.at[j], recv_sem=b_rcv_sem.at[j], device_id=to_y, device_id_type=MESH)

    def send_d(j):
        return pltpu.make_async_remote_copy(
            src_ref=b_ref.at[:, cols(j)], dst_ref=b_buf.at[j, slot(1), :],
            send_sem=d_snd_sem.at[j], recv_sem=d_rcv_sem.at[j], device_id=to_d, device_id_type=MESH)

    def relay(j):
        return pltpu.make_async_remote_copy(
            src_ref=b_buf.at[j, slot(2), :], dst_ref=b_buf.at[j, slot(3), :],
            send_sem=r_snd_sem.at[j], recv_sem=r_rcv_sem.at[j], device_id=to_d, device_id_type=MESH)

    tail_rows = pl.ds(rows - ROUND, ROUND)
    source = (depth == 1) & (row == 1) & (col == 0)
    first_relay = (depth == 1) & (row == 1) & (col == 1)
    second_relay = (depth == 1) & (row == 0) & (col == 1)

    def send_tail():
        return pltpu.make_async_remote_copy(
            src_ref=p_snd.at[n_here - 1, tail_rows, pl.ds(0, ROUND_N)], dst_ref=p_rcv.at[n_here - 1, tail_rows, pl.ds(0, ROUND_N)],
            send_sem=round_snd.at[0], recv_sem=round_rcv.at[0], device_id=to_x, device_id_type=MESH)

    def send_rest():
        rest = pl.ds(ROUND_N, TN - ROUND_N)
        return pltpu.make_async_remote_copy(
            src_ref=p_snd.at[n_here - 1, tail_rows, rest], dst_ref=p_rcv.at[n_here - 1, tail_rows, rest],
            send_sem=round_snd.at[2], recv_sem=round_rcv.at[2], device_id=to_x, device_id_type=MESH)

    early = pl.ds(0, EARLY)

    def send_early():
        return pltpu.make_async_remote_copy(
            src_ref=nbr_ref.at[early], dst_ref=early_rcv, send_sem=early_sem.at[0], recv_sem=early_sem.at[1],
            device_id=to_x, device_id_type=MESH)

    def go_round(step):
        src = p_snd.at[n_here - 1, tail_rows, pl.ds(0, ROUND_N)] if step == 0 else round_buf
        dst = p_rcv.at[n_here - 1, tail_rows, pl.ds(0, ROUND_N)] if step == 2 else round_buf
        return pltpu.make_async_remote_copy(
            src_ref=src, dst_ref=dst, send_sem=round_snd.at[1], recv_sem=round_rcv.at[0 if step == 2 else 1],
            device_id=to_x if step == 1 else to_y, device_id_type=MESH)

    def send_c(j, h):
        return pltpu.make_async_remote_copy(
            src_ref=p_snd.at[j, pl.ds(h * half, half), :], dst_ref=p_rcv.at[j, pl.ds(h * half, half), :],
            send_sem=c_snd_sem.at[j, h], recv_sem=c_rcv_sem.at[j, h], device_id=to_x, device_id_type=MESH)

    barrier = pltpu.get_barrier_semaphore()
    for peer in (to_x, {"depth": 0, "col": lax.rem(col + 1 - depth, 2)}):
        pl.semaphore_signal(barrier, inc=1, device_id=peer, device_id_type=MESH)
    pl.semaphore_wait(barrier, 3 - 2 * depth)

    for i in range(4):
        send_a(i).start()

    @pl.when(depth == 0)
    def _():
        for i in range(4, last):
            send_a(i).start()
        for i in range(2):
            hand_over(i).start()
        pl.semaphore_signal(pair_sem, inc=1, device_id=to_y, device_id_type=MESH)
        pl.semaphore_wait(pair_sem, 1)
        pl.semaphore_signal(core_sem, inc=1, device_id=to_d, device_id_type=MESH)

    @pl.when(depth == 1)
    def _():
        pl.semaphore_wait(core_sem, 1)

    @pl.loop(0, n_chunks)
    def _(j):
        send_b(j).start()

    for place in range(4):
        load_a(place).start()

    def bring(j):
        send_d(j).start()
        load_b(j).start()

    for j in range(AHEAD):
        bring(j)

    @pl.when(depth == 1)
    def _():
        for i in range(2):
            hand_over(i).wait_recv()
            send_for_other(i).start()
        for i in range(4, last + 2):
            send_a(i).start()

    for place in range(4):
        load_a(place).wait()

    def part(j, h):
        p_snd[j, pl.ds(h * half, half), :] = jnp.dot(
            a_nbr[pl.ds(h * half, half), :], b_buf[j], preferred_element_type=jnp.float32)

    def gather(j):
        send_b(j).wait_recv()
        relay(j).start()

        @pl.when(j < n_chunks - AHEAD)
        def _():
            bring(j + AHEAD)

        load_b(j).wait()
        send_d(j).wait_recv()
        relay(j).wait_recv()

    @pl.loop(0, n_here)
    def _(j):
        gather(j)

        @pl.when(j == 0)
        def _():
            for i in range(4):
                send_a(i).wait_recv()

        @pl.when(j == LAG)
        def _():
            for i in range(4, last + 2):
                send_a(i).wait_recv()

        part(j, 0)

        @pl.when(j >= LAG)
        def _():
            part(j - LAG, 1)
            send_c(j, 0).start()

        p_own[j] = jnp.dot(a_own[...], b_buf[j], preferred_element_type=jnp.float32)

        @pl.when(j < LAG)
        def _():
            send_c(j, 0).start()

        @pl.when(j >= LAG)
        def _():
            send_c(j - LAG, 1).start()

    @pl.loop(n_here - LAG, n_here)
    def _(j):
        part(j, 1)

    def send_last():
        piece = pl.ds(half, half - ROUND)
        return pltpu.make_async_remote_copy(
            src_ref=p_snd.at[n_here - 1, piece, :], dst_ref=p_rcv.at[n_here - 1, piece, :],
            send_sem=c_snd_sem.at[n_here - 1, 1], recv_sem=c_rcv_sem.at[n_here - 1, 1],
            device_id=to_x, device_id_type=MESH)

    def add(j, piece):
        c_ref[piece, cols(j)] = (p_own[j, piece, :] + p_rcv[j, piece, :]).astype(c_ref.dtype)

    def finish(j):
        for h in range(2):
            send_c(j, h).wait_recv()
            add(j, pl.ds(h * half, half))

    finish(0)
    for j in range(n_here - LAG, n_here - 1):
        send_c(j, 1).start()

    @pl.when(source)
    def _():
        go_round(0).start()

    @pl.when(first_relay)
    def _():
        go_round(0).wait_recv()
        go_round(1).start()

    send_rest().start()
    send_last().start()

    @pl.when(jnp.logical_not(source))
    def _():
        send_tail().start()

    gather(n_chunks - 1)
    nbr_ref[...] = jnp.dot(a_nbr[...], b_buf[n_chunks - 1], preferred_element_type=jnp.float32)
    own_ref[...] = jnp.dot(a_own[...], b_buf[n_chunks - 1], preferred_element_type=jnp.float32)

    @pl.when(depth == 1)
    def _():
        send_early().start()

    @pl.loop(1, n_here - LAG)
    def _(j):
        finish(j)

    for i in range(last):
        send_a(i).wait_send()

    @pl.when(depth == 0)
    def _():
        for i in range(2):
            hand_over(i).wait_send()

    @pl.when(depth == 1)
    def _():
        for i in range(2):
            send_a(last + i).wait_send()
            send_for_other(i).wait_send()

    @pl.loop(0, n_chunks)
    def _(j):
        send_b(j).wait_send()
        send_d(j).wait_send()
        relay(j).wait_send()

    @pl.loop(0, n_here - LAG)
    def _(j):
        for h in range(2):
            send_c(j, h).wait_send()

    for j in range(n_here - LAG, n_here - 1):
        finish(j)
        for h in range(2):
            send_c(j, h).wait_send()

    @pl.when(second_relay)
    def _():
        go_round(1).wait_recv()
        go_round(2).start()

    send_c(n_here - 1, 0).wait_recv()
    add(n_here - 1, pl.ds(0, half))
    send_last().wait_recv()
    add(n_here - 1, pl.ds(half, half - ROUND))
    send_rest().wait_recv()
    send_tail().wait_recv()
    add(n_here - 1, tail_rows)

    @pl.when(source | first_relay | second_relay)
    def _():
        go_round(0).wait_send()

    @pl.when(depth == 1)
    def _():
        send_early().wait_recv()
        c_ref[early, cols(n_chunks - 1)] = (own_ref[early, :] + early_rcv[...]).astype(c_ref.dtype)
        send_early().wait_send()

    send_c(n_here - 1, 0).wait_send()
    send_last().wait_send()
    send_rest().wait_send()

    @pl.when(jnp.logical_not(source))
    def _():
        send_tail().wait_send()


def last_kernel(own_ref, nbr_ref, out_ref, c_ref, rcv, snd_sem, rcv_sem):
    to_x = {"row": 1 - lax.axis_index("row")}
    depth = lax.axis_index("depth")
    rows = own_ref.shape[0]
    pieces = [pl.ds(0, EARLY), pl.ds(EARLY, rows - EARLY)]

    def send(i):
        return pltpu.make_async_remote_copy(
            src_ref=nbr_ref.at[pieces[i]], dst_ref=rcv.at[pieces[i]], send_sem=snd_sem.at[i], recv_sem=rcv_sem.at[i],
            device_id=to_x, device_id_type=MESH)

    def add(i):
        c_ref[pieces[i], :] = (own_ref[pieces[i], :] + rcv[pieces[i], :]).astype(c_ref.dtype)

    barrier = pltpu.get_barrier_semaphore()
    pl.semaphore_signal(barrier, inc=1, device_id=to_x, device_id_type=MESH)
    pl.semaphore_wait(barrier, 1)

    @pl.when(depth == 0)
    def _():
        send(0).start()

    send(1).start()

    @pl.when(depth == 0)
    def _():
        send(0).wait_recv()
        add(0)

    send(1).wait_recv()
    add(1)

    @pl.when(depth == 0)
    def _():
        send(0).wait_send()

    send(1).wait_send()


def write_first(c_ref, out_ref, sem):
    depth = lax.axis_index("depth")
    n, tail = c_ref.shape[1] - TN, pl.ds(c_ref.shape[1] - TN, TN)
    early = pl.ds(0, EARLY)
    copy = pltpu.make_async_copy(c_ref.at[:, pl.ds(0, n)], out_ref.at[:, pl.ds(0, n)], sem.at[0])
    more = pltpu.make_async_copy(c_ref.at[early, tail], out_ref.at[early, tail], sem.at[1])
    copy.start()

    @pl.when(depth == 1)
    def _():
        more.start()
        more.wait()

    copy.wait()


def write_last(whole_ref, c_ref, out_ref, sem):
    depth = lax.axis_index("depth")
    tail = pl.ds(out_ref.shape[1] - TN, TN)
    early, late = pl.ds(0, EARLY), pl.ds(EARLY, c_ref.shape[0] - EARLY)
    copy = pltpu.make_async_copy(c_ref.at[late], out_ref.at[late, tail], sem.at[0])
    more = pltpu.make_async_copy(c_ref.at[early], out_ref.at[early, tail], sem.at[1])
    copy.start()

    @pl.when(depth == 0)
    def _():
        more.start()
        more.wait()

    copy.wait()


def solution(mesh):
    all_axes = ("depth", "row", "col")

    def device_block(a_rows, b_rows):
        rows, depth = a_rows.shape
        k_rows, n = b_rows.shape
        k = 4 * k_rows
        n_chunks = n // TN
        dma = pltpu.SemaphoreType.DMA
        n_here = n_chunks - 1
        f32 = jnp.float32
        vmem, any_space = pl.BlockSpec(memory_space=pltpu.VMEM), pl.BlockSpec(memory_space=pl.ANY)
        kept = 2 * rows * n + 8 * rows * TN
        regular = pltpu.SemaphoreType.REGULAR
        c, own, nbr = pl.pallas_call(
            kernel,
            out_shape=(pltpu.VMEM((rows, n), jnp.bfloat16),
                       pltpu.VMEM((rows, TN), f32), pltpu.VMEM((rows, TN), f32)),
            in_specs=[any_space] * 2,
            out_specs=(vmem,) * 3,
            scratch_shapes=[
                pltpu.VMEM((n_chunks, k, TN), jnp.bfloat16),
                pltpu.VMEM((rows, k), jnp.bfloat16),
                pltpu.VMEM((rows, k), jnp.bfloat16),
                pltpu.VMEM((n_here, rows, TN), f32),
                pltpu.VMEM((n_here, rows, TN), f32),
                pltpu.VMEM((n_here, rows, TN), f32),
                pltpu.VMEM((2, EXTRA, k_rows), jnp.bfloat16),
                dma((4,)), dma((n_chunks,)),
                dma((10,)), dma((10,)),
                dma((n_chunks,)), dma((n_chunks,)),
                dma((n_chunks,)), dma((n_chunks,)),
                dma((n_chunks,)), dma((n_chunks,)),
                dma((n_here, 2)), dma((n_here, 2)),
                dma((2,)), dma((2,)), dma((2,)),
                regular, regular,
                pltpu.VMEM((ROUND, ROUND_N), f32), dma((3,)), dma((3,)),
                pltpu.VMEM((EARLY, TN), f32), dma((2,)),
            ],
            compiler_params=pltpu.CompilerParams(
                collective_id=0, has_side_effects=True, vmem_limit_bytes=67043328 - kept),
        )(a_rows, b_rows)
        in_vmem = lambda x: pltpu.with_memory_space_constraint(x, pltpu.VMEM)
        small = pltpu.CompilerParams(vmem_limit_bytes=2 ** 20)
        whole = jax.ShapeDtypeStruct((rows, n), jnp.bfloat16)
        out = pl.pallas_call(
            write_first, out_shape=whole, in_specs=[vmem], out_specs=any_space,
            scratch_shapes=[dma((2,))], compiler_params=small)(in_vmem(c))
        c_last = pl.pallas_call(
            last_kernel,
            out_shape=pltpu.VMEM((rows, TN), jnp.bfloat16),
            in_specs=[vmem, vmem, pl.BlockSpec(memory_space=pltpu.HBM)],
            out_specs=vmem,
            scratch_shapes=[pltpu.VMEM((rows, TN), f32), dma((2,)), dma((2,))],
            compiler_params=pltpu.CompilerParams(
                collective_id=1, has_side_effects=True, vmem_limit_bytes=2 ** 23),
        )(in_vmem(own), in_vmem(nbr), pltpu.with_memory_space_constraint(out, pltpu.HBM))
        return pl.pallas_call(
            write_last, out_shape=whole, in_specs=[any_space, vmem], out_specs=any_space,
            scratch_shapes=[dma((2,))], input_output_aliases={0: 0}, compiler_params=small)(out, in_vmem(c_last))

    return jax.shard_map(device_block, mesh=mesh, in_specs=(P(all_axes, None), P(all_axes, None)),
                         out_specs=P(all_axes, None), check_vma=False)
```

```python
import jax
import jax.numpy as jnp
from jax import lax
from jax.experimental import pallas as pl
from jax.experimental.pallas import tpu as pltpu
from jax.sharding import PartitionSpec as P

MESH = pl.DeviceIdType.MESH
TN = 512
LAG = 2
AHEAD = 2
ROUND = 16
ROUND_N = 384
EXTRA = 48
EARLY = 304


def kernel(a_ref, b_ref, c_ref, own_ref, nbr_ref, b_buf, a_own, a_nbr, p_own, p_snd, p_rcv, a_fwd,
           ld_a, ld_b, a_snd_sem, a_rcv_sem, b_snd_sem, b_rcv_sem, d_snd_sem, d_rcv_sem,
           r_snd_sem, r_rcv_sem, c_snd_sem, c_rcv_sem, f_snd_sem, f_rcv_sem, fwd_sem,
           pair_sem, core_sem, round_buf, round_snd, round_rcv, early_rcv, early_sem):
    depth, row, col = lax.axis_index("depth"), lax.axis_index("row"), lax.axis_index("col")
    to_x, to_y, to_d = {"row": 1 - row}, {"col": 1 - col}, {"depth": 1 - depth}
    rows, k_rows = a_ref.shape[0], b_ref.shape[0]
    half = rows // 2
    n_chunks, n_here = b_buf.shape[0], p_own.shape[0]

    def k_block(place, r):
        d = 1 - depth if place % 2 else depth
        c = 1 - col if place // 2 else col
        return pl.ds(pl.multiple_of((d * 4 + r * 2 + c) * k_rows, k_rows), k_rows)

    def slot(place):
        return pl.ds(place * k_rows, k_rows)

    def cols(j):
        return pl.ds(pl.multiple_of(j * TN, TN), TN)

    def load_a(place):
        return pltpu.make_async_copy(a_ref.at[:, k_block(place, row)], a_own.at[:, slot(place)], ld_a.at[place])

    def load_b(j):
        return pltpu.make_async_copy(b_ref.at[:, cols(j)], b_buf.at[j, slot(0), :], ld_b.at[j])

    pieces = [(0, half, p) for p in range(4)] + [(half, half, p) for p in range(2)]
    pieces += [(half, half - EXTRA, p) for p in (2, 3)] + [(rows - EXTRA, EXTRA, p) for p in (2, 3)]
    last = len(pieces) - 2

    def send_a(i):
        start, size, place = pieces[i]
        return pltpu.make_async_remote_copy(
            src_ref=a_ref.at[pl.ds(start, size), k_block(place, 1 - row)],
            dst_ref=a_nbr.at[pl.ds(start, size), slot(place)],
            send_sem=a_snd_sem.at[i], recv_sem=a_rcv_sem.at[i], device_id=to_x, device_id_type=MESH)

    def hand_over(i):
        start, size, place = pieces[last + i]
        return pltpu.make_async_remote_copy(
            src_ref=a_ref.at[pl.ds(start, size), k_block(place, 1 - row)], dst_ref=a_fwd.at[i],
            send_sem=f_snd_sem.at[i], recv_sem=f_rcv_sem.at[i], device_id=to_d, device_id_type=MESH)

    def send_for_other(i):
        start, size, place = pieces[last + i]
        return pltpu.make_async_remote_copy(
            src_ref=a_fwd.at[i], dst_ref=a_nbr.at[pl.ds(start, size), slot(place)],
            send_sem=fwd_sem.at[i], recv_sem=a_rcv_sem.at[last + i],
            device_id={"row": 1 - row, "depth": 0}, device_id_type=MESH)

    def send_b(j):
        return pltpu.make_async_remote_copy(
            src_ref=b_ref.at[:, cols(j)], dst_ref=b_buf.at[j, slot(2), :],
            send_sem=b_snd_sem.at[j], recv_sem=b_rcv_sem.at[j], device_id=to_y, device_id_type=MESH)

    def send_d(j):
        return pltpu.make_async_remote_copy(
            src_ref=b_ref.at[:, cols(j)], dst_ref=b_buf.at[j, slot(1), :],
            send_sem=d_snd_sem.at[j], recv_sem=d_rcv_sem.at[j], device_id=to_d, device_id_type=MESH)

    def relay(j):
        return pltpu.make_async_remote_copy(
            src_ref=b_buf.at[j, slot(2), :], dst_ref=b_buf.at[j, slot(3), :],
            send_sem=r_snd_sem.at[j], recv_sem=r_rcv_sem.at[j], device_id=to_d, device_id_type=MESH)

    tail_rows = pl.ds(rows - ROUND, ROUND)
    source = (depth == 1) & (row == 1) & (col == 0)
    first_relay = (depth == 1) & (row == 1) & (col == 1)
    second_relay = (depth == 1) & (row == 0) & (col == 1)

    def send_tail():
        return pltpu.make_async_remote_copy(
            src_ref=p_snd.at[n_here - 1, tail_rows, pl.ds(0, ROUND_N)], dst_ref=p_rcv.at[n_here - 1, tail_rows, pl.ds(0, ROUND_N)],
            send_sem=round_snd.at[0], recv_sem=round_rcv.at[0], device_id=to_x, device_id_type=MESH)

    def send_rest():
        rest = pl.ds(ROUND_N, TN - ROUND_N)
        return pltpu.make_async_remote_copy(
            src_ref=p_snd.at[n_here - 1, tail_rows, rest], dst_ref=p_rcv.at[n_here - 1, tail_rows, rest],
            send_sem=round_snd.at[2], recv_sem=round_rcv.at[2], device_id=to_x, device_id_type=MESH)

    early = pl.ds(0, EARLY)

    def send_early():
        return pltpu.make_async_remote_copy(
            src_ref=nbr_ref.at[early], dst_ref=early_rcv, send_sem=early_sem.at[0], recv_sem=early_sem.at[1],
            device_id=to_x, device_id_type=MESH)

    def go_round(step):
        src = p_snd.at[n_here - 1, tail_rows, pl.ds(0, ROUND_N)] if step == 0 else round_buf
        dst = p_rcv.at[n_here - 1, tail_rows, pl.ds(0, ROUND_N)] if step == 2 else round_buf
        return pltpu.make_async_remote_copy(
            src_ref=src, dst_ref=dst, send_sem=round_snd.at[1], recv_sem=round_rcv.at[0 if step == 2 else 1],
            device_id=to_x if step == 1 else to_y, device_id_type=MESH)

    def send_c(j, h):
        return pltpu.make_async_remote_copy(
            src_ref=p_snd.at[j, pl.ds(h * half, half), :], dst_ref=p_rcv.at[j, pl.ds(h * half, half), :],
            send_sem=c_snd_sem.at[j, h], recv_sem=c_rcv_sem.at[j, h], device_id=to_x, device_id_type=MESH)

    barrier = pltpu.get_barrier_semaphore()
    for peer in (to_x, {"depth": 0, "col": lax.rem(col + 1 - depth, 2)}):
        pl.semaphore_signal(barrier, inc=1, device_id=peer, device_id_type=MESH)
    pl.semaphore_wait(barrier, 3 - 2 * depth)

    for i in range(4):
        send_a(i).start()

    @pl.when(depth == 0)
    def _():
        for i in range(4, last):
            send_a(i).start()
        for i in range(2):
            hand_over(i).start()
        pl.semaphore_signal(pair_sem, inc=1, device_id=to_y, device_id_type=MESH)
        pl.semaphore_wait(pair_sem, 1)
        pl.semaphore_signal(core_sem, inc=1, device_id=to_d, device_id_type=MESH)

    @pl.when(depth == 1)
    def _():
        pl.semaphore_wait(core_sem, 1)

    @pl.loop(0, n_chunks)
    def _(j):
        send_b(j).start()

    for place in range(4):
        load_a(place).start()

    def bring(j):
        send_d(j).start()
        load_b(j).start()

    for j in range(AHEAD):
        bring(j)

    @pl.when(depth == 1)
    def _():
        for i in range(2):
            hand_over(i).wait_recv()
            send_for_other(i).start()
        for i in range(4, last + 2):
            send_a(i).start()

    for place in range(4):
        load_a(place).wait()

    def part(j, h):
        p_snd[j, pl.ds(h * half, half), :] = jnp.dot(
            a_nbr[pl.ds(h * half, half), :], b_buf[j], preferred_element_type=jnp.float32)

    def gather(j):
        send_b(j).wait_recv()
        relay(j).start()

        @pl.when(j < n_chunks - AHEAD)
        def _():
            bring(j + AHEAD)

        load_b(j).wait()
        send_d(j).wait_recv()
        relay(j).wait_recv()

    @pl.loop(0, n_here)
    def _(j):
        gather(j)

        @pl.when(j == 0)
        def _():
            for i in range(4):
                send_a(i).wait_recv()

        @pl.when(j == LAG)
        def _():
            for i in range(4, last + 2):
                send_a(i).wait_recv()

        part(j, 0)

        @pl.when(j >= LAG)
        def _():
            part(j - LAG, 1)
            send_c(j, 0).start()

        p_own[j] = jnp.dot(a_own[...], b_buf[j], preferred_element_type=jnp.float32)

        @pl.when(j < LAG)
        def _():
            send_c(j, 0).start()

        @pl.when(j >= LAG)
        def _():
            send_c(j - LAG, 1).start()

    @pl.loop(n_here - LAG, n_here)
    def _(j):
        part(j, 1)

    def send_last():
        piece = pl.ds(half, half - ROUND)
        return pltpu.make_async_remote_copy(
            src_ref=p_snd.at[n_here - 1, piece, :], dst_ref=p_rcv.at[n_here - 1, piece, :],
            send_sem=c_snd_sem.at[n_here - 1, 1], recv_sem=c_rcv_sem.at[n_here - 1, 1],
            device_id=to_x, device_id_type=MESH)

    def add(j, piece):
        c_ref[piece, cols(j)] = (p_own[j, piece, :] + p_rcv[j, piece, :]).astype(c_ref.dtype)

    def finish(j):
        for h in range(2):
            send_c(j, h).wait_recv()
            add(j, pl.ds(h * half, half))

    finish(0)
    for j in range(n_here - LAG, n_here - 1):
        send_c(j, 1).start()

    @pl.when(source)
    def _():
        go_round(0).start()

    @pl.when(first_relay)
    def _():
        go_round(0).wait_recv()
        go_round(1).start()

    send_rest().start()
    send_last().start()

    @pl.when(jnp.logical_not(source))
    def _():
        send_tail().start()

    gather(n_chunks - 1)
    nbr_ref[...] = jnp.dot(a_nbr[...], b_buf[n_chunks - 1], preferred_element_type=jnp.float32)
    own_ref[...] = jnp.dot(a_own[...], b_buf[n_chunks - 1], preferred_element_type=jnp.float32)

    @pl.when(depth == 1)
    def _():
        send_early().start()

    @pl.loop(1, n_here - LAG)
    def _(j):
        finish(j)

    for i in range(last):
        send_a(i).wait_send()

    @pl.when(depth == 0)
    def _():
        for i in range(2):
            hand_over(i).wait_send()

    @pl.when(depth == 1)
    def _():
        for i in range(2):
            send_a(last + i).wait_send()
            send_for_other(i).wait_send()

    @pl.loop(0, n_chunks)
    def _(j):
        send_b(j).wait_send()
        send_d(j).wait_send()
        relay(j).wait_send()

    @pl.loop(0, n_here - LAG)
    def _(j):
        for h in range(2):
            send_c(j, h).wait_send()

    for j in range(n_here - LAG, n_here - 1):
        finish(j)
        for h in range(2):
            send_c(j, h).wait_send()

    @pl.when(second_relay)
    def _():
        go_round(1).wait_recv()
        go_round(2).start()

    send_c(n_here - 1, 0).wait_recv()
    add(n_here - 1, pl.ds(0, half))
    send_last().wait_recv()
    add(n_here - 1, pl.ds(half, half - ROUND))
    send_rest().wait_recv()
    send_tail().wait_recv()
    add(n_here - 1, tail_rows)

    @pl.when(source | first_relay | second_relay)
    def _():
        go_round(0).wait_send()

    @pl.when(depth == 1)
    def _():
        send_early().wait_recv()
        c_ref[early, cols(n_chunks - 1)] = (own_ref[early, :] + early_rcv[...]).astype(c_ref.dtype)
        send_early().wait_send()

    send_c(n_here - 1, 0).wait_send()
    send_last().wait_send()
    send_rest().wait_send()

    @pl.when(jnp.logical_not(source))
    def _():
        send_tail().wait_send()


def last_kernel(own_ref, nbr_ref, out_ref, c_ref, rcv, snd_sem, rcv_sem):
    to_x = {"row": 1 - lax.axis_index("row")}
    depth = lax.axis_index("depth")
    rows = own_ref.shape[0]
    pieces = [pl.ds(0, EARLY), pl.ds(EARLY, rows - EARLY)]

    def send(i):
        return pltpu.make_async_remote_copy(
            src_ref=nbr_ref.at[pieces[i]], dst_ref=rcv.at[pieces[i]], send_sem=snd_sem.at[i], recv_sem=rcv_sem.at[i],
            device_id=to_x, device_id_type=MESH)

    def add(i):
        c_ref[pieces[i], :] = (own_ref[pieces[i], :] + rcv[pieces[i], :]).astype(c_ref.dtype)

    barrier = pltpu.get_barrier_semaphore()
    pl.semaphore_signal(barrier, inc=1, device_id=to_x, device_id_type=MESH)
    pl.semaphore_wait(barrier, 1)

    @pl.when(depth == 0)
    def _():
        send(0).start()

    send(1).start()

    @pl.when(depth == 0)
    def _():
        send(0).wait_recv()
        add(0)

    send(1).wait_recv()
    add(1)

    @pl.when(depth == 0)
    def _():
        send(0).wait_send()

    send(1).wait_send()


def write_first(c_ref, out_ref, sem):
    depth = lax.axis_index("depth")
    n, tail = c_ref.shape[1] - TN, pl.ds(c_ref.shape[1] - TN, TN)
    early = pl.ds(0, EARLY)
    copy = pltpu.make_async_copy(c_ref.at[:, pl.ds(0, n)], out_ref.at[:, pl.ds(0, n)], sem.at[0])
    more = pltpu.make_async_copy(c_ref.at[early, tail], out_ref.at[early, tail], sem.at[1])
    copy.start()

    @pl.when(depth == 1)
    def _():
        more.start()
        more.wait()

    copy.wait()


def write_last(whole_ref, c_ref, out_ref, sem):
    depth = lax.axis_index("depth")
    tail = pl.ds(out_ref.shape[1] - TN, TN)
    early, late = pl.ds(0, EARLY), pl.ds(EARLY, c_ref.shape[0] - EARLY)
    copy = pltpu.make_async_copy(c_ref.at[late], out_ref.at[late, tail], sem.at[0])
    more = pltpu.make_async_copy(c_ref.at[early], out_ref.at[early, tail], sem.at[1])
    copy.start()

    @pl.when(depth == 0)
    def _():
        more.start()
        more.wait()

    copy.wait()


def solution(mesh):
    all_axes = ("depth", "row", "col")

    def device_block(a_rows, b_rows):
        rows, depth = a_rows.shape
        k_rows, n = b_rows.shape
        k = 4 * k_rows
        n_chunks = n // TN
        dma = pltpu.SemaphoreType.DMA
        n_here = n_chunks - 1
        f32 = jnp.float32
        vmem, any_space = pl.BlockSpec(memory_space=pltpu.VMEM), pl.BlockSpec(memory_space=pl.ANY)
        kept = 2 * rows * n + 8 * rows * TN
        regular = pltpu.SemaphoreType.REGULAR
        c, own, nbr = pl.pallas_call(
            kernel,
            out_shape=(pltpu.VMEM((rows, n), jnp.bfloat16),
                       pltpu.VMEM((rows, TN), f32), pltpu.VMEM((rows, TN), f32)),
            in_specs=[any_space] * 2,
            out_specs=(vmem,) * 3,
            scratch_shapes=[
                pltpu.VMEM((n_chunks, k, TN), jnp.bfloat16),
                pltpu.VMEM((rows, k), jnp.bfloat16),
                pltpu.VMEM((rows, k), jnp.bfloat16),
                pltpu.VMEM((n_here, rows, TN), f32),
                pltpu.VMEM((n_here, rows, TN), f32),
                pltpu.VMEM((n_here, rows, TN), f32),
                pltpu.VMEM((2, EXTRA, k_rows), jnp.bfloat16),
                dma((4,)), dma((n_chunks,)),
                dma((10,)), dma((10,)),
                dma((n_chunks,)), dma((n_chunks,)),
                dma((n_chunks,)), dma((n_chunks,)),
                dma((n_chunks,)), dma((n_chunks,)),
                dma((n_here, 2)), dma((n_here, 2)),
                dma((2,)), dma((2,)), dma((2,)),
                regular, regular,
                pltpu.VMEM((ROUND, ROUND_N), f32), dma((3,)), dma((3,)),
                pltpu.VMEM((EARLY, TN), f32), dma((2,)),
            ],
            compiler_params=pltpu.CompilerParams(
                collective_id=0, has_side_effects=True, vmem_limit_bytes=67043328 - kept),
        )(a_rows, b_rows)
        in_vmem = lambda x: pltpu.with_memory_space_constraint(x, pltpu.VMEM)
        small = pltpu.CompilerParams(vmem_limit_bytes=2 ** 20)
        whole = jax.ShapeDtypeStruct((rows, n), jnp.bfloat16)
        out = pl.pallas_call(
            write_first, out_shape=whole, in_specs=[vmem], out_specs=any_space,
            scratch_shapes=[dma((2,))], compiler_params=small)(in_vmem(c))
        c_last = pl.pallas_call(
            last_kernel,
            out_shape=pltpu.VMEM((rows, TN), jnp.bfloat16),
            in_specs=[vmem, vmem, pl.BlockSpec(memory_space=pltpu.HBM)],
            out_specs=vmem,
            scratch_shapes=[pltpu.VMEM((rows, TN), f32), dma((2,)), dma((2,))],
            compiler_params=pltpu.CompilerParams(
                collective_id=1, has_side_effects=True, vmem_limit_bytes=2 ** 23),
        )(in_vmem(own), in_vmem(nbr), pltpu.with_memory_space_constraint(out, pltpu.HBM))
        return pl.pallas_call(
            write_last, out_shape=whole, in_specs=[any_space, vmem], out_specs=any_space,
            scratch_shapes=[dma((2,))], input_output_aliases={0: 0}, compiler_params=small)(out, in_vmem(c_last))

    return jax.shard_map(device_block, mesh=mesh, in_specs=(P(all_axes, None), P(all_axes, None)),
                         out_specs=P(all_axes, None), check_vma=False)
```

```python
import jax
import jax.numpy as jnp
from jax import lax
from jax.experimental import pallas as pl
from jax.experimental.pallas import tpu as pltpu
from jax.sharding import PartitionSpec as P

MESH = pl.DeviceIdType.MESH
TN = 512
LAG = 2
AHEAD = 2
ROUND = 16
ROUND_N = 384
EXTRA = 48
EARLY = 304


def kernel(a_ref, b_ref, c_ref, own_ref, nbr_ref, b_buf, a_own, a_nbr, p_own, p_snd, p_rcv, a_fwd,
           ld_a, ld_b, a_snd_sem, a_rcv_sem, b_snd_sem, b_rcv_sem, d_snd_sem, d_rcv_sem,
           r_snd_sem, r_rcv_sem, c_snd_sem, c_rcv_sem, f_snd_sem, f_rcv_sem, fwd_sem,
           pair_sem, core_sem, round_buf, round_snd, round_rcv, early_rcv, early_sem):
    depth, row, col = lax.axis_index("depth"), lax.axis_index("row"), lax.axis_index("col")
    to_x, to_y, to_d = {"row": 1 - row}, {"col": 1 - col}, {"depth": 1 - depth}
    rows, k_rows = a_ref.shape[0], b_ref.shape[0]
    half = rows // 2
    n_chunks, n_here = b_buf.shape[0], p_own.shape[0]

    def k_block(place, r):
        d = 1 - depth if place % 2 else depth
        c = 1 - col if place // 2 else col
        return pl.ds(pl.multiple_of((d * 4 + r * 2 + c) * k_rows, k_rows), k_rows)

    def slot(place):
        return pl.ds(place * k_rows, k_rows)

    def cols(j):
        return pl.ds(pl.multiple_of(j * TN, TN), TN)

    def load_a(place):
        return pltpu.make_async_copy(a_ref.at[:, k_block(place, row)], a_own.at[:, slot(place)], ld_a.at[place])

    def load_b(j):
        return pltpu.make_async_copy(b_ref.at[:, cols(j)], b_buf.at[j, slot(0), :], ld_b.at[j])

    pieces = [(0, half, p) for p in range(4)] + [(half, half, p) for p in range(2)]
    pieces += [(half, half - EXTRA, p) for p in (2, 3)] + [(rows - EXTRA, EXTRA, p) for p in (2, 3)]
    last = len(pieces) - 2

    def send_a(i):
        start, size, place = pieces[i]
        return pltpu.make_async_remote_copy(
            src_ref=a_ref.at[pl.ds(start, size), k_block(place, 1 - row)],
            dst_ref=a_nbr.at[pl.ds(start, size), slot(place)],
            send_sem=a_snd_sem.at[i], recv_sem=a_rcv_sem.at[i], device_id=to_x, device_id_type=MESH)

    def hand_over(i):
        start, size, place = pieces[last + i]
        return pltpu.make_async_remote_copy(
            src_ref=a_ref.at[pl.ds(start, size), k_block(place, 1 - row)], dst_ref=a_fwd.at[i],
            send_sem=f_snd_sem.at[i], recv_sem=f_rcv_sem.at[i], device_id=to_d, device_id_type=MESH)

    def send_for_other(i):
        start, size, place = pieces[last + i]
        return pltpu.make_async_remote_copy(
            src_ref=a_fwd.at[i], dst_ref=a_nbr.at[pl.ds(start, size), slot(place)],
            send_sem=fwd_sem.at[i], recv_sem=a_rcv_sem.at[last + i],
            device_id={"row": 1 - row, "depth": 0}, device_id_type=MESH)

    def send_b(j):
        return pltpu.make_async_remote_copy(
            src_ref=b_ref.at[:, cols(j)], dst_ref=b_buf.at[j, slot(2), :],
            send_sem=b_snd_sem.at[j], recv_sem=b_rcv_sem.at[j], device_id=to_y, device_id_type=MESH)

    def send_d(j):
        return pltpu.make_async_remote_copy(
            src_ref=b_ref.at[:, cols(j)], dst_ref=b_buf.at[j, slot(1), :],
            send_sem=d_snd_sem.at[j], recv_sem=d_rcv_sem.at[j], device_id=to_d, device_id_type=MESH)

    def relay(j):
        return pltpu.make_async_remote_copy(
            src_ref=b_buf.at[j, slot(2), :], dst_ref=b_buf.at[j, slot(3), :],
            send_sem=r_snd_sem.at[j], recv_sem=r_rcv_sem.at[j], device_id=to_d, device_id_type=MESH)

    tail_rows = pl.ds(rows - ROUND, ROUND)

    def send_tail():
        return pltpu.make_async_remote_copy(
            src_ref=p_snd.at[n_here - 1, tail_rows, pl.ds(0, ROUND_N)], dst_ref=p_rcv.at[n_here - 1, tail_rows, pl.ds(0, ROUND_N)],
            send_sem=round_snd.at[0], recv_sem=round_rcv.at[0], device_id=to_x, device_id_type=MESH)

    def send_rest():
        rest = pl.ds(ROUND_N, TN - ROUND_N)
        return pltpu.make_async_remote_copy(
            src_ref=p_snd.at[n_here - 1, tail_rows, rest], dst_ref=p_rcv.at[n_here - 1, tail_rows, rest],
            send_sem=round_snd.at[2], recv_sem=round_rcv.at[2], device_id=to_x, device_id_type=MESH)

    early = pl.ds(0, EARLY)

    def send_early():
        return pltpu.make_async_remote_copy(
            src_ref=nbr_ref.at[early], dst_ref=early_rcv, send_sem=early_sem.at[0], recv_sem=early_sem.at[1],
            device_id=to_x, device_id_type=MESH)

    def go_round(step):
        src = p_snd.at[n_here - 1, tail_rows, pl.ds(0, ROUND_N)] if step == 0 else round_buf
        dst = p_rcv.at[n_here - 1, tail_rows, pl.ds(0, ROUND_N)] if step == 2 else round_buf
        return pltpu.make_async_remote_copy(
            src_ref=src, dst_ref=dst, send_sem=round_snd.at[1], recv_sem=round_rcv.at[0 if step == 2 else 1],
            device_id=to_x if step == 1 else to_y, device_id_type=MESH)

    def send_c(j, h):
        return pltpu.make_async_remote_copy(
            src_ref=p_snd.at[j, pl.ds(h * half, half), :], dst_ref=p_rcv.at[j, pl.ds(h * half, half), :],
            send_sem=c_snd_sem.at[j, h], recv_sem=c_rcv_sem.at[j, h], device_id=to_x, device_id_type=MESH)

    barrier = pltpu.get_barrier_semaphore()
    for peer in (to_x, {"depth": 0, "col": (1 - depth - col) * (1 - depth - col)}):
        pl.semaphore_signal(barrier, inc=1, device_id=peer, device_id_type=MESH)
    pl.semaphore_wait(barrier, 3 - 2 * depth)

    for i in range(4):
        send_a(i).start()

    @pl.when(depth == 0)
    def _():
        for i in range(4, last):
            send_a(i).start()
        for i in range(2):
            hand_over(i).start()
        pl.semaphore_signal(pair_sem, inc=1, device_id=to_y, device_id_type=MESH)
        pl.semaphore_wait(pair_sem, 1)
        pl.semaphore_signal(core_sem, inc=1, device_id=to_d, device_id_type=MESH)

    @pl.when(depth == 1)
    def _():
        pl.semaphore_wait(core_sem, 1)

    @pl.loop(0, n_chunks)
    def _(j):
        send_b(j).start()

    for place in range(4):
        load_a(place).start()

    def bring(j):
        send_d(j).start()
        load_b(j).start()

    for j in range(AHEAD):
        bring(j)

    @pl.when(depth == 1)
    def _():
        for i in range(2):
            hand_over(i).wait_recv()
            send_for_other(i).start()
        for i in range(4, last + 2):
            send_a(i).start()

    for place in range(4):
        load_a(place).wait()

    def part(j, h):
        p_snd[j, pl.ds(h * half, half), :] = jnp.dot(
            a_nbr[pl.ds(h * half, half), :], b_buf[j], preferred_element_type=jnp.float32)

    def gather(j):
        send_b(j).wait_recv()
        relay(j).start()

        @pl.when(j < n_chunks - AHEAD)
        def _():
            bring(j + AHEAD)

        load_b(j).wait()
        send_d(j).wait_recv()
        relay(j).wait_recv()

    @pl.loop(0, n_here)
    def _(j):
        gather(j)

        @pl.when(j == 0)
        def _():
            for i in range(4):
                send_a(i).wait_recv()

        @pl.when(j == LAG)
        def _():
            for i in range(4, last + 2):
                send_a(i).wait_recv()

        part(j, 0)

        @pl.when(j >= LAG)
        def _():
            part(j - LAG, 1)
            send_c(j, 0).start()

        p_own[j] = jnp.dot(a_own[...], b_buf[j], preferred_element_type=jnp.float32)

        @pl.when(j < LAG)
        def _():
            send_c(j, 0).start()

        @pl.when(j >= LAG)
        def _():
            send_c(j - LAG, 1).start()

    @pl.loop(n_here - LAG, n_here)
    def _(j):
        part(j, 1)

    def send_last():
        piece = pl.ds(half, half - ROUND)
        return pltpu.make_async_remote_copy(
            src_ref=p_snd.at[n_here - 1, piece, :], dst_ref=p_rcv.at[n_here - 1, piece, :],
            send_sem=c_snd_sem.at[n_here - 1, 1], recv_sem=c_rcv_sem.at[n_here - 1, 1],
            device_id=to_x, device_id_type=MESH)

    def add(j, piece):
        c_ref[piece, cols(j)] = (p_own[j, piece, :] + p_rcv[j, piece, :]).astype(c_ref.dtype)

    def finish(j):
        for h in range(2):
            send_c(j, h).wait_recv()
            add(j, pl.ds(h * half, half))

    finish(0)
    source = (depth == 1) & (row == 1) & (col == 0)
    first_relay = (depth == 1) & (row == 1) & (col == 1)
    second_relay = (depth == 1) & (row == 0) & (col == 1)
    for j in range(n_here - LAG, n_here - 1):
        send_c(j, 1).start()

    @pl.when(source)
    def _():
        go_round(0).start()

    @pl.when(first_relay)
    def _():
        go_round(0).wait_recv()
        go_round(1).start()

    send_rest().start()
    send_last().start()

    @pl.when(jnp.logical_not(source))
    def _():
        send_tail().start()

    gather(n_chunks - 1)
    nbr_ref[...] = jnp.dot(a_nbr[...], b_buf[n_chunks - 1], preferred_element_type=jnp.float32)
    own_ref[...] = jnp.dot(a_own[...], b_buf[n_chunks - 1], preferred_element_type=jnp.float32)

    @pl.when(depth == 1)
    def _():
        send_early().start()

    @pl.loop(1, n_here - LAG)
    def _(j):
        finish(j)

    for i in range(last):
        send_a(i).wait_send()

    @pl.when(depth == 0)
    def _():
        for i in range(2):
            hand_over(i).wait_send()

    @pl.when(depth == 1)
    def _():
        for i in range(2):
            send_a(last + i).wait_send()
            send_for_other(i).wait_send()

    @pl.loop(0, n_chunks)
    def _(j):
        send_b(j).wait_send()
        send_d(j).wait_send()
        relay(j).wait_send()

    @pl.loop(0, n_here - LAG)
    def _(j):
        for h in range(2):
            send_c(j, h).wait_send()

    for j in range(n_here - LAG, n_here - 1):
        finish(j)
        for h in range(2):
            send_c(j, h).wait_send()

    @pl.when(second_relay)
    def _():
        go_round(1).wait_recv()
        go_round(2).start()

    send_c(n_here - 1, 0).wait_recv()
    add(n_here - 1, pl.ds(0, half))
    send_last().wait_recv()
    add(n_here - 1, pl.ds(half, half - ROUND))
    send_rest().wait_recv()
    send_tail().wait_recv()
    add(n_here - 1, tail_rows)

    @pl.when(source | first_relay | second_relay)
    def _():
        go_round(0).wait_send()

    @pl.when(depth == 1)
    def _():
        send_early().wait_recv()
        c_ref[early, cols(n_chunks - 1)] = (own_ref[early, :] + early_rcv[...]).astype(c_ref.dtype)
        send_early().wait_send()

    send_c(n_here - 1, 0).wait_send()
    send_last().wait_send()
    send_rest().wait_send()

    @pl.when(jnp.logical_not(source))
    def _():
        send_tail().wait_send()


def last_kernel(own_ref, nbr_ref, out_ref, c_ref, rcv, snd_sem, rcv_sem):
    to_x = {"row": 1 - lax.axis_index("row")}
    depth = lax.axis_index("depth")
    rows = own_ref.shape[0]

    def send(piece):
        return pltpu.make_async_remote_copy(
            src_ref=nbr_ref.at[piece], dst_ref=rcv.at[piece], send_sem=snd_sem, recv_sem=rcv_sem,
            device_id=to_x, device_id_type=MESH)

    def exchange(piece):
        send(piece).start()
        send(piece).wait_recv()
        c_ref[piece, :] = (own_ref[piece, :] + rcv[piece, :]).astype(c_ref.dtype)
        send(piece).wait_send()

    barrier = pltpu.get_barrier_semaphore()
    pl.semaphore_signal(barrier, inc=1, device_id=to_x, device_id_type=MESH)
    pl.semaphore_wait(barrier, 1)

    @pl.when(depth == 0)
    def _():
        exchange(pl.ds(0, rows))

    @pl.when(depth == 1)
    def _():
        exchange(pl.ds(EARLY, rows - EARLY))


def write_first(c_ref, out_ref, sem):
    depth = lax.axis_index("depth")
    n, tail = c_ref.shape[1] - TN, pl.ds(c_ref.shape[1] - TN, TN)
    early = pl.ds(0, EARLY)
    copy = pltpu.make_async_copy(c_ref.at[:, pl.ds(0, n)], out_ref.at[:, pl.ds(0, n)], sem.at[0])
    more = pltpu.make_async_copy(c_ref.at[early, tail], out_ref.at[early, tail], sem.at[1])
    copy.start()

    @pl.when(depth == 1)
    def _():
        more.start()
        more.wait()

    copy.wait()


def write_last(whole_ref, c_ref, out_ref, sem):
    depth = lax.axis_index("depth")
    tail = pl.ds(out_ref.shape[1] - TN, TN)

    def write(piece):
        copy = pltpu.make_async_copy(c_ref.at[piece], out_ref.at[piece, tail], sem)
        copy.start()
        copy.wait()

    @pl.when(depth == 0)
    def _():
        write(pl.ds(0, c_ref.shape[0]))

    @pl.when(depth == 1)
    def _():
        write(pl.ds(EARLY, c_ref.shape[0] - EARLY))


def solution(mesh):
    all_axes = ("depth", "row", "col")

    def device_block(a_rows, b_rows):
        rows, depth = a_rows.shape
        k_rows, n = b_rows.shape
        k = 4 * k_rows
        n_chunks = n // TN
        dma = pltpu.SemaphoreType.DMA
        n_here = n_chunks - 1
        f32 = jnp.float32
        vmem, any_space = pl.BlockSpec(memory_space=pltpu.VMEM), pl.BlockSpec(memory_space=pl.ANY)
        kept = 2 * rows * n + 8 * rows * TN
        regular = pltpu.SemaphoreType.REGULAR
        c, own, nbr = pl.pallas_call(
            kernel,
            out_shape=(pltpu.VMEM((rows, n), jnp.bfloat16),
                       pltpu.VMEM((rows, TN), f32), pltpu.VMEM((rows, TN), f32)),
            in_specs=[any_space] * 2,
            out_specs=(vmem,) * 3,
            scratch_shapes=[
                pltpu.VMEM((n_chunks, k, TN), jnp.bfloat16),
                pltpu.VMEM((rows, k), jnp.bfloat16),
                pltpu.VMEM((rows, k), jnp.bfloat16),
                pltpu.VMEM((n_here, rows, TN), f32),
                pltpu.VMEM((n_here, rows, TN), f32),
                pltpu.VMEM((n_here, rows, TN), f32),
                pltpu.VMEM((2, EXTRA, k_rows), jnp.bfloat16),
                dma((4,)), dma((n_chunks,)),
                dma((10,)), dma((10,)),
                dma((n_chunks,)), dma((n_chunks,)),
                dma((n_chunks,)), dma((n_chunks,)),
                dma((n_chunks,)), dma((n_chunks,)),
                dma((n_here, 2)), dma((n_here, 2)),
                dma((2,)), dma((2,)), dma((2,)),
                regular, regular,
                pltpu.VMEM((ROUND, ROUND_N), f32), dma((3,)), dma((3,)),
                pltpu.VMEM((EARLY, TN), f32), dma((2,)),
            ],
            compiler_params=pltpu.CompilerParams(
                collective_id=0, has_side_effects=True, vmem_limit_bytes=67043328 - kept),
        )(a_rows, b_rows)
        in_vmem = lambda x: pltpu.with_memory_space_constraint(x, pltpu.VMEM)
        small = pltpu.CompilerParams(vmem_limit_bytes=2 ** 20)
        whole = jax.ShapeDtypeStruct((rows, n), jnp.bfloat16)
        out = pl.pallas_call(
            write_first, out_shape=whole, in_specs=[vmem], out_specs=any_space,
            scratch_shapes=[dma((2,))], compiler_params=small)(in_vmem(c))
        c_last = pl.pallas_call(
            last_kernel,
            out_shape=pltpu.VMEM((rows, TN), jnp.bfloat16),
            in_specs=[vmem, vmem, pl.BlockSpec(memory_space=pltpu.HBM)],
            out_specs=vmem,
            scratch_shapes=[pltpu.VMEM((rows, TN), f32), dma, dma],
            compiler_params=pltpu.CompilerParams(
                collective_id=1, has_side_effects=True, vmem_limit_bytes=2 ** 23),
        )(in_vmem(own), in_vmem(nbr), pltpu.with_memory_space_constraint(out, pltpu.HBM))
        return pl.pallas_call(
            write_last, out_shape=whole, in_specs=[any_space, vmem], out_specs=any_space,
            scratch_shapes=[dma], input_output_aliases={0: 0}, compiler_params=small)(out, in_vmem(c_last))

    return jax.shard_map(device_block, mesh=mesh, in_specs=(P(all_axes, None), P(all_axes, None)),
                         out_specs=P(all_axes, None), check_vma=False)
```

```python
import jax
import jax.numpy as jnp
from jax import lax
from jax.experimental import pallas as pl
from jax.experimental.pallas import tpu as pltpu
from jax.sharding import PartitionSpec as P

MESH = pl.DeviceIdType.MESH
TN = 512
LAG = 2
AHEAD = 2
ROUND = 16
ROUND_N = 384
EXTRA = 48
EARLY = 312


def kernel(a_ref, b_ref, c_ref, own_ref, nbr_ref, b_buf, a_own, a_nbr, p_own, p_snd, p_rcv, a_fwd,
           ld_a, ld_b, a_snd_sem, a_rcv_sem, b_snd_sem, b_rcv_sem, d_snd_sem, d_rcv_sem,
           r_snd_sem, r_rcv_sem, c_snd_sem, c_rcv_sem, f_snd_sem, f_rcv_sem, fwd_sem,
           pair_sem, core_sem, round_buf, round_snd, round_rcv, early_rcv, early_sem):
    depth, row, col = lax.axis_index("depth"), lax.axis_index("row"), lax.axis_index("col")
    to_x, to_y, to_d = {"row": 1 - row}, {"col": 1 - col}, {"depth": 1 - depth}
    rows, k_rows = a_ref.shape[0], b_ref.shape[0]
    half = rows // 2
    n_chunks, n_here = b_buf.shape[0], p_own.shape[0]

    def k_block(place, r):
        d = 1 - depth if place % 2 else depth
        c = 1 - col if place // 2 else col
        return pl.ds(pl.multiple_of((d * 4 + r * 2 + c) * k_rows, k_rows), k_rows)

    def slot(place):
        return pl.ds(place * k_rows, k_rows)

    def cols(j):
        return pl.ds(pl.multiple_of(j * TN, TN), TN)

    def load_a(place):
        return pltpu.make_async_copy(a_ref.at[:, k_block(place, row)], a_own.at[:, slot(place)], ld_a.at[place])

    def load_b(j):
        return pltpu.make_async_copy(b_ref.at[:, cols(j)], b_buf.at[j, slot(0), :], ld_b.at[j])

    pieces = [(0, half, p) for p in range(4)] + [(half, half, p) for p in range(2)]
    pieces += [(half, half - EXTRA, p) for p in (2, 3)] + [(rows - EXTRA, EXTRA, p) for p in (2, 3)]
    last = len(pieces) - 2

    def send_a(i):
        start, size, place = pieces[i]
        return pltpu.make_async_remote_copy(
            src_ref=a_ref.at[pl.ds(start, size), k_block(place, 1 - row)],
            dst_ref=a_nbr.at[pl.ds(start, size), slot(place)],
            send_sem=a_snd_sem.at[i], recv_sem=a_rcv_sem.at[i], device_id=to_x, device_id_type=MESH)

    def hand_over(i):
        start, size, place = pieces[last + i]
        return pltpu.make_async_remote_copy(
            src_ref=a_ref.at[pl.ds(start, size), k_block(place, 1 - row)], dst_ref=a_fwd.at[i],
            send_sem=f_snd_sem.at[i], recv_sem=f_rcv_sem.at[i], device_id=to_d, device_id_type=MESH)

    def send_for_other(i):
        start, size, place = pieces[last + i]
        return pltpu.make_async_remote_copy(
            src_ref=a_fwd.at[i], dst_ref=a_nbr.at[pl.ds(start, size), slot(place)],
            send_sem=fwd_sem.at[i], recv_sem=a_rcv_sem.at[last + i],
            device_id={"row": 1 - row, "depth": 0}, device_id_type=MESH)

    def send_b(j):
        return pltpu.make_async_remote_copy(
            src_ref=b_ref.at[:, cols(j)], dst_ref=b_buf.at[j, slot(2), :],
            send_sem=b_snd_sem.at[j], recv_sem=b_rcv_sem.at[j], device_id=to_y, device_id_type=MESH)

    def send_d(j):
        return pltpu.make_async_remote_copy(
            src_ref=b_ref.at[:, cols(j)], dst_ref=b_buf.at[j, slot(1), :],
            send_sem=d_snd_sem.at[j], recv_sem=d_rcv_sem.at[j], device_id=to_d, device_id_type=MESH)

    def relay(j):
        return pltpu.make_async_remote_copy(
            src_ref=b_buf.at[j, slot(2), :], dst_ref=b_buf.at[j, slot(3), :],
            send_sem=r_snd_sem.at[j], recv_sem=r_rcv_sem.at[j], device_id=to_d, device_id_type=MESH)

    tail_rows = pl.ds(rows - ROUND, ROUND)

    def send_tail():
        return pltpu.make_async_remote_copy(
            src_ref=p_snd.at[n_here - 1, tail_rows, pl.ds(0, ROUND_N)], dst_ref=p_rcv.at[n_here - 1, tail_rows, pl.ds(0, ROUND_N)],
            send_sem=round_snd.at[0], recv_sem=round_rcv.at[0], device_id=to_x, device_id_type=MESH)

    def send_rest():
        rest = pl.ds(ROUND_N, TN - ROUND_N)
        return pltpu.make_async_remote_copy(
            src_ref=p_snd.at[n_here - 1, tail_rows, rest], dst_ref=p_rcv.at[n_here - 1, tail_rows, rest],
            send_sem=round_snd.at[2], recv_sem=round_rcv.at[2], device_id=to_x, device_id_type=MESH)

    early = pl.ds(0, EARLY)

    def send_early():
        return pltpu.make_async_remote_copy(
            src_ref=nbr_ref.at[early], dst_ref=early_rcv, send_sem=early_sem.at[0], recv_sem=early_sem.at[1],
            device_id=to_x, device_id_type=MESH)

    def go_round(step):
        src = p_snd.at[n_here - 1, tail_rows, pl.ds(0, ROUND_N)] if step == 0 else round_buf
        dst = p_rcv.at[n_here - 1, tail_rows, pl.ds(0, ROUND_N)] if step == 2 else round_buf
        return pltpu.make_async_remote_copy(
            src_ref=src, dst_ref=dst, send_sem=round_snd.at[1], recv_sem=round_rcv.at[0 if step == 2 else 1],
            device_id=to_x if step == 1 else to_y, device_id_type=MESH)

    def send_c(j, h):
        return pltpu.make_async_remote_copy(
            src_ref=p_snd.at[j, pl.ds(h * half, half), :], dst_ref=p_rcv.at[j, pl.ds(h * half, half), :],
            send_sem=c_snd_sem.at[j, h], recv_sem=c_rcv_sem.at[j, h], device_id=to_x, device_id_type=MESH)

    barrier = pltpu.get_barrier_semaphore()
    for peer in (to_x, {"depth": 0, "col": (1 - depth - col) * (1 - depth - col)}):
        pl.semaphore_signal(barrier, inc=1, device_id=peer, device_id_type=MESH)
    pl.semaphore_wait(barrier, 3 - 2 * depth)

    for i in range(4):
        send_a(i).start()

    @pl.when(depth == 0)
    def _():
        for i in range(4, last):
            send_a(i).start()
        for i in range(2):
            hand_over(i).start()
        pl.semaphore_signal(pair_sem, inc=1, device_id=to_y, device_id_type=MESH)
        pl.semaphore_wait(pair_sem, 1)
        pl.semaphore_signal(core_sem, inc=1, device_id=to_d, device_id_type=MESH)

    @pl.when(depth == 1)
    def _():
        pl.semaphore_wait(core_sem, 1)

    @pl.loop(0, n_chunks)
    def _(j):
        send_b(j).start()

    for place in range(4):
        load_a(place).start()

    def bring(j):
        send_d(j).start()
        load_b(j).start()

    for j in range(AHEAD):
        bring(j)

    @pl.when(depth == 1)
    def _():
        for i in range(2):
            hand_over(i).wait_recv()
            send_for_other(i).start()
        for i in range(4, last + 2):
            send_a(i).start()

    for place in range(4):
        load_a(place).wait()

    def part(j, h):
        p_snd[j, pl.ds(h * half, half), :] = jnp.dot(
            a_nbr[pl.ds(h * half, half), :], b_buf[j], preferred_element_type=jnp.float32)

    def gather(j):
        send_b(j).wait_recv()
        relay(j).start()

        @pl.when(j < n_chunks - AHEAD)
        def _():
            bring(j + AHEAD)

        load_b(j).wait()
        send_d(j).wait_recv()
        relay(j).wait_recv()

    @pl.loop(0, n_here)
    def _(j):
        gather(j)

        @pl.when(j == 0)
        def _():
            for i in range(4):
                send_a(i).wait_recv()

        @pl.when(j == LAG)
        def _():
            for i in range(4, last + 2):
                send_a(i).wait_recv()

        part(j, 0)

        @pl.when(j >= LAG)
        def _():
            part(j - LAG, 1)
            send_c(j, 0).start()

        p_own[j] = jnp.dot(a_own[...], b_buf[j], preferred_element_type=jnp.float32)

        @pl.when(j < LAG)
        def _():
            send_c(j, 0).start()

        @pl.when(j >= LAG)
        def _():
            send_c(j - LAG, 1).start()

    @pl.loop(n_here - LAG, n_here)
    def _(j):
        part(j, 1)

    def send_last():
        piece = pl.ds(half, half - ROUND)
        return pltpu.make_async_remote_copy(
            src_ref=p_snd.at[n_here - 1, piece, :], dst_ref=p_rcv.at[n_here - 1, piece, :],
            send_sem=c_snd_sem.at[n_here - 1, 1], recv_sem=c_rcv_sem.at[n_here - 1, 1],
            device_id=to_x, device_id_type=MESH)

    def add(j, piece):
        c_ref[piece, cols(j)] = (p_own[j, piece, :] + p_rcv[j, piece, :]).astype(c_ref.dtype)

    def finish(j):
        for h in range(2):
            send_c(j, h).wait_recv()
            add(j, pl.ds(h * half, half))

    finish(0)
    source = (depth == 1) & (row == 1) & (col == 0)
    first_relay = (depth == 1) & (row == 1) & (col == 1)
    second_relay = (depth == 1) & (row == 0) & (col == 1)
    for j in range(n_here - LAG, n_here - 1):
        send_c(j, 1).start()

    @pl.when(source)
    def _():
        go_round(0).start()

    @pl.when(first_relay)
    def _():
        go_round(0).wait_recv()
        go_round(1).start()

    send_rest().start()
    send_last().start()

    @pl.when(jnp.logical_not(source))
    def _():
        send_tail().start()

    gather(n_chunks - 1)
    nbr_ref[...] = jnp.dot(a_nbr[...], b_buf[n_chunks - 1], preferred_element_type=jnp.float32)
    own_ref[...] = jnp.dot(a_own[...], b_buf[n_chunks - 1], preferred_element_type=jnp.float32)

    @pl.when(depth == 1)
    def _():
        send_early().start()

    @pl.loop(1, n_here - LAG)
    def _(j):
        finish(j)

    for i in range(last):
        send_a(i).wait_send()

    @pl.when(depth == 0)
    def _():
        for i in range(2):
            hand_over(i).wait_send()

    @pl.when(depth == 1)
    def _():
        for i in range(2):
            send_a(last + i).wait_send()
            send_for_other(i).wait_send()

    @pl.loop(0, n_chunks)
    def _(j):
        send_b(j).wait_send()
        send_d(j).wait_send()
        relay(j).wait_send()

    @pl.loop(0, n_here - LAG)
    def _(j):
        for h in range(2):
            send_c(j, h).wait_send()

    for j in range(n_here - LAG, n_here - 1):
        finish(j)
        for h in range(2):
            send_c(j, h).wait_send()

    @pl.when(second_relay)
    def _():
        go_round(1).wait_recv()
        go_round(2).start()

    send_c(n_here - 1, 0).wait_recv()
    add(n_here - 1, pl.ds(0, half))
    send_last().wait_recv()
    add(n_here - 1, pl.ds(half, half - ROUND))
    send_rest().wait_recv()
    send_tail().wait_recv()
    add(n_here - 1, tail_rows)

    @pl.when(source | first_relay | second_relay)
    def _():
        go_round(0).wait_send()

    @pl.when(depth == 1)
    def _():
        send_early().wait_recv()
        c_ref[early, cols(n_chunks - 1)] = (own_ref[early, :] + early_rcv[...]).astype(c_ref.dtype)
        send_early().wait_send()

    send_c(n_here - 1, 0).wait_send()
    send_last().wait_send()
    send_rest().wait_send()

    @pl.when(jnp.logical_not(source))
    def _():
        send_tail().wait_send()


def last_kernel(own_ref, nbr_ref, out_ref, c_ref, rcv, snd_sem, rcv_sem):
    to_x = {"row": 1 - lax.axis_index("row")}
    depth = lax.axis_index("depth")
    rows = own_ref.shape[0]

    def send(piece):
        return pltpu.make_async_remote_copy(
            src_ref=nbr_ref.at[piece], dst_ref=rcv.at[piece], send_sem=snd_sem, recv_sem=rcv_sem,
            device_id=to_x, device_id_type=MESH)

    def exchange(piece):
        send(piece).start()
        send(piece).wait_recv()
        c_ref[piece, :] = (own_ref[piece, :] + rcv[piece, :]).astype(c_ref.dtype)
        send(piece).wait_send()

    barrier = pltpu.get_barrier_semaphore()
    pl.semaphore_signal(barrier, inc=1, device_id=to_x, device_id_type=MESH)
    pl.semaphore_wait(barrier, 1)

    @pl.when(depth == 0)
    def _():
        exchange(pl.ds(0, rows))

    @pl.when(depth == 1)
    def _():
        exchange(pl.ds(EARLY, rows - EARLY))


def write_first(c_ref, out_ref, sem):
    depth = lax.axis_index("depth")
    n, tail = c_ref.shape[1] - TN, pl.ds(c_ref.shape[1] - TN, TN)
    early = pl.ds(0, EARLY)
    copy = pltpu.make_async_copy(c_ref.at[:, pl.ds(0, n)], out_ref.at[:, pl.ds(0, n)], sem.at[0])
    more = pltpu.make_async_copy(c_ref.at[early, tail], out_ref.at[early, tail], sem.at[1])
    copy.start()

    @pl.when(depth == 1)
    def _():
        more.start()
        more.wait()

    copy.wait()


def write_last(whole_ref, c_ref, out_ref, sem):
    rows = c_ref.shape[0]
    tail = pl.ds(out_ref.shape[1] - TN, TN)

    def copy(start, size):
        piece = pl.ds(start, size)
        return pltpu.make_async_copy(c_ref.at[piece], out_ref.at[piece, tail], sem)

    copy(EARLY, rows - EARLY).start()
    depth = lax.axis_index("depth")

    @pl.when(depth == 0)
    def _():
        copy(0, EARLY).start()
        copy(0, rows).wait()

    @pl.when(depth == 1)
    def _():
        copy(EARLY, rows - EARLY).wait()


def solution(mesh):
    all_axes = ("depth", "row", "col")

    def device_block(a_rows, b_rows):
        rows, depth = a_rows.shape
        k_rows, n = b_rows.shape
        k = 4 * k_rows
        n_chunks = n // TN
        dma = pltpu.SemaphoreType.DMA
        n_here = n_chunks - 1
        f32 = jnp.float32
        vmem, any_space = pl.BlockSpec(memory_space=pltpu.VMEM), pl.BlockSpec(memory_space=pl.ANY)
        kept = 2 * rows * n + 8 * rows * TN
        regular = pltpu.SemaphoreType.REGULAR
        c, own, nbr = pl.pallas_call(
            kernel,
            out_shape=(pltpu.VMEM((rows, n), jnp.bfloat16),
                       pltpu.VMEM((rows, TN), f32), pltpu.VMEM((rows, TN), f32)),
            in_specs=[any_space] * 2,
            out_specs=(vmem,) * 3,
            scratch_shapes=[
                pltpu.VMEM((n_chunks, k, TN), jnp.bfloat16),
                pltpu.VMEM((rows, k), jnp.bfloat16),
                pltpu.VMEM((rows, k), jnp.bfloat16),
                pltpu.VMEM((n_here, rows, TN), f32),
                pltpu.VMEM((n_here, rows, TN), f32),
                pltpu.VMEM((n_here, rows, TN), f32),
                pltpu.VMEM((2, EXTRA, k_rows), jnp.bfloat16),
                dma((4,)), dma((n_chunks,)),
                dma((10,)), dma((10,)),
                dma((n_chunks,)), dma((n_chunks,)),
                dma((n_chunks,)), dma((n_chunks,)),
                dma((n_chunks,)), dma((n_chunks,)),
                dma((n_here, 2)), dma((n_here, 2)),
                dma((2,)), dma((2,)), dma((2,)),
                regular, regular,
                pltpu.VMEM((ROUND, ROUND_N), f32), dma((3,)), dma((3,)),
                pltpu.VMEM((EARLY, TN), f32), dma((2,)),
            ],
            compiler_params=pltpu.CompilerParams(
                collective_id=0, has_side_effects=True, vmem_limit_bytes=67043328 - kept),
        )(a_rows, b_rows)
        in_vmem = lambda x: pltpu.with_memory_space_constraint(x, pltpu.VMEM)
        small = pltpu.CompilerParams(vmem_limit_bytes=2 ** 20)
        whole = jax.ShapeDtypeStruct((rows, n), jnp.bfloat16)
        out = pl.pallas_call(
            write_first, out_shape=whole, in_specs=[vmem], out_specs=any_space,
            scratch_shapes=[dma((2,))], compiler_params=small)(in_vmem(c))
        c_last = pl.pallas_call(
            last_kernel,
            out_shape=pltpu.VMEM((rows, TN), jnp.bfloat16),
            in_specs=[vmem, vmem, pl.BlockSpec(memory_space=pltpu.HBM)],
            out_specs=vmem,
            scratch_shapes=[pltpu.VMEM((rows, TN), f32), dma, dma],
            compiler_params=pltpu.CompilerParams(
                collective_id=1, has_side_effects=True, vmem_limit_bytes=2 ** 23),
        )(in_vmem(own), in_vmem(nbr), pltpu.with_memory_space_constraint(out, pltpu.HBM))
        return pl.pallas_call(
            write_last, out_shape=whole, in_specs=[any_space, vmem], out_specs=any_space,
            scratch_shapes=[dma], input_output_aliases={0: 0}, compiler_params=small)(out, in_vmem(c_last))

    return jax.shard_map(device_block, mesh=mesh, in_specs=(P(all_axes, None), P(all_axes, None)),
                         out_specs=P(all_axes, None), check_vma=False)
```
